32 devices in a mesh: groups: 2 (over y), ctx: 4 (over z), ep: 2 (over x), tp: 2 (over core).
Axes of the slice: x: 2, y: 2, z: 4, core: 2. Of those that a mesh axis runs over, the one named last changes fastest.
Arguments:
- queries: bfloat16 [4, 512, 5120], P(('groups', 'ep'), 'ctx', 'tp'), parts along dimension 0, may hold values from -128 to 128
- keys: bfloat16 [4, 512, 1024], P(('groups', 'ep'), 'ctx', 'tp'), parts along dimension 0, may hold values from -6 to 6
- values: bfloat16 [4, 512, 1024], P(('groups', 'ep'), 'ctx', 'tp'), parts along dimension 0, may hold values from -6 to 6
- expert_ids: int32 [4, 512, 1], P(('groups', 'ep'), 'ctx'), parts along dimension 0, may hold values from 0 to 127, as said below
- router: bfloat16 [5120, 2], P('tp', 'ep'), may hold values from -0.3125 to 0.3125
- w_gate: bfloat16 [2, 5120, 4096], P('ep', 'tp', 'ctx'), may hold values from -0.3125 to 0.3125
- w_up: bfloat16 [2, 5120, 4096], P('ep', 'tp', 'ctx'), may hold values from -0.3125 to 0.3125
- w_down: bfloat16 [2, 4096, 5120], P('ep', 'ctx', 'tp'), may hold values from -0.09375 to 0.09375
Outputs:
- layer_out: bfloat16 [4, 512, 5120], P(('groups', 'ep'), 'ctx', 'tp'), parts along dimension 0
The draws below stay inside these ranges and needn't reach their ends.
There are 2 independent parts, one for each index of `groups`. The reference program is written for one: setup_inputs(seed, part) draws one part's arguments, and reference() takes and returns one part's arrays. A program takes and returns all parts, laid end to end along the dimension named above; an argument that names none is the same for every part. Nothing has to cross between parts.
Inputs may be any that keep to these rules, and one draw needn't show every extreme that they name: `expert_ids`: among the positions of one device, each expert below 2 is named at most 2 times; in every draw one of them is named exactly 2 times on every device.
All inputs are finite; a program needn't handle non-finite values.
Results may differ from the reference program's by a relative error of at most 0.023.
Values may be sent and summed in bfloat16 or wider, within the bound.
A program may use at most 64 MiB of HBM per device.

```python
import math
import jax
import jax.numpy as jnp
from jax import lax

HEAD_WIDTH = 128
QUERY_HEADS = 40
KEY_VALUE_HEADS = 8
D = 5120
EXPERTS = 128
FE = 4096
SEQ_DEV = 128
PROMPT_LENGTH = 512
PROMPT_BATCH = 2
EXP_WIN = 2
CAP = 2


def shared_keys(key):
    return jax.random.truncated_normal(jax.random.fold_in(key, 11), -6.0, 6.0, (PROMPT_BATCH, PROMPT_LENGTH, KEY_VALUE_HEADS, HEAD_WIDTH), jnp.float32)


def draw_keys(key, part):
    unprojected_keys = shared_keys(key)
    return unprojected_keys.reshape(PROMPT_BATCH, PROMPT_LENGTH, KEY_VALUE_HEADS * HEAD_WIDTH).astype(jnp.bfloat16)


def draw_queries(key, part):
    base = 2.5 * jax.random.truncated_normal(jax.random.fold_in(key, 23), -6.0, 6.0, (PROMPT_BATCH, PROMPT_LENGTH, QUERY_HEADS, HEAD_WIDTH), jnp.float32)
    return base.reshape(PROMPT_BATCH, PROMPT_LENGTH, QUERY_HEADS * HEAD_WIDTH).astype(jnp.bfloat16)


def shuffled(sub_key):
    return jax.random.permutation(sub_key, SEQ_DEV)


def draw_expert_ids(key, part):
    blocks = PROMPT_BATCH * (PROMPT_LENGTH // SEQ_DEV)
    count_key = jax.random.fold_in(key, 41)
    full_key = jax.random.fold_in(key, 43)
    outside_key = jax.random.fold_in(key, 47)
    order_key = jax.random.fold_in(key, 53)
    counts = jax.random.randint(count_key, (blocks, EXP_WIN), 0, CAP + 1, dtype=jnp.int32)
    full_expert = jax.random.randint(full_key, (), 0, EXP_WIN, dtype=jnp.int32)
    counts = jnp.where(jnp.arange(EXP_WIN, dtype=jnp.int32)[None, :] == full_expert, CAP, counts)
    count_ends = jnp.cumsum(counts, axis=1)
    rank_index = jnp.arange(SEQ_DEV, dtype=jnp.int32)
    expert_rank = jnp.sum((count_ends[:, None, :] <= rank_index[None, :, None]).astype(jnp.int32), axis=2)
    outside = jax.random.randint(outside_key, (blocks, SEQ_DEV), EXP_WIN, EXPERTS, dtype=jnp.int32)
    named = jnp.where(expert_rank < EXP_WIN, expert_rank, outside)
    shuffles = jax.vmap(shuffled)(jax.random.split(order_key, blocks))
    inverse = jnp.argsort(shuffles, axis=1)
    placed = jnp.take_along_axis(named, inverse, axis=1)
    return placed.reshape(PROMPT_BATCH, PROMPT_LENGTH, 1).astype(jnp.int32)


def block_levels(stream_key, shape, cuts, smallest, largest):
    gain = 1.0
    for dim, parts in cuts:
        steps = jax.random.uniform(jax.random.fold_in(jax.random.fold_in(stream_key, 6), dim), (parts,), jnp.float32, smallest / len(cuts), largest / len(cuts))
        gain = gain * jnp.repeat(jnp.exp(steps), shape[dim] // parts).reshape((-1,) + (1,) * (len(shape) - 1 - dim))
    return gain


def normal_values(stream_key, dims, deviation, most, cuts=(), kind=jnp.bfloat16):
    drawn = deviation * jax.random.normal(stream_key, dims, jnp.float32)
    if cuts:
        drawn = drawn * block_levels(stream_key, dims, cuts, -0.22, 0.18)
    return jnp.clip(drawn, -most, most).astype(kind)


def setup_inputs(seed: int = 0, part: int = 0) -> dict:
    arg_keys = jax.random.split(jax.random.key(seed), 9)
    own_keys = jax.random.split(jax.random.fold_in(arg_keys[8], part), 9)
    return {
        "queries": draw_queries(jax.random.fold_in(jax.random.fold_in(arg_keys[8], part), 71), part),
        "keys": draw_keys(jax.random.fold_in(jax.random.fold_in(arg_keys[8], part), 71), part),
        "values": normal_values(own_keys[2], (PROMPT_BATCH, PROMPT_LENGTH, KEY_VALUE_HEADS * HEAD_WIDTH), 1.0, 6.0, ((0, 2), (1, 4), (2, 2))),
        "expert_ids": draw_expert_ids(jax.random.fold_in(jax.random.fold_in(arg_keys[8], part), 71), part),
        "router": normal_values(arg_keys[4], (D, EXP_WIN), (D // 16) ** -0.5, 0.3125, ((0, 2), (1, 2))),
        "w_gate": normal_values(arg_keys[5], (EXP_WIN, D, FE), (D // 16) ** -0.5, 0.3125, ((0, 2), (1, 2), (2, 4))),
        "w_up": normal_values(arg_keys[6], (EXP_WIN, D, FE), (D // 16) ** -0.5, 0.3125, ((0, 2), (1, 2), (2, 4))),
        "w_down": normal_values(arg_keys[7], (EXP_WIN, FE, D), FE ** -0.5, 0.09375, ((0, 2), (1, 4), (2, 2))),
    }


def attend_sequence(query_sequence, key_sequence, value_sequence):
    group_width = QUERY_HEADS // KEY_VALUE_HEADS
    rows_per_block = math.gcd(PROMPT_LENGTH, 256)
    query_block_list = query_sequence.reshape(PROMPT_LENGTH // rows_per_block, rows_per_block, KEY_VALUE_HEADS, group_width, HEAD_WIDTH)
    complete_keys = key_sequence.reshape(PROMPT_LENGTH, KEY_VALUE_HEADS, HEAD_WIDTH).astype(jnp.float32)
    complete_values = value_sequence.reshape(PROMPT_LENGTH, KEY_VALUE_HEADS, HEAD_WIDTH).astype(jnp.float32)
    key_pos = jnp.arange(PROMPT_LENGTH, dtype=jnp.int32)

    def one_block(inputs):
        query_block, begin_row = inputs
        scores = jnp.einsum("rgqd,kgd->gqrk", query_block.astype(jnp.float32), complete_keys) * (HEAD_WIDTH ** -0.5)
        query_pos = begin_row + jnp.arange(rows_per_block, dtype=jnp.int32)
        visible = query_pos[:, None] >= key_pos[None, :]
        scores = jnp.where(visible, scores, -1e30)
        row_max = jnp.max(scores, axis=3, keepdims=True)
        weights = jnp.where(visible, jnp.exp(scores - row_max), 0.0)
        totals = jnp.sum(weights, axis=3)
        rounded = lax.optimization_barrier(weights.astype(jnp.bfloat16)).astype(jnp.float32)
        weighted = jnp.einsum("gqrk,kgd->rgqd", rounded, complete_values)
        normed = weighted / jnp.transpose(totals, (2, 0, 1))[..., None]
        return normed.astype(jnp.bfloat16).reshape(rows_per_block, D)

    starts = jnp.arange(PROMPT_LENGTH // rows_per_block, dtype=jnp.int32) * rows_per_block
    return lax.map(one_block, (query_block_list, starts)).reshape(PROMPT_LENGTH, D)


def reference(queries, keys, values, expert_ids, router, w_gate, w_up, w_down):
    attended = jnp.stack([attend_sequence(queries[prompt], keys[prompt], values[prompt]) for prompt in range(PROMPT_BATCH)])
    token_count = PROMPT_BATCH * PROMPT_LENGTH
    flat_tokens = attended.reshape(token_count, D)
    chosen = expert_ids.reshape(token_count).astype(jnp.int32)
    sort_order = jnp.argsort(chosen, stable=True).astype(jnp.int32)
    counts = jnp.sum((chosen[:, None] == jnp.arange(EXP_WIN, dtype=jnp.int32)[None, :]).astype(jnp.int32), axis=0)
    offsets = (jnp.cumsum(counts) - counts).astype(jnp.int32)
    most_rows = CAP * PROMPT_BATCH * (PROMPT_LENGTH // SEQ_DEV)
    padded_order = jnp.concatenate([sort_order, jnp.zeros((most_rows,), jnp.int32)])

    def expert_step(routed, inputs):
        expert, gate_w, up_w, down_w, router_col = inputs
        picked = lax.dynamic_slice_in_dim(padded_order, offsets[expert], most_rows)
        live_rows = jnp.arange(most_rows, dtype=jnp.int32) < counts[expert]
        members = flat_tokens[picked]
        gate_part = jnp.dot(members, gate_w, preferred_element_type=jnp.float32)
        up_part = jnp.dot(members, up_w, preferred_element_type=jnp.float32)
        router_score = jnp.dot(members, router_col[:, None], preferred_element_type=jnp.float32)
        weight = jax.nn.sigmoid(router_score)
        hidden = (jax.nn.silu(weight * gate_part) * (weight * up_part)).astype(jnp.bfloat16)
        output = jnp.dot(hidden, down_w, preferred_element_type=jnp.float32).astype(jnp.bfloat16)
        output = lax.optimization_barrier(output).astype(jnp.float32)
        output = jnp.where(live_rows[:, None], output, 0.0)
        return routed.at[picked].add(output), None

    routed, _ = lax.scan(expert_step, jnp.zeros((token_count, D), jnp.float32),
                         (jnp.arange(EXP_WIN, dtype=jnp.int32), w_gate, w_up, w_down, router.T))
    layer_out = (flat_tokens.astype(jnp.float32) + routed).astype(jnp.bfloat16)
    return layer_out.reshape(PROMPT_BATCH, PROMPT_LENGTH, D)
```

```python
import functools
import math

import jax
import jax.numpy as jnp
from jax import lax
from jax.experimental import pallas as pl
from jax.experimental.pallas import tpu as pltpu
from jax.sharding import PartitionSpec as P

HEAD_WIDTH = 128
CAP = 2
MESH = pl.DeviceIdType.MESH
MASKED = -1e30
EXP2_SCALE = HEAD_WIDTH ** (-0.5) * math.log2(math.e)


def tiles_of(width, tile):
    tile = min(width, tile)
    return [(start, min(tile, width - start)) for start in range(0, width, tile)]


def each(count, body):
    if count <= 8:
        for index in range(count):
            body(index)
    else:
        pl.loop(0, count)(body)


def kernel(
    n_ctx, n_ep, n_tp,
    ids_hbm, router_hbm, q_hbm, k_hbm, v_hbm, wg_hbm, wu_hbm, wd_hbm,
    out_ref,
    ids_ref, router_ref, q_ref, wg, wu, wd, kbuf, vbuf, acc, row_max, totals, att,
    q_out, q_in, q_all, part_out, part_got, part_all, lse_out, lse_in, lse_all, out_rows, in_rows, members_f32, part, part_in, score, score_in, hidden,
    down_out, down_in, returned,
    w_sem, in_sem, kv_send, kv_recv, row_send, row_recv, part_send, part_recv, score_sem,
    down_send, down_recv, q_send, q_recv, back_send, back_recv, lse_send, lse_recv,
):
    ctx = lax.axis_index("ctx")
    ep = lax.axis_index("ep")
    tp = lax.axis_index("tp")
    n = n_ctx * n_ep
    me = ep * n_ctx + ctx
    rows, features = q_ref.shape
    kv_heads = kbuf.shape[2] // HEAD_WIDTH
    group = features // HEAD_WIDTH // kv_heads
    half = rows // 2
    fan = n_ctx // 2
    hidden_width = wg.shape[1]
    chunk_count, _, double_width = part.shape
    chunk_width = double_width // 2
    slots = returned.shape[0]
    places = features // HEAD_WIDTH

    in_copies = [
        pltpu.make_async_copy(src, dst, in_sem.at[index])
        for index, (src, dst) in enumerate((
            (ids_hbm, ids_ref), (q_hbm.at[0], q_ref), (k_hbm.at[0], kbuf.at[ctx]),
            (v_hbm.at[0], vbuf.at[ctx]), (router_hbm, router_ref),
        ))
    ]
    for copy in in_copies:
        copy.start()
    w_copies = [
        pltpu.make_async_copy(src.at[0], dst, w_sem.at[index])
        for index, (src, dst) in enumerate(((wg_hbm, wg), (wu_hbm, wu), (wd_hbm, wd)))
    ]
    for copy in w_copies:
        copy.start()

    barrier = pltpu.get_barrier_semaphore()

    def greet(other):
        @pl.when(other != me)
        def _():
            pl.semaphore_signal(
                barrier, inc=1,
                device_id={"ep": other // n_ctx, "ctx": other % n_ctx},
                device_id_type=MESH,
            )

    each(n, greet)
    for step in range(1, n_tp):
        pl.semaphore_signal(
            barrier, inc=1, device_id={"tp": (tp + step) % n_tp}, device_id_type=MESH
        )
    in_copies[0].wait()
    ids = ids_ref[...]
    slot_row = lax.broadcasted_iota(jnp.int32, (slots, rows), 0)
    choose = jnp.where(ids == slot_row, 1.0, 0.0)
    below = lax.broadcasted_iota(jnp.int32, (rows, rows), 0)
    across = lax.broadcasted_iota(jnp.int32, (rows, rows), 1)
    strict = jnp.where(below < across, 1.0, 0.0).astype(jnp.bfloat16)
    earlier = jnp.dot(choose.astype(jnp.bfloat16), strict, preferred_element_type=jnp.float32)
    slot_index = jnp.sum(earlier * choose, axis=0, keepdims=True).astype(jnp.int32)
    target_row = jnp.where(ids < n_ep, ids * CAP + slot_index, -1)
    spread = jnp.where(target_row == slot_row, 1.0, 0.0).astype(jnp.bfloat16)
    live = n_ep * CAP
    lane_row = lax.broadcasted_iota(jnp.int32, (slots, rows), 1)
    row_place = jnp.sum(
        jnp.where(target_row == slot_row, lane_row, 0), axis=1, keepdims=True
    )
    q_all[...] = jnp.zeros_like(q_all)
    in_copies[1].wait()
    own_span = pl.ds(pl.multiple_of(ctx * slots, 8), slots)
    for start, size in tiles_of(features, 512):
        picked = jnp.dot(
            spread, q_ref[:, start:start + size], preferred_element_type=jnp.float32
        )
        q_all[own_span, start:start + size] = picked
        q_out[:, start:start + size] = picked[:live].astype(jnp.bfloat16)

    pl.semaphore_wait(barrier, n - 1 + n_tp - 1)

    def own_copy(piece):
        return block_piece(ctx, piece)

    def block_piece(block, piece):
        buf = kbuf if piece < 2 else vbuf
        span = pl.ds((piece % 2) * half, half)
        return pltpu.make_async_remote_copy(
            src_ref=buf.at[block, span],
            dst_ref=buf.at[block, span],
            send_sem=kv_send.at[block, piece],
            recv_sem=kv_recv.at[block, piece],
            device_id={"ctx": ctx + 1},
            device_id_type=MESH,
        )

    def push_own(first, last):
        @pl.when(ctx < n_ctx - 1)
        def _():
            for piece in range(first, last):
                own_copy(piece).start()

    def relay(block, first, last):
        @pl.when(block >= 0)
        def _():
            for piece in range(first, last):
                copy = block_piece(block, piece)
                copy.wait_recv()

                @pl.when(ctx < n_ctx - 1)
                def _():
                    copy.start()

    def q_copy(source, target):
        return pltpu.make_async_remote_copy(
            src_ref=q_out, dst_ref=q_in.at[source],
            send_sem=q_send.at[target], recv_sem=q_recv.at[source],
            device_id={"ctx": target}, device_id_type=MESH,
        )

    def back_copies(source, target):
        return [
            pltpu.make_async_remote_copy(
                src_ref=out.at[target], dst_ref=into.at[source],
                send_sem=sent.at[target], recv_sem=got.at[source],
                device_id={"ctx": target}, device_id_type=MESH,
            )
            for out, into, sent, got in (
                (part_out, part_got, back_send, back_recv),
                (lse_out, lse_in, lse_send, lse_recv),
            )
        ]

    def lower(body):
        def one(other):
            @pl.when(other < ctx)
            def _():
                body(other)

        each(n_ctx, one)

    def upper(body):
        def one(other):
            @pl.when(other > ctx)
            def _():
                body(other)

        each(n_ctx, one)

    lower(lambda other: q_copy(ctx, other).start())
    in_copies[2].wait()
    in_copies[3].wait()
    push_own(0, 2)

    acc[...] = jnp.zeros_like(acc)
    totals[...] = jnp.zeros_like(totals)
    row_max[...] = jnp.full_like(row_max, MASKED)

    query_offset = lax.broadcasted_iota(jnp.int32, (rows, rows), 0)
    key_offset = lax.broadcasted_iota(jnp.int32, (rows, rows), 1)
    offset_gap = query_offset - key_offset

    def process(block):
        visible = offset_gap >= (block - ctx) * rows
        visible = jnp.concatenate([visible] * group, axis=0)
        for head in range(kv_heads):
            lanes = slice(head * HEAD_WIDTH, (head + 1) * HEAD_WIDTH)
            stacked = jnp.concatenate(
                [
                    q_ref[:, (head * group + j) * HEAD_WIDTH:(head * group + j + 1) * HEAD_WIDTH]
                    for j in range(group)
                ],
                axis=0,
            )
            raw = lax.dot_general(
                stacked, kbuf[block, :, lanes], (((1,), (1,)), ((), ())),
                preferred_element_type=jnp.float32,
            )
            raw = jnp.where(visible, raw, MASKED)
            old_max = row_max[head]
            new_max = jnp.maximum(old_max, jnp.max(raw, axis=1, keepdims=True))
            factor = jnp.exp2((old_max - new_max) * EXP2_SCALE)
            weights = jnp.exp2((raw - new_max[:, :rows]) * EXP2_SCALE)
            row_max[head] = new_max
            totals[head] = totals[head] * factor + jnp.sum(weights, axis=1, keepdims=True)
            update = jnp.dot(
                weights.astype(jnp.bfloat16), vbuf[block, :, lanes],
                preferred_element_type=jnp.float32,
            )
            acc[head] = acc[head] * factor + update

    part_all[...] = jnp.zeros_like(part_all)
    lse_all[...] = jnp.full_like(lse_all, MASKED)
    source_row = lax.broadcasted_iota(jnp.int32, (n_ctx * slots, 1), 0) // slots
    limit = jnp.where(
        source_row == ctx, jnp.concatenate([row_place] * n_ctx, axis=0), rows
    )
    limit = jnp.concatenate([limit] * group, axis=0)
    upper(lambda other: q_copy(other, other).wait_recv())

    for other in range(n_ctx):
        @pl.when(other > ctx)
        def _():
            q_all[other * slots:other * slots + live, :] = q_in[other].astype(jnp.float32)

    tall = n_ctx * slots
    key_lane = lax.broadcasted_iota(jnp.int32, (group * tall, rows), 1)
    seen = key_lane <= limit
    head_lane = lax.broadcasted_iota(jnp.int32, (tall, 128), 1)
    lse = jnp.zeros((tall, 128), jnp.float32)
    for head in range(kv_heads):
        lanes = slice(head * HEAD_WIDTH, (head + 1) * HEAD_WIDTH)
        stacked = jnp.concatenate(
            [
                q_all[:, (head * group + j) * HEAD_WIDTH:(head * group + j + 1) * HEAD_WIDTH]
                for j in range(group)
            ],
            axis=0,
        ).astype(jnp.bfloat16)
        raw = lax.dot_general(
            stacked, kbuf[ctx, :, lanes], (((1,), (1,)), ((), ())),
            preferred_element_type=jnp.float32,
        )
        raw = jnp.where(seen, raw, MASKED)
        top = jnp.max(raw, axis=1, keepdims=True)
        weights = jnp.exp2((raw - top) * EXP2_SCALE)
        total = jnp.sum(weights, axis=1, keepdims=True)
        mixed = jnp.dot(
            weights.astype(jnp.bfloat16), vbuf[ctx, :, lanes],
            preferred_element_type=jnp.float32,
        ) / total
        column = top * EXP2_SCALE + jnp.log2(total)
        for j in range(group):
            place = head * group + j
            lse = jnp.where(head_lane == place, column[j * tall:(j + 1) * tall], lse)
            for other in range(n_ctx):
                first = j * tall + other * slots
                part_out[other, :, place * HEAD_WIDTH:(place + 1) * HEAD_WIDTH] = mixed[
                    first:first + live
                ].astype(jnp.bfloat16)
    for other in range(n_ctx):
        lse_out[other] = lse[other * slots:(other + 1) * slots]

    def give_back(other):
        for copy in back_copies(ctx, other):
            copy.start()

    upper(give_back)
    push_own(2, 4)

    def take_back(other):
        for copy in back_copies(other, other):
            copy.wait_recv()

    lower(take_back)
    for other in range(n_ctx):
        @pl.when(other < ctx)
        def _():
            part_all[other, :live] = part_got[other].astype(jnp.float32)
            lse_all[other] = lse_in[other]

        @pl.when(other == ctx)
        def _():
            part_all[other, :live] = part_out[other].astype(jnp.float32)
            lse_all[other] = lse_out[other]

    peak = jnp.max(lse_all[...], axis=0)
    shares = [jnp.exp2(lse_all[other] - peak) for other in range(n_ctx)]
    share_total = functools.reduce(jnp.add, shares)
    shares = [share / share_total for share in shares]
    for place in range(kv_heads * group):
        span = slice(place * HEAD_WIDTH, (place + 1) * HEAD_WIDTH)
        picked = shares[0][:, place:place + 1] * part_all[0, :, span]
        for other in range(1, n_ctx):
            picked = picked + shares[other][:, place:place + 1] * part_all[other, :, span]
        for expert in range(n_ep):
            out_rows[expert, place * CAP:(place + 1) * CAP] = picked[expert * CAP:(expert + 1) * CAP].astype(
                jnp.bfloat16
            )

    def row_copy(other, source):
        return pltpu.make_async_remote_copy(
            src_ref=out_rows.at[other // n_ctx],
            dst_ref=in_rows.at[source],
            send_sem=row_send.at[other],
            recv_sem=row_recv.at[source],
            device_id={"ep": other // n_ctx, "ctx": other % n_ctx},
            device_id_type=MESH,
        )

    def others(body):
        def one(step):
            @pl.when(step != me)
            def _():
                body(step)

        each(n, one)

    others(lambda other: row_copy(other, me).start())
    in_rows[me] = out_rows[ep]
    process(ctx)
    relay(ctx - 1, 0, 4)
    for copy in w_copies:
        copy.wait()
    others(lambda other: row_copy(other, other).wait_recv())

    def gather_member(index):
        dense = in_rows[index].astype(jnp.float32)
        for place in range(places):
            span = slice(place * HEAD_WIDTH, (place + 1) * HEAD_WIDTH)
            members_f32[index * CAP:(index + 1) * CAP, span] = dense[
                place * CAP:(place + 1) * CAP
            ]

    for index in range(n):
        gather_member(index)
    in_copies[4].wait()
    wide = members_f32[...]
    members = wide.astype(jnp.bfloat16)
    own_score = jnp.sum(wide * router_ref[...].astype(jnp.float32), axis=1, keepdims=True)
    score[...] = jnp.broadcast_to(own_score, score.shape).astype(jnp.bfloat16)
    peer = {"tp": n_tp - 1 - tp}
    score_copy = pltpu.make_async_remote_copy(
        src_ref=score, dst_ref=score_in, send_sem=score_sem.at[0], recv_sem=score_sem.at[1],
        device_id=peer, device_id_type=MESH,
    )
    score_copy.start()
    part_copies = []
    for chunk in range(chunk_count):
        span = slice(chunk * chunk_width, (chunk + 1) * chunk_width)
        part[chunk, :, :chunk_width] = jnp.dot(
            members, wg[:, span], preferred_element_type=jnp.float32
        ).astype(jnp.bfloat16)
        part[chunk, :, chunk_width:] = jnp.dot(
            members, wu[:, span], preferred_element_type=jnp.float32
        ).astype(jnp.bfloat16)
        copy = pltpu.make_async_remote_copy(
            src_ref=part.at[chunk], dst_ref=part_in.at[chunk],
            send_sem=part_send.at[chunk], recv_sem=part_recv.at[chunk],
            device_id=peer, device_id_type=MESH,
        )
        copy.start()
        part_copies.append(copy)
    relay(ctx - 2, 0, 2)
    score_copy.wait()
    gain = jax.nn.sigmoid(
        score[:, :1].astype(jnp.float32) + score_in[:, :1].astype(jnp.float32)
    )
    for chunk, copy in enumerate(part_copies):
        copy.wait()
        both = part[chunk].astype(jnp.float32) + part_in[chunk].astype(jnp.float32)
        gate = gain * both[:, :chunk_width]
        up = gain * both[:, chunk_width:]
        hidden[:, chunk * chunk_width:(chunk + 1) * chunk_width] = (
            gate * jax.nn.sigmoid(gate) * up
        ).astype(jnp.bfloat16)
    for start, size in tiles_of(features, 512):
        product = jnp.dot(
            hidden[...], wd[:, start:start + size], preferred_element_type=jnp.float32
        )
        for index in range(n):
            for place in range(start // HEAD_WIDTH, (start + size) // HEAD_WIDTH):
                lane = place * HEAD_WIDTH - start
                down_out[index, place * CAP:(place + 1) * CAP] = product[
                    index * CAP:(index + 1) * CAP, lane:lane + HEAD_WIDTH
                ].astype(jnp.bfloat16)

    def down_copy(other, source):
        return pltpu.make_async_remote_copy(
            src_ref=down_out.at[other],
            dst_ref=down_in.at[source],
            send_sem=down_send.at[other],
            recv_sem=down_recv.at[source],
            device_id={"ep": other // n_ctx, "ctx": other % n_ctx},
            device_id_type=MESH,
        )

    others(lambda other: down_copy(other, me).start())
    down_in[me] = down_out[me]
    returned[...] = jnp.zeros_like(returned)

    def visit(step, carry):
        block = ctx - step

        @pl.when(step == 2)
        def _():
            relay(block, 2, 4)

        @pl.when(step > 2)
        def _():
            relay(block, 0, 4)

        @pl.when(block >= 0)
        def _():
            process(block)

        return carry

    lax.fori_loop(1, n_ctx, visit, 0)

    for head in range(kv_heads):
        normed = (acc[head] / totals[head]).astype(jnp.bfloat16)
        for j in range(group):
            place = (head * group + j) * HEAD_WIDTH
            att[:, place:place + HEAD_WIDTH] = normed[j * rows:(j + 1) * rows]

    others(lambda other: row_copy(other, me).wait_send())
    lower(lambda other: q_copy(ctx, other).wait_send())

    def sent_back(other):
        for copy in back_copies(ctx, other):
            copy.wait_send()

    upper(sent_back)

    def drain(step, carry):
        block = ctx - step

        @pl.when((ctx < n_ctx - 1) & (block >= 0))
        def _():
            for piece in range(4):
                block_piece(block, piece).wait_send()

        return carry

    lax.fori_loop(0, n_ctx, drain, 0)

    others(lambda other: down_copy(other, other).wait_recv())
    for expert in range(n_ep):
        total = down_in[expert * n_ctx].astype(jnp.float32)
        for index in range(1, n_ctx):
            total = total + down_in[expert * n_ctx + index].astype(jnp.float32)
        total = total.astype(jnp.bfloat16).astype(jnp.float32)
        for place in range(places):
            span = slice(place * HEAD_WIDTH, (place + 1) * HEAD_WIDTH)
            returned[expert * CAP:(expert + 1) * CAP, span] = total[
                place * CAP:(place + 1) * CAP
            ]
    for start, size in tiles_of(features, 512):
        routed = lax.dot_general(
            spread, returned[:, start:start + size].astype(jnp.bfloat16),
            (((0,), (0,)), ((), ())), preferred_element_type=jnp.float32,
        )
        out_ref[0, :, start:start + size] = (
            att[:, start:start + size].astype(jnp.float32) + routed
        ).astype(jnp.bfloat16)
    others(lambda other: down_copy(other, me).wait_send())


def shards(queries, keys, values, expert_ids, router, w_gate, w_up, w_down):
    n_ctx, n_ep, n_tp = (lax.axis_size(axis) for axis in ("ctx", "ep", "tp"))
    n = n_ctx * n_ep
    _, rows, features = queries.shape
    kv_width = keys.shape[2]
    kv_heads = kv_width // HEAD_WIDTH
    group = features // kv_width
    hidden_width = w_gate.shape[2]
    chunk_width = min(hidden_width, 256)
    chunk_count = hidden_width // chunk_width
    members = n * CAP
    dense = features // HEAD_WIDTH * CAP
    live = n_ep * CAP
    slots = -(-live // 8) * 8
    bf16, f32 = jnp.bfloat16, jnp.float32
    vmem = pl.BlockSpec(memory_space=pltpu.VMEM)
    hbm = pl.BlockSpec(memory_space=pltpu.HBM)
    dma = pltpu.SemaphoreType.DMA
    return pl.pallas_call(
        functools.partial(kernel, n_ctx, n_ep, n_tp),
        out_shape=pltpu.VMEM(queries.shape, bf16),
        in_specs=[hbm] * 8,
        out_specs=vmem,
        scratch_shapes=[
            pltpu.VMEM((1, rows), jnp.int32),
            pltpu.VMEM((1, features), bf16),
            pltpu.VMEM((rows, features), bf16),
            pltpu.VMEM(w_gate.shape[1:], bf16),
            pltpu.VMEM(w_up.shape[1:], bf16),
            pltpu.VMEM(w_down.shape[1:], bf16),
            pltpu.VMEM((n_ctx, rows, kv_width), bf16),
            pltpu.VMEM((n_ctx, rows, kv_width), bf16),
            pltpu.VMEM((kv_heads, group * rows, HEAD_WIDTH), f32),
            pltpu.VMEM((kv_heads, group * rows, HEAD_WIDTH), f32),
            pltpu.VMEM((kv_heads, group * rows, HEAD_WIDTH), f32),
            pltpu.VMEM((rows, features), bf16),
            pltpu.VMEM((live, features), bf16),
            pltpu.VMEM((n_ctx, live, features), bf16),
            pltpu.VMEM((n_ctx * slots, features), f32),
            pltpu.VMEM((n_ctx, live, features), bf16),
            pltpu.VMEM((n_ctx, live, features), bf16),
            pltpu.VMEM((n_ctx, slots, features), f32),
            pltpu.VMEM((n_ctx, slots, 128), f32),
            pltpu.VMEM((n_ctx, slots, 128), f32),
            pltpu.VMEM((n_ctx, slots, 128), f32),
            pltpu.VMEM((n_ep, dense, HEAD_WIDTH), bf16),
            pltpu.VMEM((n, dense, HEAD_WIDTH), bf16),
            pltpu.VMEM((members, features), f32),
            pltpu.VMEM((chunk_count, members, 2 * chunk_width), bf16),
            pltpu.VMEM((chunk_count, members, 2 * chunk_width), bf16),
            pltpu.VMEM((members, 128), bf16),
            pltpu.VMEM((members, 128), bf16),
            pltpu.VMEM((members, hidden_width), bf16),
            pltpu.VMEM((n, dense, HEAD_WIDTH), bf16),
            pltpu.VMEM((n, dense, HEAD_WIDTH), bf16),
            pltpu.VMEM((slots, features), f32),
            dma((3,)),
            dma((5,)),
            dma((n_ctx, 4)),
            dma((n_ctx, 4)),
            dma((n,)),
            dma((n,)),
            dma((chunk_count,)),
            dma((chunk_count,)),
            dma((2,)),
            dma((n,)),
            dma((n,)),
            dma((n_ctx,)),
            dma((n_ctx,)),
            dma((n_ctx,)),
            dma((n_ctx,)),
            dma((n_ctx,)),
            dma((n_ctx,)),
        ],
        compiler_params=pltpu.CompilerParams(
            collective_id=0, has_side_effects=True, vmem_limit_bytes=60 * 1024 * 1024
        ),
    )(
        expert_ids.reshape(1, rows), router.reshape(1, features), queries, keys, values,
        w_gate, w_up, w_down,
    )


def solution(mesh):
    placed = (
        P(("groups", "ep"), "ctx", "tp"),
        P(("groups", "ep"), "ctx", "tp"),
        P(("groups", "ep"), "ctx", "tp"),
        P(("groups", "ep"), "ctx", None),
        P("tp", "ep"),
        P("ep", "tp", "ctx"),
        P("ep", "tp", "ctx"),
        P("ep", "ctx", "tp"),
    )
    return jax.shard_map(
        shards,
        mesh=mesh,
        in_specs=placed,
        out_specs=P(("groups", "ep"), "ctx", "tp"),
        check_vma=False,
    )
```

```python
import functools
import math

import jax
import jax.numpy as jnp
from jax import lax
from jax.experimental import pallas as pl
from jax.experimental.pallas import tpu as pltpu
from jax.sharding import PartitionSpec as P

HEAD_WIDTH = 128
CAP = 2
MESH = pl.DeviceIdType.MESH
MASKED = -1e30
EXP2_SCALE = HEAD_WIDTH ** (-0.5) * math.log2(math.e)
scope = jax.named_scope


def tiles_of(width, tile):
    tile = min(width, tile)
    return [(start, min(tile, width - start)) for start in range(0, width, tile)]


def padded(count, tile=8):
    return -(-count // tile) * tile


def each(count, body):
    if count <= 8:
        for index in range(count):
            body(index)
    else:
        pl.loop(0, count)(body)


def kernel(
    n_ctx, n_ep, n_tp,
    ids_hbm, router_hbm, q_hbm, k_hbm, v_hbm, wg_hbm, wu_hbm, wd_hbm,
    out_ref,
    ids_ref, router_ref, q_ref, wg, wu, wd, kv, acc, row_max, totals, att,
    q_own, q_out, q_in, q_all, part_out, part_got, part_all, lse_out, lse_in, lse_all,
    out_rows, in_rows,
    members_a, part_a, part_in_a, score_a, score_in_a, hidden_a,
    members_b, part_b, part_in_b, score_b, score_in_b, hidden_b,
    down_out, down_in, returned,
    in_sem, own_sem, w_sem, kv_send, kv_recv, row_send, row_recv,
    a_send, a_recv, a_score, b_send, b_recv, b_score,
    down_send, down_recv, q_send, q_recv, back_send, back_recv, lse_send, lse_recv,
):
    ctx = lax.axis_index("ctx")
    ep = lax.axis_index("ep")
    tp = lax.axis_index("tp")
    n = n_ctx * n_ep
    me = ep * n_ctx + ctx
    last = n_ctx - 1
    rows, features = q_ref.shape
    kv_heads = kv.shape[1]
    places = features // HEAD_WIDTH
    group = places // kv_heads
    slots = returned.shape[0]
    live = n_ep * CAP

    def lanes(place):
        return slice(place * HEAD_WIDTH, (place + 1) * HEAD_WIDTH)

    in_copies = [
        pltpu.make_async_copy(src, dst, in_sem.at[index])
        for index, (src, dst) in enumerate((
            (ids_hbm, ids_ref), (q_hbm.at[0], q_ref), (router_hbm, router_ref),
        ))
    ]
    own_copies = [
        pltpu.make_async_copy(
            src.at[0, :, lanes(head)], kv.at[ctx, head, which], own_sem.at[head, which]
        )
        for head in range(kv_heads)
        for which, src in enumerate((k_hbm, v_hbm))
    ]
    w_copies = [
        pltpu.make_async_copy(src.at[0], dst, w_sem.at[index])
        for index, (src, dst) in enumerate(((wg_hbm, wg), (wu_hbm, wu), (wd_hbm, wd)))
    ]
    for copy in in_copies[:2] + own_copies + in_copies[2:] + w_copies:
        copy.start()

    barrier = pltpu.get_barrier_semaphore()

    def greet(other):
        @pl.when(other != me)
        def _():
            pl.semaphore_signal(
                barrier, inc=1,
                device_id={"ep": other // n_ctx, "ctx": other % n_ctx},
                device_id_type=MESH,
            )

    each(n, greet)
    for step in range(1, n_tp):
        pl.semaphore_signal(
            barrier, inc=1, device_id={"tp": (tp + step) % n_tp}, device_id_type=MESH
        )

    def kv_copy(block, head):
        return pltpu.make_async_remote_copy(
            src_ref=kv.at[block, head], dst_ref=kv.at[block, head],
            send_sem=kv_send.at[block, head], recv_sem=kv_recv.at[block, head],
            device_id={"ctx": ctx + 1}, device_id_type=MESH,
        )

    def push_own(heads):
        @pl.when(ctx < last)
        def _():
            for head in heads:
                kv_copy(ctx, head).start()

    def relay(block, heads):
        @pl.when(block >= 0)
        def _():
            for head in heads:
                copy = kv_copy(block, head)
                copy.wait_recv()

                @pl.when(ctx < last)
                def _():
                    copy.start()

    def q_copy(source, target):
        return pltpu.make_async_remote_copy(
            src_ref=q_out, dst_ref=q_in.at[source],
            send_sem=q_send.at[target], recv_sem=q_recv.at[source],
            device_id={"ctx": target}, device_id_type=MESH,
        )

    def back_copies(source, target):
        return [
            pltpu.make_async_remote_copy(
                src_ref=out.at[target], dst_ref=into.at[source],
                send_sem=sent.at[target], recv_sem=got.at[source],
                device_id={"ctx": target}, device_id_type=MESH,
            )
            for out, into, sent, got in (
                (part_out, part_got, back_send, back_recv),
                (lse_out, lse_in, lse_send, lse_recv),
            )
        ]

    def to_index(other, out, into, sent, got, source):
        return pltpu.make_async_remote_copy(
            src_ref=out, dst_ref=into.at[source],
            send_sem=sent.at[other], recv_sem=got.at[source],
            device_id={"ep": other // n_ctx, "ctx": other % n_ctx}, device_id_type=MESH,
        )

    def row_copy(other, source):
        return to_index(other, out_rows.at[other // n_ctx], in_rows, row_send, row_recv, source)

    def down_copy(other, source):
        return to_index(other, down_out.at[other], down_in, down_send, down_recv, source)

    def lower(body):
        def one(other):
            @pl.when(other < ctx)
            def _():
                body(other)

        each(n_ctx, one)

    def upper(body):
        def one(step):
            other = last - step

            @pl.when(other > ctx)
            def _():
                body(other)

        each(n_ctx, one)

    def others(body):
        def one(other):
            @pl.when(other != me)
            def _():
                body(other)

        each(n, one)

    def first_owners(body):
        def one(expert):
            @pl.when(expert * n_ctx != me)
            def _():
                body(expert * n_ctx)

        each(n_ep, one)

    def later_owners(body):
        def one(other):
            @pl.when((other % n_ctx != 0) & (other != me))
            def _():
                body(other)

        each(n, one)

    with scope("a_pick"):
        in_copies[0].wait()
        ids = ids_ref[...]
        slot_row = lax.broadcasted_iota(jnp.int32, (slots, rows), 0)
        choose = jnp.where(ids == slot_row, 1.0, 0.0)
        below = lax.broadcasted_iota(jnp.int32, (rows, rows), 0)
        across = lax.broadcasted_iota(jnp.int32, (rows, rows), 1)
        strict = jnp.where(below < across, 1.0, 0.0).astype(jnp.bfloat16)
        earlier = jnp.dot(
            choose.astype(jnp.bfloat16), strict, preferred_element_type=jnp.float32
        )
        slot_index = jnp.sum(earlier * choose, axis=0, keepdims=True).astype(jnp.int32)
        target_row = jnp.where(ids < n_ep, ids * CAP + slot_index, -1)
        spread = jnp.where(target_row == slot_row, 1.0, 0.0).astype(jnp.bfloat16)
        lane_row = lax.broadcasted_iota(jnp.int32, (slots, rows), 1)
        row_place = jnp.sum(
            jnp.where(target_row == slot_row, lane_row, 0), axis=1, keepdims=True
        )
        in_copies[1].wait()
        for start, size in tiles_of(features, 512):
            picked = jnp.dot(
                spread, q_ref[:, start:start + size], preferred_element_type=jnp.float32
            )
            q_own[:, start:start + size] = picked
            q_out[:, start:start + size] = picked[:live].astype(jnp.bfloat16)

    def attend(source, tall, seen):
        raws = []
        for head in range(kv_heads):
            stacked = jnp.concatenate(
                [source[:, lanes(head * group + j)] for j in range(group)], axis=0
            ).astype(jnp.bfloat16)
            raw = lax.dot_general(
                stacked, kv[ctx, head, 0], (((1,), (1,)), ((), ())),
                preferred_element_type=jnp.float32,
            )
            raws.append(raw if seen is None else jnp.where(seen, raw, MASKED))
        tops = [jnp.max(raw, axis=1, keepdims=True) for raw in raws]
        weights = [jnp.exp2((raw - top) * EXP2_SCALE) for raw, top in zip(raws, tops)]
        sums = [jnp.sum(weight, axis=1, keepdims=True) for weight in weights]
        mixed = [
            jnp.dot(
                weight.astype(jnp.bfloat16), kv[ctx, head, 1],
                preferred_element_type=jnp.float32,
            ) / total
            for head, (weight, total) in enumerate(zip(weights, sums))
        ]
        columns = [top * EXP2_SCALE + jnp.log2(total) for top, total in zip(tops, sums)]
        head_lane = lax.broadcasted_iota(jnp.int32, (tall, 128), 1)
        lse = jnp.zeros((tall, 128), jnp.float32)
        for head in range(kv_heads):
            for j in range(group):
                lse = jnp.where(
                    head_lane == head * group + j, columns[head][j * tall:(j + 1) * tall], lse
                )
        return mixed, lse

    def own_part():
        key_lane = lax.broadcasted_iota(jnp.int32, (group * slots, rows), 1)
        seen = key_lane <= jnp.concatenate([row_place] * group, axis=0)
        mixed, lse = attend(q_own, slots, seen)
        lse_all[...] = jnp.full_like(lse_all, MASKED)
        lse_all[ctx] = lse
        for head in range(kv_heads):
            for j in range(group):
                part_all[ctx, :, lanes(head * group + j)] = mixed[head][
                    j * slots:(j + 1) * slots
                ]

    def put_row(place, picked):
        for expert in range(n_ep):
            out_rows[expert, place * CAP:(place + 1) * CAP] = picked[
                expert * CAP:(expert + 1) * CAP
            ].astype(jnp.bfloat16)

    def send_rows():
        others(lambda other: row_copy(other, me).start())
        in_rows[me] = out_rows[ep]

    part_all[...] = jnp.zeros_like(part_all)
    q_all[...] = jnp.zeros_like(q_all)

    @pl.when(ctx == 0)
    def _():
        with scope("b_own0"):
            for copy in own_copies:
                copy.wait()
            own_part()
            for place in range(places):
                put_row(place, part_all[0, :, lanes(place)])

    with scope("c_barrier"):
        pl.semaphore_wait(barrier, n - 1 + n_tp - 1)

    with scope("d_qsend"):
        lower(lambda other: q_copy(ctx, other).start())

    @pl.when(ctx == 0)
    def _():
        with scope("e_rows0"):
            send_rows()
            push_own(range(kv_heads - 1))

    @pl.when(ctx > 0)
    def _():
        with scope("f_own"):
            for copy in own_copies:
                copy.wait()
            push_own(range(kv_heads - 1))
            own_part()

    query_offset = lax.broadcasted_iota(jnp.int32, (rows, rows), 0)
    key_offset = lax.broadcasted_iota(jnp.int32, (rows, rows), 1)

    def scores(block, head):
        stacked = jnp.concatenate(
            [q_ref[:, lanes(head * group + j)] for j in range(group)], axis=0
        )
        return lax.dot_general(
            stacked, kv[block, head, 0], (((1,), (1,)), ((), ())),
            preferred_element_type=jnp.float32,
        )

    def mix(weights, block, head):
        return jnp.dot(
            weights.astype(jnp.bfloat16), kv[block, head, 1], preferred_element_type=jnp.float32
        )

    with scope("g_own_block"):
        visible = jnp.concatenate([query_offset >= key_offset] * group, axis=0)
        for head in range(kv_heads):
            raw = jnp.where(visible, scores(ctx, head), MASKED)
            top = jnp.broadcast_to(jnp.max(raw, axis=1, keepdims=True), raw.shape)
            weights = jnp.exp2((raw - top) * EXP2_SCALE)
            row_max[head] = top
            totals[head] = jnp.broadcast_to(
                jnp.sum(weights, axis=1, keepdims=True), weights.shape
            )
            acc[head] = mix(weights, ctx, head)

    def process(block, head):
        raw = scores(block, head)
        old_max = row_max[head]
        new_max = jnp.maximum(old_max, jnp.max(raw, axis=1, keepdims=True))
        factor = jnp.exp2((old_max - new_max) * EXP2_SCALE)
        weights = jnp.exp2((raw - new_max) * EXP2_SCALE)
        row_max[head] = new_max
        totals[head] = totals[head] * factor + jnp.sum(weights, axis=1, keepdims=True)
        acc[head] = acc[head] * factor + mix(weights, block, head)

    def process_block(step):
        @pl.when(ctx >= step)
        def _():
            for head in range(kv_heads):
                process(ctx - step, head)

    @pl.when(ctx < last)
    def _():
        with scope("h_qwait"):
            upper(lambda other: q_copy(other, other).wait_recv())
        with scope("i_qpart"):
            for other in range(n_ctx):
                @pl.when(other > ctx)
                def _():
                    q_all[other * live:(other + 1) * live, :] = q_in[other].astype(jnp.float32)

            tall = n_ctx * live
            mixed, lse = attend(q_all, tall, None)
            for other in range(n_ctx):
                lse_out[other, :live] = lse[other * live:(other + 1) * live]
                for place in range(places):
                    first = place % group * tall + other * live
                    part_out[other, :, lanes(place)] = mixed[place // group][
                        first:first + live
                    ].astype(jnp.bfloat16)

        with scope("j_give"):
            def give_back(other):
                for copy in back_copies(ctx, other):
                    copy.start()

            upper(give_back)
            push_own([kv_heads - 1])

    with scope("k_relay"):
        relay(ctx - 1, [0])

    peer = {"tp": n_tp - 1 - tp}

    def gate(indices, wide_ref, part, part_in, score, score_in, sent, got, score_sem):
        for at, index in enumerate(indices):
            dense = in_rows[index].astype(jnp.float32)
            for place in range(places):
                wide_ref[at * CAP:(at + 1) * CAP, lanes(place)] = dense[
                    place * CAP:(place + 1) * CAP
                ]
        wide = wide_ref[...]
        members = wide.astype(jnp.bfloat16)
        own_score = jnp.sum(wide * router_ref[...].astype(jnp.float32), axis=1, keepdims=True)
        score[...] = jnp.broadcast_to(own_score, score.shape).astype(jnp.bfloat16)
        copies = [pltpu.make_async_remote_copy(
            src_ref=score, dst_ref=score_in,
            send_sem=score_sem.at[0], recv_sem=score_sem.at[1],
            device_id=peer, device_id_type=MESH,
        )]
        copies[0].start()
        chunk_count, _, double_width = part.shape
        width = double_width // 2
        for chunk in range(chunk_count):
            span = slice(chunk * width, (chunk + 1) * width)
            for side, weight in enumerate((wg, wu)):
                part[chunk, :, side * width:(side + 1) * width] = jnp.dot(
                    members, weight[:, span], preferred_element_type=jnp.float32
                ).astype(jnp.bfloat16)
            copy = pltpu.make_async_remote_copy(
                src_ref=part.at[chunk], dst_ref=part_in.at[chunk],
                send_sem=sent.at[chunk], recv_sem=got.at[chunk],
                device_id=peer, device_id_type=MESH,
            )
            copy.start()
            copies.append(copy)
        return copies

    def activate(copies, part, part_in, score, score_in, hidden):
        copies[0].wait()
        gain = jax.nn.sigmoid(
            score[:, :1].astype(jnp.float32) + score_in[:, :1].astype(jnp.float32)
        )
        width = part.shape[2] // 2
        for chunk, copy in enumerate(copies[1:]):
            copy.wait()
            both = part[chunk].astype(jnp.float32) + part_in[chunk].astype(jnp.float32)
            gate_part = gain * both[:, :width]
            up_part = gain * both[:, width:]
            hidden[:, chunk * width:(chunk + 1) * width] = (
                gate_part * jax.nn.sigmoid(gate_part) * up_part
            ).astype(jnp.bfloat16)

    def down(indices, hidden):
        for start, size in tiles_of(features, 512):
            product = jnp.dot(
                hidden[...], wd[:, start:start + size], preferred_element_type=jnp.float32
            )
            for at, index in enumerate(indices):
                for place in range(start // HEAD_WIDTH, (start + size) // HEAD_WIDTH):
                    lane = place * HEAD_WIDTH - start
                    down_out[index, place * CAP:(place + 1) * CAP] = product[
                        at * CAP:(at + 1) * CAP, lane:lane + HEAD_WIDTH
                    ].astype(jnp.bfloat16)

    def keep_own():
        down_in[me] = down_out[me]

    first = [index for index in range(n) if index % n_ctx == 0]
    later = [index for index in range(n) if index % n_ctx != 0]
    exchange_a = (part_a, part_in_a, score_a, score_in_a)
    exchange_b = (part_b, part_in_b, score_b, score_in_b)

    with scope("l_rows_a"):
        in_copies[2].wait()
        w_copies[0].wait()
        w_copies[1].wait()
        first_owners(lambda other: row_copy(other, other).wait_recv())
    with scope("m_gate_a"):
        copies_a = gate(first, members_a, *exchange_a, a_send, a_recv, a_score)
    with scope("n_relay"):
        relay(ctx - 1, [1])

    @pl.when(ctx > 0)
    def _():
        with scope("o_takeback"):
            def take_back(other):
                for copy in back_copies(other, other):
                    copy.wait_recv()

            lower(take_back)
        with scope("p_combine"):
            for other in range(last):
                @pl.when(other < ctx)
                def _():
                    part_all[other, :live] = part_got[other].astype(jnp.float32)
                    lse_all[other, :live] = lse_in[other, :live]

            peak = jnp.max(lse_all[...], axis=0)
            shares = [jnp.exp2(lse_all[other] - peak) for other in range(n_ctx)]
            share_total = functools.reduce(jnp.add, shares)
            shares = [share / share_total for share in shares]
            for place in range(places):
                put_row(place, functools.reduce(jnp.add, [
                    shares[other][:, place:place + 1] * part_all[other, :, lanes(place)]
                    for other in range(n_ctx)
                ]))
        with scope("q_rows"):
            send_rows()

    with scope("r_relay"):
        relay(ctx - 1, range(2, kv_heads))
    with scope("s_down_a"):
        w_copies[2].wait()
        activate(copies_a, *exchange_a, hidden_a)
        down(first, hidden_a)
        first_owners(lambda other: down_copy(other, me).start())
        pl.when(ctx == 0)(keep_own)
    with scope("t_block1"):
        process_block(1)
    with scope("u_relay"):
        relay(ctx - 2, range(2))
    with scope("v_rows_b"):
        later_owners(lambda other: row_copy(other, other).wait_recv())
    with scope("w_gate_b"):
        copies_b = gate(later, members_b, *exchange_b, b_send, b_recv, b_score)
    with scope("x_relay"):
        relay(ctx - 2, range(2, kv_heads))
    with scope("xa_block2"):
        process_block(2)
    with scope("xb_down_b"):
        activate(copies_b, *exchange_b, hidden_b)
        down(later, hidden_b)
        later_owners(lambda other: down_copy(other, me).start())
        pl.when(ctx > 0)(keep_own)

    def visit(step, carry):
        @pl.when(ctx >= step)
        def _():
            for head in range(kv_heads):
                relay(ctx - step, [head])
                process(ctx - step, head)

        return carry

    with scope("xc_visit"):
        lax.fori_loop(3, n_ctx, visit, 0)

    with scope("xd_norm"):
        for head in range(kv_heads):
            normed = (acc[head] / totals[head]).astype(jnp.bfloat16)
            for j in range(group):
                att[:, lanes(head * group + j)] = normed[j * rows:(j + 1) * rows]
        returned[...] = jnp.zeros_like(returned)

    with scope("xe_sent"):
        others(lambda other: row_copy(other, me).wait_send())
        lower(lambda other: q_copy(ctx, other).wait_send())

        def sent_back(other):
            for copy in back_copies(ctx, other):
                copy.wait_send()

        upper(sent_back)

        def drain(step, carry):
            @pl.when((ctx < last) & (ctx >= step))
            def _():
                for head in range(kv_heads):
                    kv_copy(ctx - step, head).wait_send()

            return carry

        lax.fori_loop(0, n_ctx, drain, 0)

    with scope("xf_downwait"):
        others(lambda other: down_copy(other, other).wait_recv())
    with scope("xg_final"):
        for expert in range(n_ep):
            total = down_in[expert * n_ctx].astype(jnp.float32)
            for index in range(1, n_ctx):
                total = total + down_in[expert * n_ctx + index].astype(jnp.float32)
            total = total.astype(jnp.bfloat16).astype(jnp.float32)
            for place in range(places):
                returned[expert * CAP:(expert + 1) * CAP, lanes(place)] = total[
                    place * CAP:(place + 1) * CAP
                ]
        for start, size in tiles_of(features, 512):
            routed = lax.dot_general(
                spread, returned[:, start:start + size].astype(jnp.bfloat16),
                (((0,), (0,)), ((), ())), preferred_element_type=jnp.float32,
            )
            out_ref[0, :, start:start + size] = (
                att[:, start:start + size].astype(jnp.float32) + routed
            ).astype(jnp.bfloat16)
    others(lambda other: down_copy(other, me).wait_send())


def shards(queries, keys, values, expert_ids, router, w_gate, w_up, w_down):
    n_ctx, n_ep, n_tp = (lax.axis_size(axis) for axis in ("ctx", "ep", "tp"))
    n = n_ctx * n_ep
    _, rows, features = queries.shape
    kv_width = keys.shape[2]
    kv_heads = kv_width // HEAD_WIDTH
    group = features // kv_width
    hidden_width = w_gate.shape[2]
    chunk_width = min(hidden_width, 256)
    chunks = hidden_width // chunk_width
    dense = features // HEAD_WIDTH * CAP
    live = n_ep * CAP
    slots = padded(live)
    bf16, f32 = jnp.bfloat16, jnp.float32
    hbm = pl.BlockSpec(memory_space=pltpu.HBM)
    dma = pltpu.SemaphoreType.DMA

    def batch(count):
        return [
            pltpu.VMEM((count, features), f32),
            pltpu.VMEM((chunks, count, 2 * chunk_width), bf16),
            pltpu.VMEM((chunks, count, 2 * chunk_width), bf16),
            pltpu.VMEM((count, 128), bf16),
            pltpu.VMEM((count, 128), bf16),
            pltpu.VMEM((count, hidden_width), bf16),
        ]

    return pl.pallas_call(
        functools.partial(kernel, n_ctx, n_ep, n_tp),
        out_shape=pltpu.VMEM(queries.shape, bf16),
        in_specs=[hbm] * 8,
        out_specs=pl.BlockSpec(memory_space=pltpu.VMEM),
        scratch_shapes=[
            pltpu.VMEM((1, rows), jnp.int32),
            pltpu.VMEM((1, features), bf16),
            pltpu.VMEM((rows, features), bf16),
            pltpu.VMEM(w_gate.shape[1:], bf16),
            pltpu.VMEM(w_up.shape[1:], bf16),
            pltpu.VMEM(w_down.shape[1:], bf16),
            pltpu.VMEM((n_ctx, kv_heads, 2, rows, HEAD_WIDTH), bf16),
            pltpu.VMEM((kv_heads, group * rows, HEAD_WIDTH), f32),
            pltpu.VMEM((kv_heads, group * rows, HEAD_WIDTH), f32),
            pltpu.VMEM((kv_heads, group * rows, HEAD_WIDTH), f32),
            pltpu.VMEM((rows, features), bf16),
            pltpu.VMEM((slots, features), f32),
            pltpu.VMEM((live, features), bf16),
            pltpu.VMEM((n_ctx, live, features), bf16),
            pltpu.VMEM((n_ctx * live, features), f32),
            pltpu.VMEM((n_ctx, live, features), bf16),
            pltpu.VMEM((n_ctx, live, features), bf16),
            pltpu.VMEM((n_ctx, slots, features), f32),
            pltpu.VMEM((n_ctx, slots, 128), f32),
            pltpu.VMEM((n_ctx, slots, 128), f32),
            pltpu.VMEM((n_ctx, slots, 128), f32),
            pltpu.VMEM((n_ep, dense, HEAD_WIDTH), bf16),
            pltpu.VMEM((n, dense, HEAD_WIDTH), bf16),
            *batch(n_ep * CAP),
            *batch((n - n_ep) * CAP),
            pltpu.VMEM((n, dense, HEAD_WIDTH), bf16),
            pltpu.VMEM((n, dense, HEAD_WIDTH), bf16),
            pltpu.VMEM((slots, features), f32),
            dma((3,)),
            dma((kv_heads, 2)),
            dma((3,)),
            dma((n_ctx, kv_heads)),
            dma((n_ctx, kv_heads)),
            dma((n,)),
            dma((n,)),
            dma((chunks,)),
            dma((chunks,)),
            dma((2,)),
            dma((chunks,)),
            dma((chunks,)),
            dma((2,)),
            dma((n,)),
            dma((n,)),
            dma((n_ctx,)),
            dma((n_ctx,)),
            dma((n_ctx,)),
            dma((n_ctx,)),
            dma((n_ctx,)),
            dma((n_ctx,)),
        ],
        compiler_params=pltpu.CompilerParams(
            collective_id=0, has_side_effects=True, vmem_limit_bytes=60 * 1024 * 1024
        ),
    )(
        expert_ids.reshape(1, rows), router.reshape(1, features), queries, keys, values,
        w_gate, w_up, w_down,
    )


def solution(mesh):
    placed = (
        P(("groups", "ep"), "ctx", "tp"),
        P(("groups", "ep"), "ctx", "tp"),
        P(("groups", "ep"), "ctx", "tp"),
        P(("groups", "ep"), "ctx", None),
        P("tp", "ep"),
        P("ep", "tp", "ctx"),
        P("ep", "tp", "ctx"),
        P("ep", "ctx", "tp"),
    )
    return jax.shard_map(
        shards,
        mesh=mesh,
        in_specs=placed,
        out_specs=P(("groups", "ep"), "ctx", "tp"),
        check_vma=False,
    )
```

```python
import functools
import math

import jax
import jax.numpy as jnp
from jax import lax
from jax.experimental import pallas as pl
from jax.experimental.pallas import tpu as pltpu
from jax.sharding import PartitionSpec as P

HEAD_WIDTH = 128
CAP = 2
MESH = pl.DeviceIdType.MESH
MASKED = -1e30
EXP2_SCALE = HEAD_WIDTH ** (-0.5) * math.log2(math.e)
scope = jax.named_scope


def tiles_of(width, tile):
    tile = min(width, tile)
    return [(start, min(tile, width - start)) for start in range(0, width, tile)]


def padded(count, tile=8):
    return -(-count // tile) * tile


def each(count, body):
    if count <= 8:
        for index in range(count):
            body(index)
    else:
        pl.loop(0, count)(body)


def kernel(
    n_ctx, n_ep, n_tp,
    ids_hbm, router_hbm, q_hbm, k_hbm, v_hbm, wg_hbm, wu_hbm, wd_hbm,
    out_ref,
    ids_ref, router_ref, q_ref, wgu, wd, kv, acc, row_max, totals, att,
    q_own, q_out, q_in, q_pad, part_out, part_got, part_all, lse_out, lse_in, lse_all,
    out_rows, in_rows,
    members_a, part_a, part_in_a, hidden_a,
    members_b, part_b, part_in_b, hidden_b,
    down_out, down_in, returned,
    in_sem, own_sem, w_sem, kv_send, kv_recv, row_send, row_recv,
    a_send, a_recv, b_send, b_recv,
    down_send, down_recv, q_send, q_recv, back_send, back_recv, lse_send, lse_recv,
):
    ctx = lax.axis_index("ctx")
    ep = lax.axis_index("ep")
    tp = lax.axis_index("tp")
    n = n_ctx * n_ep
    me = ep * n_ctx + ctx
    last = n_ctx - 1
    rows, features = q_ref.shape
    kv_heads = kv.shape[1]
    places = features // HEAD_WIDTH
    group = places // kv_heads
    slots = returned.shape[0]
    live = n_ep * CAP

    def lanes(place):
        return slice(place * HEAD_WIDTH, (place + 1) * HEAD_WIDTH)

    in_copies = [
        pltpu.make_async_copy(src, dst, in_sem.at[index])
        for index, (src, dst) in enumerate((
            (ids_hbm, ids_ref), (q_hbm.at[0], q_ref), (router_hbm, router_ref),
        ))
    ]
    own_copies = [
        pltpu.make_async_copy(
            src.at[0, :, lanes(head)], kv.at[ctx, head, which], own_sem
        )
        for head in range(kv_heads)
        for which, src in enumerate((k_hbm, v_hbm))
    ]
    w_copies = [
        pltpu.make_async_copy(src.at[0], dst, sem)
        for src, dst, sem in (
            (wg_hbm, wgu.at[0], w_sem.at[0]), (wu_hbm, wgu.at[1], w_sem.at[0]),
            (wd_hbm, wd, w_sem.at[1]),
        )
    ]
    for copy in in_copies[:2] + own_copies + in_copies[2:]:
        copy.start()

    barrier = pltpu.get_barrier_semaphore()

    def greet(other):
        @pl.when(other != me)
        def _():
            pl.semaphore_signal(
                barrier, inc=1,
                device_id={"ep": other // n_ctx, "ctx": other % n_ctx},
                device_id_type=MESH,
            )

    each(n, greet)
    for step in range(1, n_tp):
        pl.semaphore_signal(
            barrier, inc=1, device_id={"tp": (tp + step) % n_tp}, device_id_type=MESH
        )

    peer = {"tp": n_tp - 1 - tp}

    def settled(ref, sem):
        return pltpu.make_async_remote_copy(
            src_ref=ref, dst_ref=ref, send_sem=sem, recv_sem=sem,
            device_id=peer, device_id_type=MESH,
        )

    def by_ctx(body):
        for index in range(n_ctx):
            pl.when(ctx == index)(functools.partial(body, index))

    def kv_copy(block, head):
        return pltpu.make_async_remote_copy(
            src_ref=kv.at[block, head], dst_ref=kv.at[block, head],
            send_sem=kv_send, recv_sem=kv_recv.at[block, head],
            device_id={"ctx": ctx + 1}, device_id_type=MESH,
        )

    def push_own(heads):
        @pl.when(ctx < last)
        def _():
            for head in heads:
                kv_copy(ctx, head).start()

    def relay(block, heads):
        @pl.when(block >= 0)
        def _():
            for head in heads:
                copy = kv_copy(block, head)
                copy.wait_recv()

                @pl.when(ctx < last)
                def _():
                    copy.start()

    def q_copy(source, target):
        return pltpu.make_async_remote_copy(
            src_ref=q_out, dst_ref=q_in.at[source],
            send_sem=q_send, recv_sem=q_recv.at[source],
            device_id={"ctx": target}, device_id_type=MESH,
        )

    def back_copies(source, target):
        return [
            pltpu.make_async_remote_copy(
                src_ref=out.at[target], dst_ref=into.at[source],
                send_sem=sent, recv_sem=got,
                device_id={"ctx": target}, device_id_type=MESH,
            )
            for out, into, sent, got in (
                (part_out, part_got, back_send, back_recv),
                (lse_out, lse_in, lse_send, lse_recv),
            )
        ]

    def to_index(other, out, into, sent, got, source):
        return pltpu.make_async_remote_copy(
            src_ref=out, dst_ref=into.at[source],
            send_sem=sent, recv_sem=got,
            device_id={"ep": other // n_ctx, "ctx": other % n_ctx}, device_id_type=MESH,
        )

    def row_copy(other, source):
        got = row_recv.at[jnp.where(ctx == 0, 0, 1)]
        return to_index(other, out_rows.at[other // n_ctx], in_rows, row_send, got, source)

    def down_copy(other, source):
        return to_index(other, down_out.at[other], down_in, down_send, down_recv, source)

    def lower(body):
        def one(other):
            @pl.when(other < ctx)
            def _():
                body(other)

        each(n_ctx, one)

    def upper(body):
        def one(step):
            other = last - step

            @pl.when(other > ctx)
            def _():
                body(other)

        each(n_ctx, one)

    def others(body):
        def one(other):
            @pl.when(other != me)
            def _():
                body(other)

        each(n, one)

    def first_owners(body):
        def one(expert):
            @pl.when(expert * n_ctx != me)
            def _():
                body(expert * n_ctx)

        each(n_ep, one)

    def later_owners(body):
        def one(other):
            @pl.when((other % n_ctx != 0) & (other != me))
            def _():
                body(other)

        each(n, one)

    with scope("a_ids"):
        in_copies[0].wait()
    with scope("a_pick"):
        ids = ids_ref[...]
        slot_row = lax.broadcasted_iota(jnp.int32, (slots, rows), 0)
        choose = jnp.where(ids == slot_row, 1.0, 0.0)
        below = lax.broadcasted_iota(jnp.int32, (rows, rows), 0)
        across = lax.broadcasted_iota(jnp.int32, (rows, rows), 1)
        strict = jnp.where(below < across, 1.0, 0.0).astype(jnp.bfloat16)
        earlier = jnp.dot(
            choose.astype(jnp.bfloat16), strict, preferred_element_type=jnp.float32
        )
        slot_index = jnp.sum(earlier * choose, axis=0, keepdims=True).astype(jnp.int32)
        target_row = jnp.where(ids < n_ep, ids * CAP + slot_index, -1)
        spread = jnp.where(target_row == slot_row, 1.0, 0.0).astype(jnp.bfloat16)
        lane_row = lax.broadcasted_iota(jnp.int32, (slots, rows), 1)
        row_place = jnp.sum(
            jnp.where(target_row == slot_row, lane_row, 0), axis=1, keepdims=True
        )
        in_copies[1].wait()
        for copy in w_copies:
            copy.start()
        for start, size in tiles_of(features, 512):
            picked = jnp.dot(
                spread, q_ref[:, start:start + size], preferred_element_type=jnp.float32
            )
            q_own[:, start:start + size] = picked
            q_out[:, start:start + size] = picked[:live].astype(jnp.bfloat16)

    def attend(source, tall, seen):
        raws = []
        for head in range(kv_heads):
            stacked = jnp.concatenate(
                [source[:, lanes(head * group + j)] for j in range(group)], axis=0
            ).astype(jnp.bfloat16)
            raw = lax.dot_general(
                stacked, kv[ctx, head, 0], (((1,), (1,)), ((), ())),
                preferred_element_type=jnp.float32,
            )
            raws.append(raw if seen is None else jnp.where(seen, raw, MASKED))
        tops = [jnp.max(raw, axis=1, keepdims=True) for raw in raws]
        weights = [jnp.exp2((raw - top) * EXP2_SCALE) for raw, top in zip(raws, tops)]
        sums = [jnp.sum(weight, axis=1, keepdims=True) for weight in weights]
        mixed = [
            jnp.dot(
                weight.astype(jnp.bfloat16), kv[ctx, head, 1],
                preferred_element_type=jnp.float32,
            ) / total
            for head, (weight, total) in enumerate(zip(weights, sums))
        ]
        columns = [top * EXP2_SCALE + jnp.log2(total) for top, total in zip(tops, sums)]
        head_lane = lax.broadcasted_iota(jnp.int32, (tall, 128), 1)
        lse = jnp.zeros((tall, 128), jnp.float32)
        for head in range(kv_heads):
            for j in range(group):
                lse = jnp.where(
                    head_lane == head * group + j, columns[head][j * tall:(j + 1) * tall], lse
                )
        return mixed, lse

    def own_landed():
        pltpu.make_async_copy(kv.at[ctx], kv.at[ctx], own_sem).wait()

    def own_part():
        key_lane = lax.broadcasted_iota(jnp.int32, (group * slots, rows), 1)
        seen = key_lane <= jnp.concatenate([row_place] * group, axis=0)
        mixed, lse = attend(q_own, slots, seen)
        lse_all[...] = jnp.full_like(lse_all, MASKED)
        lse_all[ctx] = lse
        for head in range(kv_heads):
            for j in range(group):
                part_all[ctx, :, lanes(head * group + j)] = mixed[head][
                    j * slots:(j + 1) * slots
                ]

    def put_row(place, picked):
        for expert in range(n_ep):
            out_rows[expert, place * CAP:(place + 1) * CAP] = picked[
                expert * CAP:(expert + 1) * CAP
            ].astype(jnp.bfloat16)

    def send_rows():
        others(lambda other: row_copy(other, me).start())
        in_rows[me] = out_rows[ep]

    part_all[...] = jnp.zeros_like(part_all)
    q_pad[...] = jnp.zeros_like(q_pad)

    @pl.when(ctx == 0)
    def _():
        with scope("b_own0"):
            own_landed()
            own_part()
            for place in range(places):
                put_row(place, part_all[0, :, lanes(place)])

    with scope("c_barrier"):
        pl.semaphore_wait(barrier, n - 1 + n_tp - 1)

    with scope("d_qsend"):
        lower(lambda other: q_copy(ctx, other).start())

    @pl.when(ctx == 0)
    def _():
        with scope("e_rows0"):
            send_rows()
            push_own(range(2))

    @pl.when(ctx > 0)
    def _():
        with scope("f_own"):
            own_landed()
            push_own(range(kv_heads - 1))
            own_part()

    query_offset = lax.broadcasted_iota(jnp.int32, (rows, rows), 0)
    key_offset = lax.broadcasted_iota(jnp.int32, (rows, rows), 1)

    def scores(block, head):
        stacked = jnp.concatenate(
            [q_ref[:, lanes(head * group + j)] for j in range(group)], axis=0
        )
        return lax.dot_general(
            stacked, kv[block, head, 0], (((1,), (1,)), ((), ())),
            preferred_element_type=jnp.float32,
        )

    def mix(weights, block, head):
        return jnp.dot(
            weights.astype(jnp.bfloat16), kv[block, head, 1], preferred_element_type=jnp.float32
        )

    with scope("g_own_block"):
        visible = jnp.concatenate([query_offset >= key_offset] * group, axis=0)
        for head in range(kv_heads):
            raw = jnp.where(visible, scores(ctx, head), MASKED)
            top = jnp.broadcast_to(jnp.max(raw, axis=1, keepdims=True), raw.shape)
            weights = jnp.exp2((raw - top) * EXP2_SCALE)
            row_max[head] = top
            totals[head] = jnp.broadcast_to(
                jnp.sum(weights, axis=1, keepdims=True), weights.shape
            )
            acc[head] = mix(weights, ctx, head)

    def process(block, head):
        raw = scores(block, head)
        old_max = row_max[head]
        new_max = jnp.maximum(old_max, jnp.max(raw, axis=1, keepdims=True))
        factor = jnp.exp2((old_max - new_max) * EXP2_SCALE)
        weights = jnp.exp2((raw - new_max) * EXP2_SCALE)
        row_max[head] = new_max
        totals[head] = totals[head] * factor + jnp.sum(weights, axis=1, keepdims=True)
        acc[head] = acc[head] * factor + mix(weights, block, head)

    def process_block(step):
        @pl.when(ctx >= step)
        def _():
            for head in range(kv_heads):
                process(ctx - step, head)

    @pl.when(ctx < last)
    def _():
        def answer(step, carry):
            other = ctx + step

            @pl.when(other <= last)
            def _():
                with scope("h_qwait"):
                    q_copy(other, other).wait_recv()
                with scope("i_qpart"):
                    q_pad[:live] = q_in[other].astype(jnp.float32)
                    mixed, lse = attend(q_pad, slots, None)
                    lse_out[other] = lse[:live]
                    for place in range(places):
                        first = place % group * slots
                        part_out[other, :, lanes(place)] = mixed[place // group][
                            first:first + live
                        ].astype(jnp.bfloat16)
                    for copy in back_copies(ctx, other):
                        copy.start()

            return carry

        lax.fori_loop(1, n_ctx, answer, 0)
        pl.when(ctx == 0)(lambda: push_own(range(2, kv_heads)))
        pl.when(ctx > 0)(lambda: push_own([kv_heads - 1]))

    with scope("k_relay"):
        pl.when(ctx > 1)(lambda: relay(ctx - 1, [0]))

    def gate(indices, wide_ref, part, part_in, sent, got):
        for at, index in enumerate(indices):
            dense = in_rows[index].astype(jnp.float32)
            for place in range(places):
                wide_ref[at * CAP:(at + 1) * CAP, lanes(place)] = dense[
                    place * CAP:(place + 1) * CAP
                ]
        wide = wide_ref[...]
        members = wide.astype(jnp.bfloat16)
        own_score = jnp.sum(wide * router_ref[...].astype(jnp.float32), axis=1, keepdims=True)
        chunks, _, double_width = part.shape
        width = double_width // 2
        for chunk in range(chunks):
            if chunk == 0:
                part[0] = jnp.broadcast_to(own_score, part.shape[1:]).astype(jnp.bfloat16)
            else:
                span = slice((chunk - 1) * width, chunk * width)
                for side in range(2):
                    part[chunk, :, side * width:(side + 1) * width] = jnp.dot(
                        members, wgu[side, :, span], preferred_element_type=jnp.float32
                    ).astype(jnp.bfloat16)
            which = chunk // (chunks - 1)
            pltpu.make_async_remote_copy(
                src_ref=part.at[chunk], dst_ref=part_in.at[chunk],
                send_sem=sent, recv_sem=got.at[which],
                device_id=peer, device_id_type=MESH,
            ).start()

    def activate(part, part_in, sent, got, hidden):
        chunks = part.shape[0]
        width = part.shape[2] // 2
        settled(part_in.at[pl.ds(0, chunks - 1)], got.at[0]).wait_recv()
        gain = jax.nn.sigmoid(
            part[0, :, :1].astype(jnp.float32) + part_in[0, :, :1].astype(jnp.float32)
        )
        for chunk in range(1, chunks):
            if chunk == chunks - 1:
                settled(part_in.at[chunk], got.at[1]).wait_recv()
            both = part[chunk].astype(jnp.float32) + part_in[chunk].astype(jnp.float32)
            gate_part = gain * both[:, :width]
            up_part = gain * both[:, width:]
            hidden[:, (chunk - 1) * width:chunk * width] = (
                gate_part * jax.nn.sigmoid(gate_part) * up_part
            ).astype(jnp.bfloat16)

    def down(indices, hidden):
        for start, size in tiles_of(features, 512):
            product = jnp.dot(
                hidden[...], wd[:, start:start + size], preferred_element_type=jnp.float32
            )
            for at, index in enumerate(indices):
                for place in range(start // HEAD_WIDTH, (start + size) // HEAD_WIDTH):
                    lane = place * HEAD_WIDTH - start
                    down_out[index, place * CAP:(place + 1) * CAP] = product[
                        at * CAP:(at + 1) * CAP, lane:lane + HEAD_WIDTH
                    ].astype(jnp.bfloat16)

    def keep_own():
        down_in[me] = down_out[me]

    first = [index for index in range(n) if index % n_ctx == 0]
    later = [index for index in range(n) if index % n_ctx != 0]
    exchange_a = (part_a, part_in_a, a_send, a_recv)
    exchange_b = (part_b, part_in_b, b_send, b_recv)

    with scope("l_rows_a"):
        in_copies[2].wait()
        pltpu.make_async_copy(wgu, wgu, w_sem.at[0]).wait()

        @pl.when(ctx == 0)
        def _():
            if n_ep > 1:
                settled(in_rows.at[pl.ds(0, n_ep - 1)], row_recv.at[0]).wait_recv()

        @pl.when(ctx > 0)
        def _():
            settled(in_rows.at[pl.ds(0, n_ep)], row_recv.at[0]).wait_recv()
    with scope("m_gate_a"):
        gate(first, members_a, *exchange_a)
    with scope("n_relay"):
        pl.when(ctx == 1)(lambda: relay(ctx - 1, [0]))
        pl.when(ctx > 1)(lambda: relay(ctx - 1, range(1, kv_heads - 1)))

    @pl.when(ctx > 0)
    def _():
        with scope("o_takeback"):
            def take_back(count):
                if count:
                    settled(part_got.at[pl.ds(0, count)], back_recv).wait_recv()
                    settled(lse_in.at[pl.ds(0, count)], lse_recv).wait_recv()

            by_ctx(take_back)
        with scope("p_combine"):
            for other in range(last):
                @pl.when(other < ctx)
                def _():
                    part_all[other, :live] = part_got[other].astype(jnp.float32)
                    lse_all[other, :live] = lse_in[other]

            peak = jnp.max(lse_all[...], axis=0)
            shares = [jnp.exp2(lse_all[other] - peak) for other in range(n_ctx)]
            share_total = functools.reduce(jnp.add, shares)
            shares = [share / share_total for share in shares]
            for place in range(places):
                put_row(place, functools.reduce(jnp.add, [
                    shares[other][:, place:place + 1] * part_all[other, :, lanes(place)]
                    for other in range(n_ctx)
                ]))
        with scope("q_rows"):
            send_rows()

    with scope("r_relay"):
        pl.when(ctx == 1)(lambda: relay(ctx - 1, range(1, kv_heads)))
        pl.when(ctx > 1)(lambda: relay(ctx - 1, [kv_heads - 1]))
    with scope("s_down_a"):
        w_copies[2].wait()
        activate(*exchange_a, hidden_a)
        down(first, hidden_a)
        first_owners(lambda other: down_copy(other, me).start())
        pl.when(ctx == 0)(keep_own)
    with scope("t_block1"):
        process_block(1)
    with scope("u_relay"):
        relay(ctx - 2, range(2))
    with scope("v_rows_b"):
        @pl.when(ctx == 0)
        def _():
            settled(in_rows.at[pl.ds(0, n - n_ep)], row_recv.at[1]).wait_recv()

        @pl.when(ctx > 0)
        def _():
            settled(in_rows.at[pl.ds(0, n - n_ep - 1)], row_recv.at[1]).wait_recv()

    with scope("w_gate_b"):
        gate(later, members_b, *exchange_b)
    with scope("x_relay"):
        relay(ctx - 2, range(2, kv_heads))
    with scope("xa_block2"):
        process_block(2)
    with scope("xb_down_b"):
        activate(*exchange_b, hidden_b)
        down(later, hidden_b)
        later_owners(lambda other: down_copy(other, me).start())
        pl.when(ctx > 0)(keep_own)

    def visit(step, carry):
        @pl.when(ctx >= step)
        def _():
            for head in range(kv_heads):
                relay(ctx - step, [head])
                process(ctx - step, head)

        return carry

    with scope("xc_visit"):
        lax.fori_loop(3, n_ctx, visit, 0)

    with scope("xd_norm"):
        for head in range(kv_heads):
            normed = (acc[head] / totals[head]).astype(jnp.bfloat16)
            for j in range(group):
                att[:, lanes(head * group + j)] = normed[j * rows:(j + 1) * rows]
        returned[...] = jnp.zeros_like(returned)

    with scope("xe_sent"):
        settled(in_rows.at[pl.ds(0, n - 1)], row_send).wait_send()
        settled(part_a, a_send).wait_send()
        settled(part_b, b_send).wait_send()

        def drain(index):
            if index:
                settled(q_in.at[pl.ds(0, index)], q_send).wait_send()
            if index < last:
                settled(part_out.at[pl.ds(0, last - index)], back_send).wait_send()
                settled(lse_out.at[pl.ds(0, last - index)], lse_send).wait_send()
                settled(kv.at[pl.ds(0, index + 1)], kv_send).wait_send()

        by_ctx(drain)

    with scope("xf_downwait"):
        settled(down_in.at[pl.ds(0, n - 1)], down_recv).wait_recv()
    with scope("xg_final"):
        for expert in range(n_ep):
            total = down_in[expert * n_ctx].astype(jnp.float32)
            for index in range(1, n_ctx):
                total = total + down_in[expert * n_ctx + index].astype(jnp.float32)
            total = total.astype(jnp.bfloat16).astype(jnp.float32)
            for place in range(places):
                returned[expert * CAP:(expert + 1) * CAP, lanes(place)] = total[
                    place * CAP:(place + 1) * CAP
                ]
        for start, size in tiles_of(features, 512):
            routed = lax.dot_general(
                spread, returned[:, start:start + size].astype(jnp.bfloat16),
                (((0,), (0,)), ((), ())), preferred_element_type=jnp.float32,
            )
            out_ref[0, :, start:start + size] = (
                att[:, start:start + size].astype(jnp.float32) + routed
            ).astype(jnp.bfloat16)
    with scope("xh_sent"):
        settled(down_out.at[pl.ds(0, n - 1)], down_send).wait_send()


def shards(queries, keys, values, expert_ids, router, w_gate, w_up, w_down):
    n_ctx, n_ep, n_tp = (lax.axis_size(axis) for axis in ("ctx", "ep", "tp"))
    n = n_ctx * n_ep
    _, rows, features = queries.shape
    kv_width = keys.shape[2]
    kv_heads = kv_width // HEAD_WIDTH
    group = features // kv_width
    hidden_width = w_gate.shape[2]
    chunk_width = min(hidden_width, 256)
    chunks = hidden_width // chunk_width
    dense = features // HEAD_WIDTH * CAP
    live = n_ep * CAP
    slots = padded(live)
    bf16, f32 = jnp.bfloat16, jnp.float32
    hbm = pl.BlockSpec(memory_space=pltpu.HBM)
    dma = pltpu.SemaphoreType.DMA

    def batch(count):
        return [
            pltpu.VMEM((count, features), f32),
            pltpu.VMEM((chunks + 1, count, 2 * chunk_width), bf16),
            pltpu.VMEM((chunks + 1, count, 2 * chunk_width), bf16),
            pltpu.VMEM((count, hidden_width), bf16),
        ]

    return pl.pallas_call(
        functools.partial(kernel, n_ctx, n_ep, n_tp),
        out_shape=pltpu.VMEM(queries.shape, bf16),
        in_specs=[hbm] * 8,
        out_specs=pl.BlockSpec(memory_space=pltpu.VMEM),
        scratch_shapes=[
            pltpu.VMEM((1, rows), jnp.int32),
            pltpu.VMEM((1, features), bf16),
            pltpu.VMEM((rows, features), bf16),
            pltpu.VMEM((2, *w_gate.shape[1:]), bf16),
            pltpu.VMEM(w_down.shape[1:], bf16),
            pltpu.VMEM((n_ctx, kv_heads, 2, rows, HEAD_WIDTH), bf16),
            pltpu.VMEM((kv_heads, group * rows, HEAD_WIDTH), f32),
            pltpu.VMEM((kv_heads, group * rows, HEAD_WIDTH), f32),
            pltpu.VMEM((kv_heads, group * rows, HEAD_WIDTH), f32),
            pltpu.VMEM((rows, features), bf16),
            pltpu.VMEM((slots, features), f32),
            pltpu.VMEM((live, features), bf16),
            pltpu.VMEM((n_ctx, live, features), bf16),
            pltpu.VMEM((slots, features), f32),
            pltpu.VMEM((n_ctx, live, features), bf16),
            pltpu.VMEM((n_ctx, live, features), bf16),
            pltpu.VMEM((n_ctx, slots, features), f32),
            pltpu.VMEM((n_ctx, live, 128), f32),
            pltpu.VMEM((n_ctx, live, 128), f32),
            pltpu.VMEM((n_ctx, slots, 128), f32),
            pltpu.VMEM((n_ep, dense, HEAD_WIDTH), bf16),
            pltpu.VMEM((n, dense, HEAD_WIDTH), bf16),
            *batch(n_ep * CAP),
            *batch((n - n_ep) * CAP),
            pltpu.VMEM((n, dense, HEAD_WIDTH), bf16),
            pltpu.VMEM((n, dense, HEAD_WIDTH), bf16),
            pltpu.VMEM((slots, features), f32),
            dma((3,)),
            dma,
            dma((2,)),
            dma,
            dma((n_ctx - 1, kv_heads)),
            dma,
            dma((2,)),
            dma,
            dma((2,)),
            dma,
            dma((2,)),
            dma,
            dma,
            dma,
            dma((n_ctx,)),
            *[dma] * 4,
        ],
        compiler_params=pltpu.CompilerParams(
            collective_id=0, has_side_effects=True, vmem_limit_bytes=60 * 1024 * 1024
        ),
    )(
        expert_ids.reshape(1, rows), router.reshape(1, features), queries, keys, values,
        w_gate, w_up, w_down,
    )


def solution(mesh):
    placed = (
        P(("groups", "ep"), "ctx", "tp"),
        P(("groups", "ep"), "ctx", "tp"),
        P(("groups", "ep"), "ctx", "tp"),
        P(("groups", "ep"), "ctx", None),
        P("tp", "ep"),
        P("ep", "tp", "ctx"),
        P("ep", "tp", "ctx"),
        P("ep", "ctx", "tp"),
    )
    return jax.shard_map(
        shards,
        mesh=mesh,
        in_specs=placed,
        out_specs=P(("groups", "ep"), "ctx", "tp"),
        check_vma=False,
    )
```

```python
import functools
import math

import jax
import jax.numpy as jnp
from jax import lax
from jax.experimental import pallas as pl
from jax.experimental.pallas import tpu as pltpu
from jax.sharding import PartitionSpec as P

HEAD_WIDTH = 128
CAP = 2
MESH = pl.DeviceIdType.MESH
MASKED = -1e30
EXP2_SCALE = HEAD_WIDTH ** (-0.5) * math.log2(math.e)
scope = jax.named_scope


def tiles_of(width, tile):
    tile = min(width, tile)
    return [(start, min(tile, width - start)) for start in range(0, width, tile)]


def padded(count, tile=8):
    return -(-count // tile) * tile


def each(count, body):
    if count <= 8:
        for index in range(count):
            body(index)
    else:
        pl.loop(0, count)(body)


def kernel(
    n_ctx, n_ep, n_tp,
    ids_hbm, router_hbm, q_hbm, k_hbm, v_hbm, wg_hbm, wu_hbm, wd_hbm,
    out_ref,
    ids_ref, router_ref, q_ref, wgu, wd, kv, acc, row_max, totals, att,
    q_own, q_out, q_in, q_all, part_out, part_got, part_all, lse_out, lse_in, lse_all,
    out_rows, in_rows,
    members_a, part_a, part_in_a, hidden_a,
    members_b, part_b, part_in_b, hidden_b,
    down_out, down_in, returned,
    in_sem, own_sem, w_sem, kv_send, kv_recv, row_send, row_recv,
    a_send, a_recv, b_send, b_recv,
    down_send, down_recv, q_send, q_recv, back_send, back_recv, lse_send, lse_recv,
):
    ctx = lax.axis_index("ctx")
    ep = lax.axis_index("ep")
    tp = lax.axis_index("tp")
    n = n_ctx * n_ep
    me = ep * n_ctx + ctx
    last = n_ctx - 1
    rows, features = q_ref.shape
    kv_heads = kv.shape[1]
    places = features // HEAD_WIDTH
    group = places // kv_heads
    slots = returned.shape[0]
    live = n_ep * CAP

    def lanes(place):
        return slice(place * HEAD_WIDTH, (place + 1) * HEAD_WIDTH)

    in_copies = [
        pltpu.make_async_copy(src, dst, in_sem.at[index])
        for index, (src, dst) in enumerate((
            (ids_hbm, ids_ref), (q_hbm.at[0], q_ref), (router_hbm, router_ref),
        ))
    ]
    own_copies = [
        pltpu.make_async_copy(
            src.at[0, :, lanes(head)], kv.at[ctx, head, which], own_sem
        )
        for head in range(kv_heads)
        for which, src in enumerate((k_hbm, v_hbm))
    ]
    w_copies = [
        pltpu.make_async_copy(src.at[0], dst, sem)
        for src, dst, sem in (
            (wg_hbm, wgu.at[0], w_sem.at[0]), (wu_hbm, wgu.at[1], w_sem.at[0]),
            (wd_hbm, wd, w_sem.at[1]),
        )
    ]
    for copy in in_copies[:2] + own_copies + in_copies[2:]:
        copy.start()

    barrier = pltpu.get_barrier_semaphore()

    def greet(other):
        @pl.when(other != me)
        def _():
            pl.semaphore_signal(
                barrier, inc=1,
                device_id={"ep": other // n_ctx, "ctx": other % n_ctx},
                device_id_type=MESH,
            )

    each(n, greet)
    for step in range(1, n_tp):
        pl.semaphore_signal(
            barrier, inc=1, device_id={"tp": (tp + step) % n_tp}, device_id_type=MESH
        )

    peer = {"tp": n_tp - 1 - tp}

    def settled(ref, sem):
        return pltpu.make_async_remote_copy(
            src_ref=ref, dst_ref=ref, send_sem=sem, recv_sem=sem,
            device_id=peer, device_id_type=MESH,
        )

    def by_ctx(body):
        for index in range(n_ctx):
            pl.when(ctx == index)(functools.partial(body, index))

    def kv_copy(block, head):
        return pltpu.make_async_remote_copy(
            src_ref=kv.at[block, head], dst_ref=kv.at[block, head],
            send_sem=kv_send, recv_sem=kv_recv.at[block, head],
            device_id={"ctx": ctx + 1}, device_id_type=MESH,
        )

    def push_own(heads):
        @pl.when(ctx < last)
        def _():
            for head in heads:
                kv_copy(ctx, head).start()

    def relay(block, heads):
        @pl.when((block >= 0) & (ctx < last))
        def _():
            for head in heads:
                copy = kv_copy(block, head)
                copy.wait_recv()
                copy.start()

    def q_copy(source, target):
        return pltpu.make_async_remote_copy(
            src_ref=q_out, dst_ref=q_in.at[source],
            send_sem=q_send, recv_sem=q_recv.at[source],
            device_id={"ctx": target}, device_id_type=MESH,
        )

    def back_copies(source, target):
        return [
            pltpu.make_async_remote_copy(
                src_ref=out.at[target], dst_ref=into.at[source],
                send_sem=sent, recv_sem=got,
                device_id={"ctx": target}, device_id_type=MESH,
            )
            for out, into, sent, got in (
                (part_out, part_got, back_send, back_recv),
                (lse_out, lse_in, lse_send, lse_recv),
            )
        ]

    def to_index(other, out, into, sent, got, source):
        return pltpu.make_async_remote_copy(
            src_ref=out, dst_ref=into.at[source],
            send_sem=sent, recv_sem=got,
            device_id={"ep": other // n_ctx, "ctx": other % n_ctx}, device_id_type=MESH,
        )

    def row_copy(other, source):
        got = row_recv.at[jnp.where(ctx == 0, 0, 1)]
        return to_index(other, out_rows.at[other // n_ctx], in_rows, row_send, got, source)

    def down_copy(other, source):
        return to_index(other, down_out.at[other], down_in, down_send, down_recv, source)

    def lower(body):
        def one(other):
            @pl.when(other < ctx)
            def _():
                body(other)

        each(n_ctx, one)

    def upper(body):
        def one(step):
            other = last - step

            @pl.when(other > ctx)
            def _():
                body(other)

        each(n_ctx, one)

    def others(body):
        def one(other):
            @pl.when(other != me)
            def _():
                body(other)

        each(n, one)

    def first_owners(body):
        def one(expert):
            @pl.when(expert * n_ctx != me)
            def _():
                body(expert * n_ctx)

        each(n_ep, one)

    def later_owners(body):
        def one(other):
            @pl.when((other % n_ctx != 0) & (other != me))
            def _():
                body(other)

        each(n, one)

    with scope("a_ids"):
        in_copies[0].wait()
    with scope("a_pick"):
        ids = ids_ref[...]
        slot_row = lax.broadcasted_iota(jnp.int32, (slots, rows), 0)
        choose = jnp.where(ids == slot_row, 1.0, 0.0)
        below = lax.broadcasted_iota(jnp.int32, (rows, rows), 0)
        across = lax.broadcasted_iota(jnp.int32, (rows, rows), 1)
        strict = jnp.where(below < across, 1.0, 0.0).astype(jnp.bfloat16)
        earlier = jnp.dot(
            choose.astype(jnp.bfloat16), strict, preferred_element_type=jnp.float32
        )
        slot_index = jnp.sum(earlier * choose, axis=0, keepdims=True).astype(jnp.int32)
        target_row = jnp.where(ids < n_ep, ids * CAP + slot_index, -1)
        spread = jnp.where(target_row == slot_row, 1.0, 0.0).astype(jnp.bfloat16)
        lane_row = lax.broadcasted_iota(jnp.int32, (slots, rows), 1)
        row_place = jnp.sum(
            jnp.where(target_row == slot_row, lane_row, 0), axis=1, keepdims=True
        )
        in_copies[1].wait()
        for copy in w_copies:
            copy.start()
        for start, size in tiles_of(features, 512):
            picked = jnp.dot(
                spread, q_ref[:, start:start + size], preferred_element_type=jnp.float32
            )
            q_own[:, start:start + size] = picked
            q_out[:, start:start + size] = picked[:live].astype(jnp.bfloat16)

    def attend(source, tall, seen):
        raws = []
        for head in range(kv_heads):
            stacked = jnp.concatenate(
                [source[:, lanes(head * group + j)] for j in range(group)], axis=0
            ).astype(jnp.bfloat16)
            raw = lax.dot_general(
                stacked, kv[ctx, head, 0], (((1,), (1,)), ((), ())),
                preferred_element_type=jnp.float32,
            )
            raws.append(raw if seen is None else jnp.where(seen, raw, MASKED))
        tops = [jnp.max(raw, axis=1, keepdims=True) for raw in raws]
        weights = [jnp.exp2((raw - top) * EXP2_SCALE) for raw, top in zip(raws, tops)]
        sums = [jnp.sum(weight, axis=1, keepdims=True) for weight in weights]
        mixed = [
            jnp.dot(
                weight.astype(jnp.bfloat16), kv[ctx, head, 1],
                preferred_element_type=jnp.float32,
            ) / total
            for head, (weight, total) in enumerate(zip(weights, sums))
        ]
        columns = [top * EXP2_SCALE + jnp.log2(total) for top, total in zip(tops, sums)]
        head_lane = lax.broadcasted_iota(jnp.int32, (tall, 128), 1)
        lse = jnp.zeros((tall, 128), jnp.float32)
        for head in range(kv_heads):
            for j in range(group):
                lse = jnp.where(
                    head_lane == head * group + j, columns[head][j * tall:(j + 1) * tall], lse
                )
        return mixed, lse

    def own_landed():
        pltpu.make_async_copy(kv.at[ctx], kv.at[ctx], own_sem).wait()

    def own_part():
        key_lane = lax.broadcasted_iota(jnp.int32, (group * slots, rows), 1)
        seen = key_lane <= jnp.concatenate([row_place] * group, axis=0)
        mixed, lse = attend(q_own, slots, seen)
        lse_all[...] = jnp.full_like(lse_all, MASKED)
        lse_all[ctx] = lse
        for head in range(kv_heads):
            for j in range(group):
                part_all[ctx, :, lanes(head * group + j)] = mixed[head][
                    j * slots:(j + 1) * slots
                ]

    def put_row(place, picked):
        for expert in range(n_ep):
            out_rows[expert, place * CAP:(place + 1) * CAP] = picked[
                expert * CAP:(expert + 1) * CAP
            ].astype(jnp.bfloat16)

    def send_rows():
        others(lambda other: row_copy(other, me).start())
        in_rows[me] = out_rows[ep]

    part_all[...] = jnp.zeros_like(part_all)
    q_all[...] = jnp.zeros_like(q_all)

    @pl.when(ctx == 0)
    def _():
        with scope("b_own0"):
            own_landed()
            own_part()
            for place in range(places):
                put_row(place, part_all[0, :, lanes(place)])

    with scope("c_barrier"):
        pl.semaphore_wait(barrier, n - 1 + n_tp - 1)

    with scope("d_qsend"):
        lower(lambda other: q_copy(ctx, other).start())

    @pl.when(ctx == 0)
    def _():
        with scope("e_rows0"):
            send_rows()
            push_own(range(1))

    @pl.when(ctx > 0)
    def _():
        with scope("f_own"):
            own_landed()
            push_own(range(2))
            pl.when(ctx > 1)(lambda: push_own([2]))
            own_part()

    query_offset = lax.broadcasted_iota(jnp.int32, (rows, rows), 0)
    key_offset = lax.broadcasted_iota(jnp.int32, (rows, rows), 1)

    def scores(block, head):
        stacked = jnp.concatenate(
            [q_ref[:, lanes(head * group + j)] for j in range(group)], axis=0
        )
        return lax.dot_general(
            stacked, kv[block, head, 0], (((1,), (1,)), ((), ())),
            preferred_element_type=jnp.float32,
        )

    def mix(weights, block, head):
        return jnp.dot(
            weights.astype(jnp.bfloat16), kv[block, head, 1], preferred_element_type=jnp.float32
        )

    with scope("g_own_block"):
        visible = jnp.concatenate([query_offset >= key_offset] * group, axis=0)
        for head in range(kv_heads):
            raw = jnp.where(visible, scores(ctx, head), MASKED)
            top = jnp.broadcast_to(jnp.max(raw, axis=1, keepdims=True), raw.shape)
            weights = jnp.exp2((raw - top) * EXP2_SCALE)
            row_max[head] = top
            totals[head] = jnp.broadcast_to(
                jnp.sum(weights, axis=1, keepdims=True), weights.shape
            )
            acc[head] = mix(weights, ctx, head)

    def process(block, head):
        raw = scores(block, head)
        old_max = row_max[head]
        new_max = jnp.maximum(old_max, jnp.max(raw, axis=1, keepdims=True))
        factor = jnp.exp2((old_max - new_max) * EXP2_SCALE)
        weights = jnp.exp2((raw - new_max) * EXP2_SCALE)
        row_max[head] = new_max
        totals[head] = totals[head] * factor + jnp.sum(weights, axis=1, keepdims=True)
        acc[head] = acc[head] * factor + mix(weights, block, head)

    def visit(step):
        def arrived(heads):
            for head in heads:
                kv_copy(ctx - step, head).wait_recv()

        pl.when(ctx == last)(lambda: arrived(range(kv_heads)))
        for head in range(kv_heads):
            process(ctx - step, head)

    def visit_by_head(step):
        for head in range(kv_heads):
            pl.when(ctx == last)(lambda: kv_copy(ctx - step, head).wait_recv())
            relay(ctx - step, [head])
            process(ctx - step, head)

    @pl.when(ctx < last)
    def _():
        with scope("h_qwait"):
            upper(lambda other: q_copy(other, other).wait_recv())
        with scope("i_qpart"):
            for other in range(n_ctx):
                @pl.when(other > ctx)
                def _():
                    q_all[other * live:(other + 1) * live, :] = q_in[other].astype(jnp.float32)

            tall = n_ctx * live
            mixed, lse = attend(q_all, tall, None)
            for other in range(n_ctx):
                lse_out[other] = lse[other * live:(other + 1) * live]
                for place in range(places):
                    first = place % group * tall + other * live
                    part_out[other, :, lanes(place)] = mixed[place // group][
                        first:first + live
                    ].astype(jnp.bfloat16)

        with scope("j_give"):
            def give_back(other):
                for copy in back_copies(ctx, other):
                    copy.start()

            upper(give_back)
            pl.when(ctx == 0)(lambda: push_own(range(1, kv_heads)))
    def gate(indices, wide_ref, part, part_in, sent, got, between):
        for at, index in enumerate(indices):
            dense = in_rows[index].astype(jnp.float32)
            for place in range(places):
                wide_ref[at * CAP:(at + 1) * CAP, lanes(place)] = dense[
                    place * CAP:(place + 1) * CAP
                ]
        wide = wide_ref[...]
        members = wide.astype(jnp.bfloat16)
        own_score = jnp.sum(wide * router_ref[...].astype(jnp.float32), axis=1, keepdims=True)
        chunks, _, double_width = part.shape
        width = double_width // 2
        for chunk in range(chunks):
            if chunk == 0:
                part[0] = jnp.broadcast_to(own_score, part.shape[1:]).astype(jnp.bfloat16)
            else:
                span = slice((chunk - 1) * width, chunk * width)
                for side in range(2):
                    part[chunk, :, side * width:(side + 1) * width] = jnp.dot(
                        members, wgu[side, :, span], preferred_element_type=jnp.float32
                    ).astype(jnp.bfloat16)
            which = chunk // (chunks - 1)
            pltpu.make_async_remote_copy(
                src_ref=part.at[chunk], dst_ref=part_in.at[chunk],
                send_sem=sent, recv_sem=got.at[which],
                device_id=peer, device_id_type=MESH,
            ).start()
            between(chunk, chunks - 1)

    def activate(part, part_in, sent, got, hidden):
        chunks = part.shape[0]
        width = part.shape[2] // 2
        settled(part_in.at[pl.ds(0, chunks - 1)], got.at[0]).wait_recv()
        gain = jax.nn.sigmoid(
            part[0, :, :1].astype(jnp.float32) + part_in[0, :, :1].astype(jnp.float32)
        )
        for chunk in range(1, chunks):
            if chunk == chunks - 1:
                settled(part_in.at[chunk], got.at[1]).wait_recv()
            both = part[chunk].astype(jnp.float32) + part_in[chunk].astype(jnp.float32)
            gate_part = gain * both[:, :width]
            up_part = gain * both[:, width:]
            hidden[:, (chunk - 1) * width:chunk * width] = (
                gate_part * jax.nn.sigmoid(gate_part) * up_part
            ).astype(jnp.bfloat16)

    def down(indices, hidden):
        for start, size in tiles_of(features, 512):
            product = jnp.dot(
                hidden[...], wd[:, start:start + size], preferred_element_type=jnp.float32
            )
            for at, index in enumerate(indices):
                for place in range(start // HEAD_WIDTH, (start + size) // HEAD_WIDTH):
                    lane = place * HEAD_WIDTH - start
                    down_out[index, place * CAP:(place + 1) * CAP] = product[
                        at * CAP:(at + 1) * CAP, lane:lane + HEAD_WIDTH
                    ].astype(jnp.bfloat16)

    def keep_own():
        down_in[me] = down_out[me]

    first = [index for index in range(n) if index % n_ctx == 0]
    later = [index for index in range(n) if index % n_ctx != 0]
    exchange_a = (part_a, part_in_a, a_send, a_recv)
    exchange_b = (part_b, part_in_b, b_send, b_recv)

    with scope("l_rows_a"):
        in_copies[2].wait()
        pltpu.make_async_copy(wgu, wgu, w_sem.at[0]).wait()

        @pl.when(ctx == 0)
        def _():
            if n_ep > 1:
                settled(in_rows.at[pl.ds(0, n_ep - 1)], row_recv.at[0]).wait_recv()

        @pl.when(ctx > 0)
        def _():
            settled(in_rows.at[pl.ds(0, n_ep)], row_recv.at[0]).wait_recv()
    def between_a(chunk, count):
        if chunk == count // 2:
            pl.when(ctx == 1)(lambda: push_own(range(2, kv_heads)))
            pl.when(ctx > 1)(lambda: push_own([kv_heads - 1]))
            pl.when(ctx > 1)(lambda: relay(ctx - 1, [0]))
        if chunk == count:
            pl.when(ctx == 1)(lambda: relay(ctx - 1, [0]))
            pl.when(ctx > 1)(lambda: relay(ctx - 1, [1]))

    def between_b(chunk, count):
        if chunk == count // 2:
            relay(ctx - 2, [1])

    with scope("m_gate_a"):
        gate(first, members_a, *exchange_a, between_a)

    @pl.when(ctx > 0)
    def _():
        with scope("o_takeback"):
            def take_back(count):
                if count:
                    settled(part_got.at[pl.ds(0, count)], back_recv).wait_recv()
                    settled(lse_in.at[pl.ds(0, count)], lse_recv).wait_recv()

            by_ctx(take_back)
        with scope("p_combine"):
            for other in range(last):
                @pl.when(other < ctx)
                def _():
                    part_all[other, :live] = part_got[other].astype(jnp.float32)
                    lse_all[other, :live] = lse_in[other]

            peak = jnp.max(lse_all[...], axis=0)
            shares = [jnp.exp2(lse_all[other] - peak) for other in range(n_ctx)]
            share_total = functools.reduce(jnp.add, shares)
            shares = [share / share_total for share in shares]
            for place in range(places):
                put_row(place, functools.reduce(jnp.add, [
                    shares[other][:, place:place + 1] * part_all[other, :, lanes(place)]
                    for other in range(n_ctx)
                ]))
        with scope("q_rows"):
            send_rows()

    with scope("r_down_a"):
        w_copies[2].wait()
        activate(*exchange_a, hidden_a)
        down(first, hidden_a)
        first_owners(lambda other: down_copy(other, me).start())
        pl.when(ctx == 0)(keep_own)
    with scope("s_relay"):
        pl.when(ctx == 1)(lambda: relay(ctx - 1, range(1, kv_heads)))
        pl.when(ctx > 1)(lambda: relay(ctx - 1, range(2, kv_heads)))
    with scope("t_block1"):
        pl.when(ctx > 1)(lambda: visit(1))
    with scope("u_relay"):
        relay(ctx - 2, [0])
    with scope("v_rows_b"):
        @pl.when(ctx == 0)
        def _():
            settled(in_rows.at[pl.ds(0, n - n_ep)], row_recv.at[1]).wait_recv()

        @pl.when(ctx > 0)
        def _():
            settled(in_rows.at[pl.ds(0, n - n_ep - 1)], row_recv.at[1]).wait_recv()

    with scope("w_gate_b"):
        gate(later, members_b, *exchange_b, between_b)
    with scope("x_relay"):
        relay(ctx - 2, range(2, kv_heads - 1))
    early = (tp == n_tp - 1) & (ctx > 2)
    with scope("xa_block2"):
        pl.when(early)(lambda: visit(2))
    with scope("xb_down_b"):
        activate(*exchange_b, hidden_b)
        down(later, hidden_b)
        later_owners(lambda other: down_copy(other, me).start())
        pl.when(ctx > 0)(keep_own)

    def remaining(step, carry):
        pl.when(ctx >= step)(lambda: visit_by_head(step))
        return carry

    with scope("xc_visit"):
        relay(ctx - 2, [kv_heads - 1])
        left = jnp.where(ctx == 1, 1, 2)

        @pl.when((ctx > 0) & jnp.logical_not(early))
        def _():
            visit(left)

        lax.fori_loop(3, n_ctx, remaining, 0)

    with scope("xd_norm"):
        for head in range(kv_heads):
            normed = (acc[head] / totals[head]).astype(jnp.bfloat16)
            for j in range(group):
                att[:, lanes(head * group + j)] = normed[j * rows:(j + 1) * rows]
        returned[...] = jnp.zeros_like(returned)

    with scope("xe_sent"):
        settled(in_rows.at[pl.ds(0, n - 1)], row_send).wait_send()
        settled(part_a, a_send).wait_send()
        settled(part_b, b_send).wait_send()

        def drain(index):
            if index:
                settled(q_in.at[pl.ds(0, index)], q_send).wait_send()
            if index < last:
                settled(part_out.at[pl.ds(0, last - index)], back_send).wait_send()
                settled(lse_out.at[pl.ds(0, last - index)], lse_send).wait_send()
                settled(kv.at[pl.ds(0, index + 1)], kv_send).wait_send()

        by_ctx(drain)

    with scope("xf_downwait"):
        settled(down_in.at[pl.ds(0, n - 1)], down_recv).wait_recv()
    with scope("xg_final"):
        for expert in range(n_ep):
            total = down_in[expert * n_ctx].astype(jnp.float32)
            for index in range(1, n_ctx):
                total = total + down_in[expert * n_ctx + index].astype(jnp.float32)
            total = total.astype(jnp.bfloat16).astype(jnp.float32)
            for place in range(places):
                returned[expert * CAP:(expert + 1) * CAP, lanes(place)] = total[
                    place * CAP:(place + 1) * CAP
                ]
        for start, size in tiles_of(features, 512):
            routed = lax.dot_general(
                spread, returned[:, start:start + size].astype(jnp.bfloat16),
                (((0,), (0,)), ((), ())), preferred_element_type=jnp.float32,
            )
            out_ref[0, :, start:start + size] = (
                att[:, start:start + size].astype(jnp.float32) + routed
            ).astype(jnp.bfloat16)
    with scope("xh_sent"):
        settled(down_out.at[pl.ds(0, n - 1)], down_send).wait_send()


def shards(queries, keys, values, expert_ids, router, w_gate, w_up, w_down):
    n_ctx, n_ep, n_tp = (lax.axis_size(axis) for axis in ("ctx", "ep", "tp"))
    n = n_ctx * n_ep
    _, rows, features = queries.shape
    kv_width = keys.shape[2]
    kv_heads = kv_width // HEAD_WIDTH
    group = features // kv_width
    hidden_width = w_gate.shape[2]
    chunk_width = min(hidden_width, 256)
    chunks = hidden_width // chunk_width
    dense = features // HEAD_WIDTH * CAP
    live = n_ep * CAP
    slots = padded(live)
    bf16, f32 = jnp.bfloat16, jnp.float32
    hbm = pl.BlockSpec(memory_space=pltpu.HBM)
    dma = pltpu.SemaphoreType.DMA

    def batch(count):
        return [
            pltpu.VMEM((count, features), f32),
            pltpu.VMEM((chunks + 1, count, 2 * chunk_width), bf16),
            pltpu.VMEM((chunks + 1, count, 2 * chunk_width), bf16),
            pltpu.VMEM((count, hidden_width), bf16),
        ]

    return pl.pallas_call(
        functools.partial(kernel, n_ctx, n_ep, n_tp),
        out_shape=pltpu.VMEM(queries.shape, bf16),
        in_specs=[hbm] * 8,
        out_specs=pl.BlockSpec(memory_space=pltpu.VMEM),
        scratch_shapes=[
            pltpu.VMEM((1, rows), jnp.int32),
            pltpu.VMEM((1, features), bf16),
            pltpu.VMEM((rows, features), bf16),
            pltpu.VMEM((2, *w_gate.shape[1:]), bf16),
            pltpu.VMEM(w_down.shape[1:], bf16),
            pltpu.VMEM((n_ctx, kv_heads, 2, rows, HEAD_WIDTH), bf16),
            pltpu.VMEM((kv_heads, group * rows, HEAD_WIDTH), f32),
            pltpu.VMEM((kv_heads, group * rows, HEAD_WIDTH), f32),
            pltpu.VMEM((kv_heads, group * rows, HEAD_WIDTH), f32),
            pltpu.VMEM((rows, features), bf16),
            pltpu.VMEM((slots, features), f32),
            pltpu.VMEM((live, features), bf16),
            pltpu.VMEM((n_ctx, live, features), bf16),
            pltpu.VMEM((n_ctx * live, features), f32),
            pltpu.VMEM((n_ctx, live, features), bf16),
            pltpu.VMEM((n_ctx, live, features), bf16),
            pltpu.VMEM((n_ctx, slots, features), f32),
            pltpu.VMEM((n_ctx, live, 128), f32),
            pltpu.VMEM((n_ctx, live, 128), f32),
            pltpu.VMEM((n_ctx, slots, 128), f32),
            pltpu.VMEM((n_ep, dense, HEAD_WIDTH), bf16),
            pltpu.VMEM((n, dense, HEAD_WIDTH), bf16),
            *batch(n_ep * CAP),
            *batch((n - n_ep) * CAP),
            pltpu.VMEM((n, dense, HEAD_WIDTH), bf16),
            pltpu.VMEM((n, dense, HEAD_WIDTH), bf16),
            pltpu.VMEM((slots, features), f32),
            dma((3,)),
            dma,
            dma((2,)),
            dma,
            dma((n_ctx - 1, kv_heads)),
            dma,
            dma((2,)),
            dma,
            dma((2,)),
            dma,
            dma((2,)),
            dma,
            dma,
            dma,
            dma((n_ctx,)),
            *[dma] * 4,
        ],
        compiler_params=pltpu.CompilerParams(
            collective_id=0, has_side_effects=True, vmem_limit_bytes=60 * 1024 * 1024
        ),
    )(
        expert_ids.reshape(1, rows), router.reshape(1, features), queries, keys, values,
        w_gate, w_up, w_down,
    )


def solution(mesh):
    placed = (
        P(("groups", "ep"), "ctx", "tp"),
        P(("groups", "ep"), "ctx", "tp"),
        P(("groups", "ep"), "ctx", "tp"),
        P(("groups", "ep"), "ctx", None),
        P("tp", "ep"),
        P("ep", "tp", "ctx"),
        P("ep", "tp", "ctx"),
        P("ep", "ctx", "tp"),
    )
    return jax.shard_map(
        shards,
        mesh=mesh,
        in_specs=placed,
        out_specs=P(("groups", "ep"), "ctx", "tp"),
        check_vma=False,
    )
```

```python
import functools
import math

import jax
import jax.numpy as jnp
from jax import lax
from jax.experimental import pallas as pl
from jax.experimental.pallas import tpu as pltpu
from jax.sharding import PartitionSpec as P

HEAD_WIDTH = 128
CAP = 2
MESH = pl.DeviceIdType.MESH
MASKED = -1e30
EXP2_SCALE = HEAD_WIDTH ** (-0.5) * math.log2(math.e)
scope = jax.named_scope


def tiles_of(width, tile):
    tile = min(width, tile)
    return [(start, min(tile, width - start)) for start in range(0, width, tile)]


def padded(count, tile=8):
    return -(-count // tile) * tile


def each(count, body):
    if count <= 8:
        for index in range(count):
            body(index)
    else:
        pl.loop(0, count)(body)


def kernel(
    n_ctx, n_ep, n_tp,
    ids_hbm, router_hbm, q_hbm, k_hbm, v_hbm, wg_hbm, wu_hbm, wd_hbm,
    out_ref,
    ids_ref, router_ref, q_ref, wgu, wd, kv, acc, row_max, totals, att,
    q_own, q_out, q_in, q_all, part_out, part_got, part_all, lse_out, lse_in, lse_all,
    out_rows, in_rows,
    members_a, part_a, part_in_a, hidden_a,
    members_b, part_b, part_in_b, hidden_b,
    down_out, down_in, returned,
    in_sem, own_sem, w_sem, kv_send, kv_recv, row_send, row_recv,
    a_send, a_recv, b_send, b_recv,
    down_send, down_recv, q_send, q_recv, back_send, back_recv, lse_send, lse_recv,
):
    ctx = lax.axis_index("ctx")
    ep = lax.axis_index("ep")
    tp = lax.axis_index("tp")
    n = n_ctx * n_ep
    me = ep * n_ctx + ctx
    last = n_ctx - 1
    rows, features = q_ref.shape
    kv_heads = kv.shape[1]
    places = features // HEAD_WIDTH
    group = places // kv_heads
    slots = returned.shape[0]
    live = n_ep * CAP

    def lanes(place):
        return slice(place * HEAD_WIDTH, (place + 1) * HEAD_WIDTH)

    in_copies = [
        pltpu.make_async_copy(src, dst, in_sem.at[index])
        for index, (src, dst) in enumerate((
            (ids_hbm, ids_ref), (q_hbm.at[0], q_ref), (router_hbm, router_ref),
        ))
    ]
    own_copies = [
        pltpu.make_async_copy(
            src.at[0, :, lanes(head)], kv.at[ctx, head, which], own_sem
        )
        for head in range(kv_heads)
        for which, src in enumerate((k_hbm, v_hbm))
    ]
    w_copies = [
        pltpu.make_async_copy(src.at[0], dst, sem)
        for src, dst, sem in (
            (wg_hbm, wgu.at[0], w_sem.at[0]), (wu_hbm, wgu.at[1], w_sem.at[0]),
            (wd_hbm, wd, w_sem.at[1]),
        )
    ]
    for copy in in_copies[:2] + own_copies + in_copies[2:]:
        copy.start()

    barrier = pltpu.get_barrier_semaphore()

    def greet(other):
        @pl.when(other != me)
        def _():
            pl.semaphore_signal(
                barrier, inc=1,
                device_id={"ep": other // n_ctx, "ctx": other % n_ctx},
                device_id_type=MESH,
            )

    each(n, greet)
    for step in range(1, n_tp):
        pl.semaphore_signal(
            barrier, inc=1, device_id={"tp": (tp + step) % n_tp}, device_id_type=MESH
        )

    peer = {"tp": n_tp - 1 - tp}

    def settled(ref, sem):
        return pltpu.make_async_remote_copy(
            src_ref=ref, dst_ref=ref, send_sem=sem, recv_sem=sem,
            device_id=peer, device_id_type=MESH,
        )

    def by_ctx(body):
        for index in range(n_ctx):
            pl.when(ctx == index)(functools.partial(body, index))

    def kv_copy(block, head):
        return pltpu.make_async_remote_copy(
            src_ref=kv.at[block, head], dst_ref=kv.at[block, head],
            send_sem=kv_send, recv_sem=kv_recv.at[block, head],
            device_id={"ctx": ctx + 1}, device_id_type=MESH,
        )

    def push_own(heads):
        @pl.when(ctx < last)
        def _():
            for head in heads:
                kv_copy(ctx, head).start()

    def relay(block, heads):
        @pl.when((block >= 0) & (ctx < last))
        def _():
            for head in heads:
                copy = kv_copy(block, head)
                copy.wait_recv()
                copy.start()

    def q_copy(source, target):
        return pltpu.make_async_remote_copy(
            src_ref=q_out, dst_ref=q_in.at[source],
            send_sem=q_send, recv_sem=q_recv.at[source],
            device_id={"ctx": target}, device_id_type=MESH,
        )

    def back_copies(source, target):
        return [
            pltpu.make_async_remote_copy(
                src_ref=out.at[target], dst_ref=into.at[source],
                send_sem=sent, recv_sem=got,
                device_id={"ctx": target}, device_id_type=MESH,
            )
            for out, into, sent, got in (
                (part_out, part_got, back_send, back_recv),
                (lse_out, lse_in, lse_send, lse_recv),
            )
        ]

    def to_index(other, out, into, sent, got, source):
        return pltpu.make_async_remote_copy(
            src_ref=out, dst_ref=into.at[source],
            send_sem=sent, recv_sem=got,
            device_id={"ep": other // n_ctx, "ctx": other % n_ctx}, device_id_type=MESH,
        )

    def row_copy(other, source):
        got = row_recv.at[jnp.where(ctx == 0, 0, 1)]
        return to_index(other, out_rows.at[other // n_ctx], in_rows, row_send, got, source)

    def down_copy(other, source):
        return to_index(other, down_out.at[other], down_in, down_send, down_recv, source)

    def lower(body):
        def one(other):
            @pl.when(other < ctx)
            def _():
                body(other)

        each(n_ctx, one)

    def upper(body):
        def one(step):
            other = last - step

            @pl.when(other > ctx)
            def _():
                body(other)

        each(n_ctx, one)

    def others(body):
        def one(other):
            @pl.when(other != me)
            def _():
                body(other)

        each(n, one)

    def first_owners(body):
        def one(expert):
            @pl.when(expert * n_ctx != me)
            def _():
                body(expert * n_ctx)

        each(n_ep, one)

    def later_owners(body):
        def one(other):
            @pl.when((other % n_ctx != 0) & (other != me))
            def _():
                body(other)

        each(n, one)

    with scope("a_ids"):
        in_copies[0].wait()
    with scope("a_pick"):
        ids = ids_ref[...]
        slot_row = lax.broadcasted_iota(jnp.int32, (slots, rows), 0)
        choose = jnp.where(ids == slot_row, 1.0, 0.0)
        below = lax.broadcasted_iota(jnp.int32, (rows, rows), 0)
        across = lax.broadcasted_iota(jnp.int32, (rows, rows), 1)
        strict = jnp.where(below < across, 1.0, 0.0).astype(jnp.bfloat16)
        earlier = jnp.dot(
            choose.astype(jnp.bfloat16), strict, preferred_element_type=jnp.float32
        )
        slot_index = jnp.sum(earlier * choose, axis=0, keepdims=True).astype(jnp.int32)
        target_row = jnp.where(ids < n_ep, ids * CAP + slot_index, -1)
        spread = jnp.where(target_row == slot_row, 1.0, 0.0).astype(jnp.bfloat16)
        lane_row = lax.broadcasted_iota(jnp.int32, (slots, rows), 1)
        row_place = jnp.sum(
            jnp.where(target_row == slot_row, lane_row, 0), axis=1, keepdims=True
        )
        in_copies[1].wait()
        for copy in w_copies:
            copy.start()
        for start, size in tiles_of(features, 512):
            picked = jnp.dot(
                spread, q_ref[:, start:start + size], preferred_element_type=jnp.float32
            )
            q_own[:, start:start + size] = picked
            q_out[:, start:start + size] = picked[:live].astype(jnp.bfloat16)

    def attend(source, tall, seen):
        raws = []
        for head in range(kv_heads):
            stacked = jnp.concatenate(
                [source[:, lanes(head * group + j)] for j in range(group)], axis=0
            ).astype(jnp.bfloat16)
            raw = lax.dot_general(
                stacked, kv[ctx, head, 0], (((1,), (1,)), ((), ())),
                preferred_element_type=jnp.float32,
            )
            raws.append(raw if seen is None else jnp.where(seen, raw, MASKED))
        tops = [jnp.max(raw, axis=1, keepdims=True) for raw in raws]
        weights = [jnp.exp2((raw - top) * EXP2_SCALE) for raw, top in zip(raws, tops)]
        sums = [jnp.sum(weight, axis=1, keepdims=True) for weight in weights]
        mixed = [
            jnp.dot(
                weight.astype(jnp.bfloat16), kv[ctx, head, 1],
                preferred_element_type=jnp.float32,
            ) / total
            for head, (weight, total) in enumerate(zip(weights, sums))
        ]
        columns = [top * EXP2_SCALE + jnp.log2(total) for top, total in zip(tops, sums)]
        head_lane = lax.broadcasted_iota(jnp.int32, (tall, 128), 1)
        lse = jnp.zeros((tall, 128), jnp.float32)
        for head in range(kv_heads):
            for j in range(group):
                lse = jnp.where(
                    head_lane == head * group + j, columns[head][j * tall:(j + 1) * tall], lse
                )
        return mixed, lse

    def own_landed():
        pltpu.make_async_copy(kv.at[ctx], kv.at[ctx], own_sem).wait()

    def own_part():
        key_lane = lax.broadcasted_iota(jnp.int32, (group * slots, rows), 1)
        seen = key_lane <= jnp.concatenate([row_place] * group, axis=0)
        mixed, lse = attend(q_own, slots, seen)
        lse_all[...] = jnp.full_like(lse_all, MASKED)
        lse_all[ctx] = lse
        for head in range(kv_heads):
            for j in range(group):
                part_all[ctx, :, lanes(head * group + j)] = mixed[head][
                    j * slots:(j + 1) * slots
                ]

    def put_row(place, picked):
        for expert in range(n_ep):
            out_rows[expert, place * CAP:(place + 1) * CAP] = picked[
                expert * CAP:(expert + 1) * CAP
            ].astype(jnp.bfloat16)

    def send_rows():
        others(lambda other: row_copy(other, me).start())
        in_rows[me] = out_rows[ep]

    part_all[...] = jnp.zeros_like(part_all)
    q_all[...] = jnp.zeros_like(q_all)

    @pl.when(ctx == 0)
    def _():
        with scope("b_own0"):
            own_landed()
            own_part()
            for place in range(places):
                put_row(place, part_all[0, :, lanes(place)])

    with scope("c_barrier"):
        pl.semaphore_wait(barrier, n - 1 + n_tp - 1)

    with scope("d_qsend"):
        lower(lambda other: q_copy(ctx, other).start())

    @pl.when(ctx == 0)
    def _():
        with scope("e_rows0"):
            send_rows()
            push_own(range(1))

    @pl.when(ctx > 0)
    def _():
        with scope("f_own"):
            own_landed()
            push_own(range(2))
            pl.when(ctx > 1)(lambda: push_own([2]))
            own_part()

    query_offset = lax.broadcasted_iota(jnp.int32, (rows, rows), 0)
    key_offset = lax.broadcasted_iota(jnp.int32, (rows, rows), 1)

    def scores(block, head):
        stacked = jnp.concatenate(
            [q_ref[:, lanes(head * group + j)] for j in range(group)], axis=0
        )
        return lax.dot_general(
            stacked, kv[block, head, 0], (((1,), (1,)), ((), ())),
            preferred_element_type=jnp.float32,
        )

    def mix(weights, block, head):
        return jnp.dot(
            weights.astype(jnp.bfloat16), kv[block, head, 1], preferred_element_type=jnp.float32
        )

    with scope("g_own_block"):
        visible = jnp.concatenate([query_offset >= key_offset] * group, axis=0)
        for head in range(kv_heads):
            raw = jnp.where(visible, scores(ctx, head), MASKED)
            top = jnp.broadcast_to(jnp.max(raw, axis=1, keepdims=True), raw.shape)
            weights = jnp.exp2((raw - top) * EXP2_SCALE)
            row_max[head] = top
            totals[head] = jnp.broadcast_to(
                jnp.sum(weights, axis=1, keepdims=True), weights.shape
            )
            acc[head] = mix(weights, ctx, head)

    def process(block, head):
        raw = scores(block, head)
        old_max = row_max[head]
        new_max = jnp.maximum(old_max, jnp.max(raw, axis=1, keepdims=True))
        factor = jnp.exp2((old_max - new_max) * EXP2_SCALE)
        weights = jnp.exp2((raw - new_max) * EXP2_SCALE)
        row_max[head] = new_max
        totals[head] = totals[head] * factor + jnp.sum(weights, axis=1, keepdims=True)
        acc[head] = acc[head] * factor + mix(weights, block, head)

    def visit(step):
        def arrived(heads):
            for head in heads:
                kv_copy(ctx - step, head).wait_recv()

        pl.when(ctx == last)(lambda: arrived(range(kv_heads)))
        for head in range(kv_heads):
            process(ctx - step, head)

    def visit_by_head(step):
        for head in range(kv_heads):
            pl.when(ctx == last)(lambda: kv_copy(ctx - step, head).wait_recv())
            relay(ctx - step, [head])
            process(ctx - step, head)

    @pl.when(ctx < last)
    def _():
        with scope("h_qwait"):
            upper(lambda other: q_copy(other, other).wait_recv())
        with scope("i_qpart"):
            for other in range(n_ctx):
                @pl.when(other > ctx)
                def _():
                    q_all[other * live:(other + 1) * live, :] = q_in[other].astype(jnp.float32)

            tall = n_ctx * live
            mixed, lse = attend(q_all, tall, None)
            for other in range(n_ctx):
                lse_out[other] = lse[other * live:(other + 1) * live]
                for place in range(places):
                    first = place % group * tall + other * live
                    part_out[other, :, lanes(place)] = mixed[place // group][
                        first:first + live
                    ].astype(jnp.bfloat16)

        with scope("j_give"):
            def give_back(other):
                for copy in back_copies(ctx, other):
                    copy.start()

            upper(give_back)
            pl.when(ctx == 0)(lambda: push_own(range(1, kv_heads)))
    def gate(indices, wide_ref, part, part_in, sent, got, between):
        for at, index in enumerate(indices):
            dense = in_rows[index].astype(jnp.float32)
            for place in range(places):
                wide_ref[at * CAP:(at + 1) * CAP, lanes(place)] = dense[
                    place * CAP:(place + 1) * CAP
                ]
        wide = wide_ref[...]
        members = wide.astype(jnp.bfloat16)
        own_score = jnp.sum(wide * router_ref[...].astype(jnp.float32), axis=1, keepdims=True)
        chunks, _, double_width = part.shape
        width = double_width // 2
        for chunk in range(chunks):
            if chunk == 0:
                part[0] = jnp.broadcast_to(own_score, part.shape[1:]).astype(jnp.bfloat16)
            else:
                span = slice((chunk - 1) * width, chunk * width)
                for side in range(2):
                    part[chunk, :, side * width:(side + 1) * width] = jnp.dot(
                        members, wgu[side, :, span], preferred_element_type=jnp.float32
                    ).astype(jnp.bfloat16)
            which = chunk // (chunks - 1)
            pltpu.make_async_remote_copy(
                src_ref=part.at[chunk], dst_ref=part_in.at[chunk],
                send_sem=sent, recv_sem=got.at[which],
                device_id=peer, device_id_type=MESH,
            ).start()
            between(chunk, chunks - 1)

    def activate(part, part_in, sent, got, hidden):
        chunks = part.shape[0]
        width = part.shape[2] // 2
        settled(part_in.at[pl.ds(0, chunks - 1)], got.at[0]).wait_recv()
        gain = jax.nn.sigmoid(
            part[0, :, :1].astype(jnp.float32) + part_in[0, :, :1].astype(jnp.float32)
        )
        for chunk in range(1, chunks):
            if chunk == chunks - 1:
                settled(part_in.at[chunk], got.at[1]).wait_recv()
            both = part[chunk].astype(jnp.float32) + part_in[chunk].astype(jnp.float32)
            gate_part = gain * both[:, :width]
            up_part = gain * both[:, width:]
            hidden[:, (chunk - 1) * width:chunk * width] = (
                gate_part * jax.nn.sigmoid(gate_part) * up_part
            ).astype(jnp.bfloat16)

    def down(indices, hidden):
        for start, size in tiles_of(features, 512):
            product = jnp.dot(
                hidden[...], wd[:, start:start + size], preferred_element_type=jnp.float32
            )
            for at, index in enumerate(indices):
                for place in range(start // HEAD_WIDTH, (start + size) // HEAD_WIDTH):
                    lane = place * HEAD_WIDTH - start
                    down_out[index, place * CAP:(place + 1) * CAP] = product[
                        at * CAP:(at + 1) * CAP, lane:lane + HEAD_WIDTH
                    ].astype(jnp.bfloat16)

    def keep_own():
        down_in[me] = down_out[me]

    first = [index for index in range(n) if index % n_ctx == 0]
    later = [index for index in range(n) if index % n_ctx != 0]
    exchange_a = (part_a, part_in_a, a_send, a_recv)
    exchange_b = (part_b, part_in_b, b_send, b_recv)

    with scope("l_rows_a"):
        in_copies[2].wait()
        pltpu.make_async_copy(wgu, wgu, w_sem.at[0]).wait()

        @pl.when(ctx == 0)
        def _():
            if n_ep > 1:
                settled(in_rows.at[pl.ds(0, n_ep - 1)], row_recv.at[0]).wait_recv()

        @pl.when(ctx > 0)
        def _():
            settled(in_rows.at[pl.ds(0, n_ep)], row_recv.at[0]).wait_recv()
    def between_a(chunk, count):
        if chunk == count // 2:
            pl.when(ctx == 1)(lambda: push_own(range(2, kv_heads)))
            pl.when(ctx > 1)(lambda: push_own([kv_heads - 1]))
            pl.when(ctx > 1)(lambda: relay(ctx - 1, [0]))
        if chunk == count:
            pl.when(ctx == 1)(lambda: relay(ctx - 1, [0]))
            pl.when(ctx > 1)(lambda: relay(ctx - 1, [1]))

    def between_b(chunk, count):
        pass

    with scope("m_gate_a"):
        gate(first, members_a, *exchange_a, between_a)

    @pl.when(ctx > 0)
    def _():
        with scope("o_takeback"):
            def take_back(count):
                if count:
                    settled(part_got.at[pl.ds(0, count)], back_recv).wait_recv()
                    settled(lse_in.at[pl.ds(0, count)], lse_recv).wait_recv()

            by_ctx(take_back)
        with scope("p_combine"):
            for other in range(last):
                @pl.when(other < ctx)
                def _():
                    part_all[other, :live] = part_got[other].astype(jnp.float32)
                    lse_all[other, :live] = lse_in[other]

            peak = jnp.max(lse_all[...], axis=0)
            shares = [jnp.exp2(lse_all[other] - peak) for other in range(n_ctx)]
            share_total = functools.reduce(jnp.add, shares)
            shares = [share / share_total for share in shares]
            for place in range(places):
                put_row(place, functools.reduce(jnp.add, [
                    shares[other][:, place:place + 1] * part_all[other, :, lanes(place)]
                    for other in range(n_ctx)
                ]))
        with scope("q_rows"):
            send_rows()

    with scope("r_down_a"):
        w_copies[2].wait()
        activate(*exchange_a, hidden_a)
        down(first, hidden_a)
        first_owners(lambda other: down_copy(other, me).start())
        pl.when(ctx == 0)(keep_own)
    with scope("s_relay"):
        pl.when(ctx == 1)(lambda: relay(ctx - 1, range(1, kv_heads)))
        pl.when(ctx > 1)(lambda: relay(ctx - 1, range(2, kv_heads)))
    with scope("t_block1"):
        pl.when(ctx > 1)(lambda: visit(1))
    with scope("u_relay"):
        relay(ctx - 2, [0])
    with scope("v_rows_b"):
        @pl.when(ctx == 0)
        def _():
            settled(in_rows.at[pl.ds(0, n - n_ep)], row_recv.at[1]).wait_recv()

        @pl.when(ctx > 0)
        def _():
            settled(in_rows.at[pl.ds(0, n - n_ep - 1)], row_recv.at[1]).wait_recv()

    with scope("w_gate_b"):
        gate(later, members_b, *exchange_b, between_b)
    with scope("x_relay"):
        relay(ctx - 2, [1])
    early = (tp == n_tp - 1) & (ctx > 2)
    with scope("xa_block2"):
        pl.when(early)(lambda: visit(2))
    with scope("xb_down_b"):
        activate(*exchange_b, hidden_b)
        down(later, hidden_b)
        later_owners(lambda other: down_copy(other, me).start())
        pl.when(ctx > 0)(keep_own)

    def remaining(step, carry):
        pl.when(ctx >= step)(lambda: visit_by_head(step))
        return carry

    def norm(head):
        normed = (acc[head] / totals[head]).astype(jnp.bfloat16)
        for j in range(group):
            att[:, lanes(head * group + j)] = normed[j * rows:(j + 1) * rows]

    def settle_down():
        settled(down_in.at[pl.ds(0, n - 1)], down_recv).wait_recv()
        returned[...] = jnp.zeros_like(returned)
        for expert in range(n_ep):
            total = down_in[expert * n_ctx].astype(jnp.float32)
            for index in range(1, n_ctx):
                total = total + down_in[expert * n_ctx + index].astype(jnp.float32)
            total = total.astype(jnp.bfloat16).astype(jnp.float32)
            for place in range(places):
                returned[expert * CAP:(expert + 1) * CAP, lanes(place)] = total[
                    place * CAP:(place + 1) * CAP
                ]

    def finish(head):
        width = group * HEAD_WIDTH
        span = slice(head * width, (head + 1) * width)
        routed = lax.dot_general(
            spread, returned[:, span].astype(jnp.bfloat16),
            (((0,), (0,)), ((), ())), preferred_element_type=jnp.float32,
        )
        out_ref[0, :, span] = (att[:, span].astype(jnp.float32) + routed).astype(jnp.bfloat16)

    with scope("xc_visit"):
        relay(ctx - 2, range(2, kv_heads))
        left = jnp.where(ctx == 1, 1, 2)

        @pl.when((ctx > 0) & jnp.logical_not(early))
        def _():
            visit(left)

    ends = (ctx == last) & (last > 2)

    @pl.when(ends)
    def _():
        with scope("xd_visit"):
            lax.fori_loop(3, last, remaining, 0)

            def arrived(head):
                kv_copy(0, head).wait_recv()
                process(0, head)
                norm(head)

            for head in range(kv_heads - 1):
                arrived(head)
        with scope("xe_down"):
            settle_down()
            for head in range(kv_heads - 1):
                finish(head)
        with scope("xf_last"):
            arrived(kv_heads - 1)
            finish(kv_heads - 1)

    @pl.when(jnp.logical_not(ends))
    def _():
        lax.fori_loop(3, n_ctx, remaining, 0)
        with scope("xd_norm"):
            for head in range(kv_heads):
                norm(head)
        with scope("xe_down"):
            settle_down()
        with scope("xg_final"):
            for head in range(kv_heads):
                finish(head)

    with scope("xh_sent"):
        settled(in_rows.at[pl.ds(0, n - 1)], row_send).wait_send()
        settled(part_a, a_send).wait_send()
        settled(part_b, b_send).wait_send()

        def drain(index):
            if index:
                settled(q_in.at[pl.ds(0, index)], q_send).wait_send()
            if index < last:
                settled(part_out.at[pl.ds(0, last - index)], back_send).wait_send()
                settled(lse_out.at[pl.ds(0, last - index)], lse_send).wait_send()
                settled(kv.at[pl.ds(0, index + 1)], kv_send).wait_send()

        by_ctx(drain)
        settled(down_out.at[pl.ds(0, n - 1)], down_send).wait_send()


def shards(queries, keys, values, expert_ids, router, w_gate, w_up, w_down):
    n_ctx, n_ep, n_tp = (lax.axis_size(axis) for axis in ("ctx", "ep", "tp"))
    n = n_ctx * n_ep
    _, rows, features = queries.shape
    kv_width = keys.shape[2]
    kv_heads = kv_width // HEAD_WIDTH
    group = features // kv_width
    hidden_width = w_gate.shape[2]
    chunk_width = min(hidden_width, 256)
    chunks = hidden_width // chunk_width
    dense = features // HEAD_WIDTH * CAP
    live = n_ep * CAP
    slots = padded(live)
    bf16, f32 = jnp.bfloat16, jnp.float32
    hbm = pl.BlockSpec(memory_space=pltpu.HBM)
    dma = pltpu.SemaphoreType.DMA

    def batch(count):
        return [
            pltpu.VMEM((count, features), f32),
            pltpu.VMEM((chunks + 1, count, 2 * chunk_width), bf16),
            pltpu.VMEM((chunks + 1, count, 2 * chunk_width), bf16),
            pltpu.VMEM((count, hidden_width), bf16),
        ]

    return pl.pallas_call(
        functools.partial(kernel, n_ctx, n_ep, n_tp),
        out_shape=pltpu.VMEM(queries.shape, bf16),
        in_specs=[hbm] * 8,
        out_specs=pl.BlockSpec(memory_space=pltpu.VMEM),
        scratch_shapes=[
            pltpu.VMEM((1, rows), jnp.int32),
            pltpu.VMEM((1, features), bf16),
            pltpu.VMEM((rows, features), bf16),
            pltpu.VMEM((2, *w_gate.shape[1:]), bf16),
            pltpu.VMEM(w_down.shape[1:], bf16),
            pltpu.VMEM((n_ctx, kv_heads, 2, rows, HEAD_WIDTH), bf16),
            pltpu.VMEM((kv_heads, group * rows, HEAD_WIDTH), f32),
            pltpu.VMEM((kv_heads, group * rows, HEAD_WIDTH), f32),
            pltpu.VMEM((kv_heads, group * rows, HEAD_WIDTH), f32),
            pltpu.VMEM((rows, features), bf16),
            pltpu.VMEM((slots, features), f32),
            pltpu.VMEM((live, features), bf16),
            pltpu.VMEM((n_ctx, live, features), bf16),
            pltpu.VMEM((n_ctx * live, features), f32),
            pltpu.VMEM((n_ctx, live, features), bf16),
            pltpu.VMEM((n_ctx, live, features), bf16),
            pltpu.VMEM((n_ctx, slots, features), f32),
            pltpu.VMEM((n_ctx, live, 128), f32),
            pltpu.VMEM((n_ctx, live, 128), f32),
            pltpu.VMEM((n_ctx, slots, 128), f32),
            pltpu.VMEM((n_ep, dense, HEAD_WIDTH), bf16),
            pltpu.VMEM((n, dense, HEAD_WIDTH), bf16),
            *batch(n_ep * CAP),
            *batch((n - n_ep) * CAP),
            pltpu.VMEM((n, dense, HEAD_WIDTH), bf16),
            pltpu.VMEM((n, dense, HEAD_WIDTH), bf16),
            pltpu.VMEM((slots, features), f32),
            dma((3,)),
            dma,
            dma((2,)),
            dma,
            dma((n_ctx - 1, kv_heads)),
            dma,
            dma((2,)),
            dma,
            dma((2,)),
            dma,
            dma((2,)),
            dma,
            dma,
            dma,
            dma((n_ctx,)),
            *[dma] * 4,
        ],
        compiler_params=pltpu.CompilerParams(
            collective_id=0, has_side_effects=True, vmem_limit_bytes=60 * 1024 * 1024
        ),
    )(
        expert_ids.reshape(1, rows), router.reshape(1, features), queries, keys, values,
        w_gate, w_up, w_down,
    )


def solution(mesh):
    placed = (
        P(("groups", "ep"), "ctx", "tp"),
        P(("groups", "ep"), "ctx", "tp"),
        P(("groups", "ep"), "ctx", "tp"),
        P(("groups", "ep"), "ctx", None),
        P("tp", "ep"),
        P("ep", "tp", "ctx"),
        P("ep", "tp", "ctx"),
        P("ep", "ctx", "tp"),
    )
    return jax.shard_map(
        shards,
        mesh=mesh,
        in_specs=placed,
        out_specs=P(("groups", "ep"), "ctx", "tp"),
        check_vma=False,
    )
```

```python
import functools
import math

import jax
import jax.numpy as jnp
from jax import lax
from jax.experimental import pallas as pl
from jax.experimental.pallas import tpu as pltpu
from jax.sharding import PartitionSpec as P

HEAD_WIDTH = 128
CAP = 2
MESH = pl.DeviceIdType.MESH
MASKED = -1e30
EXP2_SCALE = HEAD_WIDTH ** (-0.5) * math.log2(math.e)
scope = jax.named_scope


def tiles_of(width, tile):
    tile = min(width, tile)
    return [(start, min(tile, width - start)) for start in range(0, width, tile)]


def padded(count, tile=8):
    return -(-count // tile) * tile


def each(count, body):
    if count <= 8:
        for index in range(count):
            body(index)
    else:
        pl.loop(0, count)(body)


def kernel(
    n_ctx, n_ep, n_tp,
    ids_hbm, router_hbm, q_hbm, k_hbm, v_hbm, wg_hbm, wu_hbm, wd_hbm,
    out_ref,
    ids_ref, router_ref, q_ref, wgu, wd, kv, acc, row_max, totals, att,
    q_own, q_out, q_in, q_all, part_out, part_got, part_all, lse_out, lse_in, lse_all,
    out_rows, in_rows,
    members_a, part_a, part_in_a, hidden_a,
    members_b, part_b, part_in_b, hidden_b,
    down_out, down_in, returned,
    in_sem, own_sem, w_sem, kv_send, kv_recv, row_send, row_recv,
    a_send, a_recv, b_send, b_recv,
    down_send, down_recv, q_send, q_recv, back_send, back_recv, lse_send, lse_recv,
):
    ctx = lax.axis_index("ctx")
    ep = lax.axis_index("ep")
    tp = lax.axis_index("tp")
    n = n_ctx * n_ep
    me = ep * n_ctx + ctx
    last = n_ctx - 1
    home = last - 1
    rows, features = q_ref.shape
    kv_heads = kv.shape[1]
    places = features // HEAD_WIDTH
    group = places // kv_heads
    slots = returned.shape[0]
    live = n_ep * CAP

    def lanes(place):
        return slice(place * HEAD_WIDTH, (place + 1) * HEAD_WIDTH)

    in_copies = [
        pltpu.make_async_copy(src, dst, in_sem.at[index])
        for index, (src, dst) in enumerate((
            (ids_hbm, ids_ref), (q_hbm.at[0], q_ref), (router_hbm, router_ref),
        ))
    ]
    own_copies = [
        pltpu.make_async_copy(
            src.at[0, :, lanes(head)], kv.at[ctx, head, which], own_sem
        )
        for head in range(kv_heads)
        for which, src in enumerate((k_hbm, v_hbm))
    ]
    w_copies = [
        pltpu.make_async_copy(src.at[0], dst, sem)
        for src, dst, sem in (
            (wg_hbm, wgu.at[0], w_sem.at[0]), (wu_hbm, wgu.at[1], w_sem.at[0]),
            (wd_hbm, wd, w_sem.at[1]),
        )
    ]
    for copy in in_copies[:2] + own_copies + in_copies[2:]:
        copy.start()

    barrier = pltpu.get_barrier_semaphore()

    def greet(other):
        @pl.when(other != me)
        def _():
            pl.semaphore_signal(
                barrier, inc=1,
                device_id={"ep": other // n_ctx, "ctx": other % n_ctx},
                device_id_type=MESH,
            )

    each(n, greet)
    for step in range(1, n_tp):
        pl.semaphore_signal(
            barrier, inc=1, device_id={"tp": (tp + step) % n_tp}, device_id_type=MESH
        )

    peer = {"tp": n_tp - 1 - tp}

    def settled(ref, sem):
        return pltpu.make_async_remote_copy(
            src_ref=ref, dst_ref=ref, send_sem=sem, recv_sem=sem,
            device_id=peer, device_id_type=MESH,
        )

    def by_ctx(body):
        for index in range(n_ctx):
            pl.when(ctx == index)(functools.partial(body, index))

    def kv_copies(block, head):
        parts = [kv.at[block, head]]
        if head == kv_heads - 1:
            parts = [kv.at[block, head, 0], kv.at[block, head, 1]]
        return [
            pltpu.make_async_remote_copy(
                src_ref=part, dst_ref=part,
                send_sem=kv_send, recv_sem=kv_recv.at[block, head + index],
                device_id={"ctx": ctx + 1}, device_id_type=MESH,
            )
            for index, part in enumerate(parts)
        ]

    def push_own(heads):
        @pl.when(ctx < last)
        def _():
            for head in heads:
                for copy in kv_copies(ctx, head):
                    copy.start()

    def relay(block, heads):
        @pl.when((block >= 0) & (ctx < last))
        def _():
            for head in heads:
                for copy in kv_copies(block, head):
                    copy.wait_recv()
                    copy.start()

    def arrive(block, heads):
        for head in heads:
            for copy in kv_copies(block, head):
                copy.wait_recv()

    def q_copy(source, target):
        return pltpu.make_async_remote_copy(
            src_ref=q_out, dst_ref=q_in.at[source],
            send_sem=q_send, recv_sem=q_recv.at[source],
            device_id={"ctx": target}, device_id_type=MESH,
        )

    def back_copies(target):
        slot = jnp.where(target == last, n_ctx, 0) + ctx
        return [
            pltpu.make_async_remote_copy(
                src_ref=out.at[target], dst_ref=into.at[slot],
                send_sem=sent, recv_sem=got,
                device_id={"ctx": jnp.minimum(target, home)}, device_id_type=MESH,
            )
            for out, into, sent, got in (
                (part_out, part_got, back_send, back_recv),
                (lse_out, lse_in, lse_send, lse_recv),
            )
        ]

    def to_index(other, out, into, sent, got, source):
        return pltpu.make_async_remote_copy(
            src_ref=out, dst_ref=into.at[source],
            send_sem=sent, recv_sem=got,
            device_id={"ep": other // n_ctx, "ctx": other % n_ctx}, device_id_type=MESH,
        )

    def row_copy(other, which):
        got = row_recv.at[jnp.where(ctx == 0, 0, 1)]
        return to_index(
            other, out_rows.at[which, other // n_ctx], in_rows, row_send.at[which], got, me + which
        )

    def down_copy(other, source):
        return to_index(other, down_out.at[other], down_in, down_send, down_recv, source)

    def lower(body):
        def one(other):
            @pl.when(other < ctx)
            def _():
                body(other)

        each(n_ctx, one)

    def upper(body):
        def one(step):
            other = last - step

            @pl.when(other > ctx)
            def _():
                body(other)

        each(n_ctx, one)

    def others(body):
        def one(other):
            @pl.when(other != me)
            def _():
                body(other)

        each(n, one)

    def first_owners(body):
        def one(expert):
            @pl.when(expert * n_ctx != me)
            def _():
                body(expert * n_ctx)

        each(n_ep, one)

    def later_owners(body):
        def one(other):
            @pl.when((other % n_ctx != 0) & (other != me))
            def _():
                body(other)

        each(n, one)

    with scope("a_ids"):
        in_copies[0].wait()
    with scope("a_pick"):
        ids = ids_ref[...]
        slot_row = lax.broadcasted_iota(jnp.int32, (slots, rows), 0)
        choose = jnp.where(ids == slot_row, 1.0, 0.0)
        below = lax.broadcasted_iota(jnp.int32, (rows, rows), 0)
        across = lax.broadcasted_iota(jnp.int32, (rows, rows), 1)
        strict = jnp.where(below < across, 1.0, 0.0).astype(jnp.bfloat16)
        earlier = jnp.dot(
            choose.astype(jnp.bfloat16), strict, preferred_element_type=jnp.float32
        )
        slot_index = jnp.sum(earlier * choose, axis=0, keepdims=True).astype(jnp.int32)
        target_row = jnp.where(ids < n_ep, ids * CAP + slot_index, -1)
        spread = jnp.where(target_row == slot_row, 1.0, 0.0).astype(jnp.bfloat16)
        lane_row = lax.broadcasted_iota(jnp.int32, (slots, rows), 1)
        row_place = jnp.sum(
            jnp.where(target_row == slot_row, lane_row, 0), axis=1, keepdims=True
        )
        in_copies[1].wait()
        for copy in w_copies:
            copy.start()
        for start, size in tiles_of(features, 512):
            picked = jnp.dot(
                spread, q_ref[:, start:start + size], preferred_element_type=jnp.float32
            )
            q_own[:, start:start + size] = picked
            q_out[:, start:start + size] = picked[:live].astype(jnp.bfloat16)

    def attend(source, tall, seen):
        raws = []
        for head in range(kv_heads):
            stacked = jnp.concatenate(
                [source[:, lanes(head * group + j)] for j in range(group)], axis=0
            ).astype(jnp.bfloat16)
            raw = lax.dot_general(
                stacked, kv[ctx, head, 0], (((1,), (1,)), ((), ())),
                preferred_element_type=jnp.float32,
            )
            raws.append(raw if seen is None else jnp.where(seen, raw, MASKED))
        tops = [jnp.max(raw, axis=1, keepdims=True) for raw in raws]
        weights = [jnp.exp2((raw - top) * EXP2_SCALE) for raw, top in zip(raws, tops)]
        sums = [jnp.sum(weight, axis=1, keepdims=True) for weight in weights]
        mixed = [
            jnp.dot(
                weight.astype(jnp.bfloat16), kv[ctx, head, 1],
                preferred_element_type=jnp.float32,
            ) / total
            for head, (weight, total) in enumerate(zip(weights, sums))
        ]
        columns = [top * EXP2_SCALE + jnp.log2(total) for top, total in zip(tops, sums)]
        head_lane = lax.broadcasted_iota(jnp.int32, (tall, 128), 1)
        lse = jnp.zeros((tall, 128), jnp.float32)
        for head in range(kv_heads):
            for j in range(group):
                lse = jnp.where(
                    head_lane == head * group + j, columns[head][j * tall:(j + 1) * tall], lse
                )
        return mixed, lse

    def own_landed():
        pltpu.make_async_copy(kv.at[ctx], kv.at[ctx], own_sem).wait()

    def own_part():
        key_lane = lax.broadcasted_iota(jnp.int32, (group * slots, rows), 1)
        seen = key_lane <= jnp.concatenate([row_place] * group, axis=0)
        mixed, lse = attend(q_own, slots, seen)
        lse_all[...] = jnp.full_like(lse_all, MASKED)
        lse_all[0, ctx] = lse
        for head in range(kv_heads):
            for j in range(group):
                part_all[0, ctx, :, lanes(head * group + j)] = mixed[head][
                    j * slots:(j + 1) * slots
                ]

        return mixed, lse

    def put_row(which, place, picked):
        for expert in range(n_ep):
            out_rows[which, expert, place * CAP:(place + 1) * CAP] = picked[
                expert * CAP:(expert + 1) * CAP
            ].astype(jnp.bfloat16)

    def send_rows(which):
        others(lambda other: row_copy(other, which).start())
        in_rows[me + which] = out_rows[which, ep]

    part_all[...] = jnp.zeros_like(part_all)
    q_all[...] = jnp.zeros_like(q_all)

    @pl.when(ctx == 0)
    def _():
        with scope("b_own0"):
            own_landed()
            own_part()
            for place in range(places):
                put_row(0, place, part_all[0, 0, :, lanes(place)])

    with scope("c_barrier"):
        pl.semaphore_wait(barrier, n - 1 + n_tp - 1)

    with scope("d_qsend"):
        lower(lambda other: q_copy(ctx, other).start())

    @pl.when(ctx == 0)
    def _():
        with scope("e_rows0"):
            send_rows(0)
            push_own(range(1))

    @pl.when(ctx > 0)
    def _():
        with scope("f_own"):
            own_landed()
            push_own(range(2))
            pl.when(ctx > 1)(lambda: push_own(range(2, kv_heads)))
            mixed, lse = own_part()

            @pl.when(ctx == last)
            def _():
                lse_out[last] = lse[:live]
                for place in range(places):
                    first = place % group * slots
                    part_out[last, :, lanes(place)] = mixed[place // group][
                        first:first + live
                    ].astype(jnp.bfloat16)
                for copy in back_copies(last):
                    copy.start()

    query_offset = lax.broadcasted_iota(jnp.int32, (rows, rows), 0)
    key_offset = lax.broadcasted_iota(jnp.int32, (rows, rows), 1)

    def scores(block, head):
        stacked = jnp.concatenate(
            [q_ref[:, lanes(head * group + j)] for j in range(group)], axis=0
        )
        return lax.dot_general(
            stacked, kv[block, head, 0], (((1,), (1,)), ((), ())),
            preferred_element_type=jnp.float32,
        )

    def mix(weights, block, head):
        return jnp.dot(
            weights.astype(jnp.bfloat16), kv[block, head, 1], preferred_element_type=jnp.float32
        )

    with scope("g_own_block"):
        visible = jnp.concatenate([query_offset >= key_offset] * group, axis=0)
        for head in range(kv_heads):
            raw = jnp.where(visible, scores(ctx, head), MASKED)
            top = jnp.broadcast_to(jnp.max(raw, axis=1, keepdims=True), raw.shape)
            weights = jnp.exp2((raw - top) * EXP2_SCALE)
            row_max[head] = top
            totals[head] = jnp.broadcast_to(
                jnp.sum(weights, axis=1, keepdims=True), weights.shape
            )
            acc[head] = mix(weights, ctx, head)

    def process(block, head, before_values=None):
        raw = scores(block, head)
        old_max = row_max[head]
        new_max = jnp.maximum(old_max, jnp.max(raw, axis=1, keepdims=True))
        factor = jnp.exp2((old_max - new_max) * EXP2_SCALE)
        weights = jnp.exp2((raw - new_max) * EXP2_SCALE)
        row_max[head] = new_max
        totals[head] = totals[head] * factor + jnp.sum(weights, axis=1, keepdims=True)
        if before_values is not None:
            before_values()
        acc[head] = acc[head] * factor + mix(weights, block, head)

    def visit(step):
        pl.when(ctx == last)(lambda: arrive(ctx - step, range(kv_heads)))
        for head in range(kv_heads):
            process(ctx - step, head)

    def visit_by_head(step):
        for head in range(kv_heads):
            pl.when(ctx == last)(lambda: arrive(ctx - step, [head]))
            relay(ctx - step, [head])
            process(ctx - step, head)

    @pl.when(ctx < last)
    def _():
        with scope("h_qwait"):
            upper(lambda other: q_copy(other, other).wait_recv())
        with scope("i_qpart"):
            for other in range(n_ctx):
                @pl.when(other > ctx)
                def _():
                    q_all[other * live:(other + 1) * live, :] = q_in[other].astype(jnp.float32)

            tall = n_ctx * live
            mixed, lse = attend(q_all, tall, None)
            @pl.when(ctx == home)
            def _():
                lse_all[1, home, :live] = lse[last * live:]
                for place in range(places):
                    first = place % group * tall + last * live
                    part_all[1, home, :live, lanes(place)] = mixed[place // group][
                        first:first + live
                    ]

            for other in range(n_ctx):
                lse_out[other] = lse[other * live:(other + 1) * live]
                for place in range(places):
                    first = place % group * tall + other * live
                    part_out[other, :, lanes(place)] = mixed[place // group][
                        first:first + live
                    ].astype(jnp.bfloat16)

        with scope("j_give"):
            def give_back(other):
                for copy in back_copies(other):
                    copy.start()

            pl.when(ctx < home)(lambda: upper(give_back))
            pl.when(ctx == 0)(lambda: push_own(range(1, kv_heads)))
    def gate(indices, wide_ref, part, part_in, sent, got, between):
        for at, index in enumerate(indices):
            dense = in_rows[index].astype(jnp.float32)
            for place in range(places):
                wide_ref[at * CAP:(at + 1) * CAP, lanes(place)] = dense[
                    place * CAP:(place + 1) * CAP
                ]
        wide = wide_ref[...]
        members = wide.astype(jnp.bfloat16)
        own_score = jnp.sum(wide * router_ref[...].astype(jnp.float32), axis=1, keepdims=True)
        chunks, _, double_width = part.shape
        width = double_width // 2
        for chunk in range(chunks):
            if chunk == 0:
                part[0] = jnp.broadcast_to(own_score, part.shape[1:]).astype(jnp.bfloat16)
            else:
                span = slice((chunk - 1) * width, chunk * width)
                for side in range(2):
                    part[chunk, :, side * width:(side + 1) * width] = jnp.dot(
                        members, wgu[side, :, span], preferred_element_type=jnp.float32
                    ).astype(jnp.bfloat16)
            which = chunk // (chunks - 1)
            pltpu.make_async_remote_copy(
                src_ref=part.at[chunk], dst_ref=part_in.at[chunk],
                send_sem=sent, recv_sem=got.at[which],
                device_id=peer, device_id_type=MESH,
            ).start()
            between(chunk, chunks - 1)

    def activate(part, part_in, sent, got, hidden):
        chunks = part.shape[0]
        width = part.shape[2] // 2
        settled(part_in.at[pl.ds(0, chunks - 1)], got.at[0]).wait_recv()
        gain = jax.nn.sigmoid(
            part[0, :, :1].astype(jnp.float32) + part_in[0, :, :1].astype(jnp.float32)
        )
        for chunk in range(1, chunks):
            if chunk == chunks - 1:
                settled(part_in.at[chunk], got.at[1]).wait_recv()
            both = part[chunk].astype(jnp.float32) + part_in[chunk].astype(jnp.float32)
            gate_part = gain * both[:, :width]
            up_part = gain * both[:, width:]
            hidden[:, (chunk - 1) * width:chunk * width] = (
                gate_part * jax.nn.sigmoid(gate_part) * up_part
            ).astype(jnp.bfloat16)

    def down(indices, hidden):
        for start, size in tiles_of(features, 512):
            product = jnp.dot(
                hidden[...], wd[:, start:start + size], preferred_element_type=jnp.float32
            )
            for at, index in enumerate(indices):
                for place in range(start // HEAD_WIDTH, (start + size) // HEAD_WIDTH):
                    lane = place * HEAD_WIDTH - start
                    down_out[index, place * CAP:(place + 1) * CAP] = product[
                        at * CAP:(at + 1) * CAP, lane:lane + HEAD_WIDTH
                    ].astype(jnp.bfloat16)

    def keep_own():
        down_in[me] = down_out[me]

    first = [index for index in range(n) if index % n_ctx == 0]
    later = [index for index in range(n) if index % n_ctx != 0]
    exchange_a = (part_a, part_in_a, a_send, a_recv)
    exchange_b = (part_b, part_in_b, b_send, b_recv)

    with scope("l_rows_a"):
        in_copies[2].wait()
        pltpu.make_async_copy(wgu, wgu, w_sem.at[0]).wait()

        @pl.when(ctx == 0)
        def _():
            if n_ep > 1:
                settled(in_rows.at[pl.ds(0, n_ep - 1)], row_recv.at[0]).wait_recv()

        @pl.when(ctx > 0)
        def _():
            settled(in_rows.at[pl.ds(0, n_ep)], row_recv.at[0]).wait_recv()
    def between_a(chunk, count):
        if chunk == (count + 1) // 2:
            pl.when(ctx == 1)(lambda: push_own(range(2, kv_heads)))
            pl.when(ctx > 1)(lambda: relay(ctx - 1, [0]))

    def between_b(chunk, count):
        if chunk == (count + 1) // 2:
            relay(ctx - 2, [0])

    with scope("m_gate_a"):
        gate(first, members_a, *exchange_a, between_a)

    def combine(which):
        peak = jnp.max(lse_all[which], axis=0)
        shares = [jnp.exp2(lse_all[which, other] - peak) for other in range(n_ctx)]
        share_total = functools.reduce(jnp.add, shares)
        shares = [share / share_total for share in shares]
        for place in range(places):
            put_row(which, place, functools.reduce(jnp.add, [
                shares[other][:, place:place + 1] * part_all[which, other, :, lanes(place)]
                for other in range(n_ctx)
            ]))

    def take(which, other):
        slot = which * n_ctx + other
        part_all[which, other, :live] = part_got[slot].astype(jnp.float32)
        lse_all[which, other, :live] = lse_in[slot]

    @pl.when((ctx > 0) & (ctx < last))
    def _():
        with scope("o_takeback"):
            def take_back(count):
                if 0 < count < last:
                    count = 2 * count + 1 if count == home else count
                    settled(part_got.at[pl.ds(0, count)], back_recv).wait_recv()
                    settled(lse_in.at[pl.ds(0, count)], lse_recv).wait_recv()

            by_ctx(take_back)
        with scope("p_combine"):
            for other in range(home):
                pl.when(other < ctx)(functools.partial(take, 0, other))

            @pl.when(ctx == home)
            def _():
                for other in range(n_ctx):
                    if other != home:
                        take(1, other)
                combine(1)
                send_rows(1)

            combine(0)
        with scope("q_rows"):
            send_rows(0)
            pl.when(ctx == 1)(lambda: relay(ctx - 1, [0]))
            pl.when(ctx > 1)(lambda: relay(ctx - 1, [1]))

    with scope("r_down_a"):
        w_copies[2].wait()
        activate(*exchange_a, hidden_a)
        down(first, hidden_a)
        first_owners(lambda other: down_copy(other, me).start())
        pl.when(ctx == 0)(keep_own)
    with scope("s_relay"):
        pl.when(ctx == 1)(lambda: relay(ctx - 1, range(1, kv_heads)))
        pl.when(ctx > 1)(lambda: relay(ctx - 1, range(2, kv_heads)))
    with scope("t_block1"):
        pl.when(ctx > 1)(lambda: visit(1))
    with scope("v_rows_b"):
        @pl.when((ctx == 0) | (ctx == last))
        def _():
            settled(in_rows.at[pl.ds(0, n - n_ep)], row_recv.at[1]).wait_recv()

        @pl.when((ctx > 0) & (ctx < home))
        def _():
            settled(in_rows.at[pl.ds(0, n - n_ep - 1)], row_recv.at[1]).wait_recv()

        @pl.when(ctx == home)
        def _():
            settled(in_rows.at[pl.ds(0, n - n_ep - 2)], row_recv.at[1]).wait_recv()

    with scope("w_gate_b"):
        gate(later, members_b, *exchange_b, between_b)
    ahead = tp == n_tp - 1
    early = ahead & (ctx > 2)
    with scope("x_relay"):
        relay(ctx - 2, [1])
        pl.when(ahead)(lambda: relay(ctx - 2, range(2, kv_heads)))
    with scope("xa_block2"):
        pl.when(early)(lambda: visit(2))
    with scope("xb_down_b"):
        activate(*exchange_b, hidden_b)
        down(later, hidden_b)
        later_owners(lambda other: down_copy(other, me).start())
        pl.when(ctx > 0)(keep_own)

    def remaining(step, carry):
        pl.when(ctx >= step)(lambda: visit_by_head(step))
        return carry

    def norm(head):
        normed = (acc[head] / totals[head]).astype(jnp.bfloat16)
        for j in range(group):
            att[:, lanes(head * group + j)] = normed[j * rows:(j + 1) * rows]

    def settle_down():
        settled(down_in.at[pl.ds(0, n - 1)], down_recv).wait_recv()
        returned[...] = jnp.zeros_like(returned)
        for expert in range(n_ep):
            total = down_in[expert * n_ctx].astype(jnp.float32)
            for index in range(1, n_ctx):
                total = total + down_in[expert * n_ctx + index].astype(jnp.float32)
            total = total.astype(jnp.bfloat16).astype(jnp.float32)
            for place in range(places):
                returned[expert * CAP:(expert + 1) * CAP, lanes(place)] = total[
                    place * CAP:(place + 1) * CAP
                ]

    def finish(head):
        width = group * HEAD_WIDTH
        span = slice(head * width, (head + 1) * width)
        routed = lax.dot_general(
            spread, returned[:, span].astype(jnp.bfloat16),
            (((0,), (0,)), ((), ())), preferred_element_type=jnp.float32,
        )
        out_ref[0, :, span] = (att[:, span].astype(jnp.float32) + routed).astype(jnp.bfloat16)

    with scope("xc_visit"):
        pl.when(jnp.logical_not(ahead))(lambda: relay(ctx - 2, range(2, kv_heads)))
        left = jnp.where(ctx == 1, 1, 2)

        @pl.when((ctx > 0) & jnp.logical_not(early))
        def _():
            visit(left)

    ends = (ctx == last) & (last > 2)

    @pl.when(ends)
    def _():
        with scope("xd_visit"):
            lax.fori_loop(3, last, remaining, 0)

            def arrived(head):
                first, *rest = kv_copies(0, head)
                first.wait_recv()
                process(0, head, rest[0].wait_recv if rest else None)
                norm(head)

            for head in range(kv_heads - 1):
                arrived(head)
        with scope("xe_down"):
            settle_down()
            for head in range(kv_heads - 1):
                finish(head)
        with scope("xf_last"):
            arrived(kv_heads - 1)
            finish(kv_heads - 1)

    @pl.when(jnp.logical_not(ends))
    def _():
        lax.fori_loop(3, n_ctx, remaining, 0)
        with scope("xd_norm"):
            for head in range(kv_heads):
                norm(head)
        with scope("xe_down"):
            settle_down()
        with scope("xg_final"):
            for head in range(kv_heads):
                finish(head)

    with scope("xh_sent"):
        settled(part_a, a_send).wait_send()
        settled(part_b, b_send).wait_send()

        def drain(index):
            if index:
                settled(q_in.at[pl.ds(0, index)], q_send).wait_send()
            given = {home: 0, last: 1}.get(index, last - index)
            if given:
                settled(part_out.at[pl.ds(0, given)], back_send).wait_send()
                settled(lse_out.at[pl.ds(0, given)], lse_send).wait_send()
            for which in range({home: 2, last: 0}.get(index, 1)):
                settled(in_rows.at[pl.ds(0, n - 1)], row_send.at[which]).wait_send()
            if index < last:
                settled(kv.at[pl.ds(0, index + 1)], kv_send).wait_send()

        by_ctx(drain)
        settled(down_out.at[pl.ds(0, n - 1)], down_send).wait_send()


def shards(queries, keys, values, expert_ids, router, w_gate, w_up, w_down):
    n_ctx, n_ep, n_tp = (lax.axis_size(axis) for axis in ("ctx", "ep", "tp"))
    n = n_ctx * n_ep
    _, rows, features = queries.shape
    kv_width = keys.shape[2]
    kv_heads = kv_width // HEAD_WIDTH
    group = features // kv_width
    hidden_width = w_gate.shape[2]
    chunk_width = min(hidden_width, 256)
    chunks = hidden_width // chunk_width
    dense = features // HEAD_WIDTH * CAP
    live = n_ep * CAP
    slots = padded(live)
    bf16, f32 = jnp.bfloat16, jnp.float32
    hbm = pl.BlockSpec(memory_space=pltpu.HBM)
    dma = pltpu.SemaphoreType.DMA

    def batch(count):
        return [
            pltpu.VMEM((count, features), f32),
            pltpu.VMEM((chunks + 1, count, 2 * chunk_width), bf16),
            pltpu.VMEM((chunks + 1, count, 2 * chunk_width), bf16),
            pltpu.VMEM((count, hidden_width), bf16),
        ]

    return pl.pallas_call(
        functools.partial(kernel, n_ctx, n_ep, n_tp),
        out_shape=pltpu.VMEM(queries.shape, bf16),
        in_specs=[hbm] * 8,
        out_specs=pl.BlockSpec(memory_space=pltpu.VMEM),
        scratch_shapes=[
            pltpu.VMEM((1, rows), jnp.int32),
            pltpu.VMEM((1, features), bf16),
            pltpu.VMEM((rows, features), bf16),
            pltpu.VMEM((2, *w_gate.shape[1:]), bf16),
            pltpu.VMEM(w_down.shape[1:], bf16),
            pltpu.VMEM((n_ctx, kv_heads, 2, rows, HEAD_WIDTH), bf16),
            pltpu.VMEM((kv_heads, group * rows, HEAD_WIDTH), f32),
            pltpu.VMEM((kv_heads, group * rows, HEAD_WIDTH), f32),
            pltpu.VMEM((kv_heads, group * rows, HEAD_WIDTH), f32),
            pltpu.VMEM((rows, features), bf16),
            pltpu.VMEM((slots, features), f32),
            pltpu.VMEM((live, features), bf16),
            pltpu.VMEM((n_ctx, live, features), bf16),
            pltpu.VMEM((n_ctx * live, features), f32),
            pltpu.VMEM((n_ctx, live, features), bf16),
            pltpu.VMEM((2 * n_ctx, live, features), bf16),
            pltpu.VMEM((2, n_ctx, slots, features), f32),
            pltpu.VMEM((n_ctx, live, 128), f32),
            pltpu.VMEM((2 * n_ctx, live, 128), f32),
            pltpu.VMEM((2, n_ctx, slots, 128), f32),
            pltpu.VMEM((2, n_ep, dense, HEAD_WIDTH), bf16),
            pltpu.VMEM((n, dense, HEAD_WIDTH), bf16),
            *batch(n_ep * CAP),
            *batch((n - n_ep) * CAP),
            pltpu.VMEM((n, dense, HEAD_WIDTH), bf16),
            pltpu.VMEM((n, dense, HEAD_WIDTH), bf16),
            pltpu.VMEM((slots, features), f32),
            dma((3,)),
            dma,
            dma((2,)),
            dma,
            dma((n_ctx - 1, kv_heads + 1)),
            dma((2,)),
            dma((2,)),
            dma,
            dma((2,)),
            dma,
            dma((2,)),
            dma,
            dma,
            dma,
            dma((n_ctx,)),
            *[dma] * 4,
        ],
        compiler_params=pltpu.CompilerParams(
            collective_id=0, has_side_effects=True, vmem_limit_bytes=60 * 1024 * 1024
        ),
    )(
        expert_ids.reshape(1, rows), router.reshape(1, features), queries, keys, values,
        w_gate, w_up, w_down,
    )


def solution(mesh):
    placed = (
        P(("groups", "ep"), "ctx", "tp"),
        P(("groups", "ep"), "ctx", "tp"),
        P(("groups", "ep"), "ctx", "tp"),
        P(("groups", "ep"), "ctx", None),
        P("tp", "ep"),
        P("ep", "tp", "ctx"),
        P("ep", "tp", "ctx"),
        P("ep", "ctx", "tp"),
    )
    return jax.shard_map(
        shards,
        mesh=mesh,
        in_specs=placed,
        out_specs=P(("groups", "ep"), "ctx", "tp"),
        check_vma=False,
    )
```

```python
import functools
import math

import jax
import jax.numpy as jnp
from jax import lax
from jax.experimental import pallas as pl
from jax.experimental.pallas import tpu as pltpu
from jax.sharding import PartitionSpec as P

HEAD_WIDTH = 128
CAP = 2
MESH = pl.DeviceIdType.MESH
MASKED = -1e30
EXP2_SCALE = HEAD_WIDTH ** (-0.5) * math.log2(math.e)
scope = jax.named_scope


def tiles_of(width, tile):
    tile = min(width, tile)
    return [(start, min(tile, width - start)) for start in range(0, width, tile)]


def padded(count, tile=8):
    return -(-count // tile) * tile


def each(count, body):
    if count <= 8:
        for index in range(count):
            body(index)
    else:
        pl.loop(0, count)(body)


def kernel(
    n_ctx, n_ep, n_tp,
    ids_hbm, router_hbm, q_hbm, k_hbm, v_hbm, wg_hbm, wu_hbm, wd_hbm,
    out_ref,
    ids_ref, router_ref, q_ref, wgu, wd, kv, acc, row_max, totals, att,
    q_own, q_out, q_in, q_all, part_out, part_got, part_all, lse_out, lse_in, lse_all,
    out_rows, in_rows,
    members_a, part_a, part_in_a, hidden_a,
    members_b, part_b, part_in_b, hidden_b,
    down_out, down_in, returned,
    in_sem, own_sem, w_sem, kv_send, kv_recv, row_send, row_recv,
    a_send, a_recv, b_send, b_recv,
    down_send, down_recv, q_send, q_recv, back_send, back_recv, lse_send, lse_recv,
):
    ctx = lax.axis_index("ctx")
    ep = lax.axis_index("ep")
    tp = lax.axis_index("tp")
    n = n_ctx * n_ep
    me = ep * n_ctx + ctx
    last = n_ctx - 1
    home = last - 1
    rows, features = q_ref.shape
    kv_heads = kv.shape[1]
    places = features // HEAD_WIDTH
    group = places // kv_heads
    slots = returned.shape[0]
    live = n_ep * CAP

    def lanes(place):
        return slice(place * HEAD_WIDTH, (place + 1) * HEAD_WIDTH)

    in_copies = [
        pltpu.make_async_copy(src, dst, in_sem.at[index])
        for index, (src, dst) in enumerate((
            (ids_hbm, ids_ref), (q_hbm.at[0], q_ref), (router_hbm, router_ref),
        ))
    ]
    own_copies = [
        pltpu.make_async_copy(
            src.at[0, :, lanes(head)], kv.at[ctx, head, which], own_sem
        )
        for head in range(kv_heads)
        for which, src in enumerate((k_hbm, v_hbm))
    ]
    w_copies = [
        pltpu.make_async_copy(src.at[0], dst, sem)
        for src, dst, sem in (
            (wg_hbm, wgu.at[0], w_sem.at[0]), (wu_hbm, wgu.at[1], w_sem.at[0]),
            (wd_hbm, wd, w_sem.at[1]),
        )
    ]
    for copy in in_copies[:2] + own_copies + in_copies[2:]:
        copy.start()

    barrier = pltpu.get_barrier_semaphore()

    def greet(other):
        @pl.when(other != me)
        def _():
            pl.semaphore_signal(
                barrier, inc=1,
                device_id={"ep": other // n_ctx, "ctx": other % n_ctx},
                device_id_type=MESH,
            )

    each(n, greet)
    for step in range(1, n_tp):
        pl.semaphore_signal(
            barrier, inc=1, device_id={"tp": (tp + step) % n_tp}, device_id_type=MESH
        )

    peer = {"tp": n_tp - 1 - tp}

    def settled(ref, sem):
        return pltpu.make_async_remote_copy(
            src_ref=ref, dst_ref=ref, send_sem=sem, recv_sem=sem,
            device_id=peer, device_id_type=MESH,
        )

    def by_ctx(body):
        for index in range(n_ctx):
            pl.when(ctx == index)(functools.partial(body, index))

    def kv_copies(block, head):
        parts = [kv.at[block, head]]
        if head == kv_heads - 1:
            parts = [kv.at[block, head, 0], kv.at[block, head, 1]]
        return [
            pltpu.make_async_remote_copy(
                src_ref=part, dst_ref=part,
                send_sem=kv_send, recv_sem=kv_recv.at[block, head + index],
                device_id={"ctx": ctx + 1}, device_id_type=MESH,
            )
            for index, part in enumerate(parts)
        ]

    def push_own(heads):
        @pl.when(ctx < last)
        def _():
            for head in heads:
                for copy in kv_copies(ctx, head):
                    copy.start()

    def relay(block, heads):
        @pl.when((block >= 0) & (ctx < last))
        def _():
            for head in heads:
                for copy in kv_copies(block, head):
                    copy.wait_recv()
                    copy.start()

    def arrive(block, heads):
        for head in heads:
            for copy in kv_copies(block, head):
                copy.wait_recv()

    def q_copy(source, target):
        return pltpu.make_async_remote_copy(
            src_ref=q_out, dst_ref=q_in.at[source],
            send_sem=q_send, recv_sem=q_recv.at[source],
            device_id={"ctx": target}, device_id_type=MESH,
        )

    def back_copies(target):
        slot = jnp.where(target == last, n_ctx, 0) + ctx
        return [
            pltpu.make_async_remote_copy(
                src_ref=out.at[target], dst_ref=into.at[slot],
                send_sem=sent, recv_sem=got,
                device_id={"ctx": jnp.minimum(target, home)}, device_id_type=MESH,
            )
            for out, into, sent, got in (
                (part_out, part_got, back_send, back_recv),
                (lse_out, lse_in, lse_send, lse_recv),
            )
        ]

    def to_index(other, out, into, sent, got, source):
        return pltpu.make_async_remote_copy(
            src_ref=out, dst_ref=into.at[source],
            send_sem=sent, recv_sem=got,
            device_id={"ep": other // n_ctx, "ctx": other % n_ctx}, device_id_type=MESH,
        )

    def row_copy(other, which):
        got = row_recv.at[jnp.where(ctx == 0, 0, 1)]
        return to_index(
            other, out_rows.at[which, other // n_ctx], in_rows, row_send.at[which], got, me + which
        )

    def down_copy(other, source):
        return to_index(other, down_out.at[other], down_in, down_send, down_recv, source)

    def lower(body):
        def one(other):
            @pl.when(other < ctx)
            def _():
                body(other)

        each(n_ctx, one)

    def upper(body):
        def one(step):
            other = last - step

            @pl.when(other > ctx)
            def _():
                body(other)

        each(n_ctx, one)

    def others(body):
        def one(other):
            @pl.when(other != me)
            def _():
                body(other)

        each(n, one)

    def first_owners(body):
        def one(expert):
            @pl.when(expert * n_ctx != me)
            def _():
                body(expert * n_ctx)

        each(n_ep, one)

    def later_owners(body):
        def one(other):
            @pl.when((other % n_ctx != 0) & (other != me))
            def _():
                body(other)

        each(n, one)

    with scope("a_ids"):
        in_copies[0].wait()
    with scope("a_pick"):
        ids = ids_ref[...]
        slot_row = lax.broadcasted_iota(jnp.int32, (slots, rows), 0)
        choose = jnp.where(ids == slot_row, 1.0, 0.0)
        below = lax.broadcasted_iota(jnp.int32, (rows, rows), 0)
        across = lax.broadcasted_iota(jnp.int32, (rows, rows), 1)
        strict = jnp.where(below < across, 1.0, 0.0).astype(jnp.bfloat16)
        earlier = jnp.dot(
            choose.astype(jnp.bfloat16), strict, preferred_element_type=jnp.float32
        )
        slot_index = jnp.sum(earlier * choose, axis=0, keepdims=True).astype(jnp.int32)
        target_row = jnp.where(ids < n_ep, ids * CAP + slot_index, -1)
        spread = jnp.where(target_row == slot_row, 1.0, 0.0).astype(jnp.bfloat16)
        lane_row = lax.broadcasted_iota(jnp.int32, (slots, rows), 1)
        row_place = jnp.sum(
            jnp.where(target_row == slot_row, lane_row, 0), axis=1, keepdims=True
        )
        in_copies[1].wait()
        for copy in w_copies:
            copy.start()
        for start, size in tiles_of(features, 512):
            picked = jnp.dot(
                spread, q_ref[:, start:start + size], preferred_element_type=jnp.float32
            )
            q_own[:, start:start + size] = picked
            q_out[:, start:start + size] = picked[:live].astype(jnp.bfloat16)

    def attend(source, tall, seen):
        raws = []
        for head in range(kv_heads):
            stacked = jnp.concatenate(
                [source[:, lanes(head * group + j)] for j in range(group)], axis=0
            ).astype(jnp.bfloat16)
            raw = lax.dot_general(
                stacked, kv[ctx, head, 0], (((1,), (1,)), ((), ())),
                preferred_element_type=jnp.float32,
            )
            raws.append(raw if seen is None else jnp.where(seen, raw, MASKED))
        tops = [jnp.max(raw, axis=1, keepdims=True) for raw in raws]
        weights = [jnp.exp2((raw - top) * EXP2_SCALE) for raw, top in zip(raws, tops)]
        sums = [jnp.sum(weight, axis=1, keepdims=True) for weight in weights]
        mixed = [
            jnp.dot(
                weight.astype(jnp.bfloat16), kv[ctx, head, 1],
                preferred_element_type=jnp.float32,
            ) / total
            for head, (weight, total) in enumerate(zip(weights, sums))
        ]
        columns = [top * EXP2_SCALE + jnp.log2(total) for top, total in zip(tops, sums)]
        head_lane = lax.broadcasted_iota(jnp.int32, (tall, 128), 1)
        lse = jnp.zeros((tall, 128), jnp.float32)
        for head in range(kv_heads):
            for j in range(group):
                lse = jnp.where(
                    head_lane == head * group + j, columns[head][j * tall:(j + 1) * tall], lse
                )
        return mixed, lse

    def own_landed():
        pltpu.make_async_copy(kv.at[ctx], kv.at[ctx], own_sem).wait()

    def own_part():
        key_lane = lax.broadcasted_iota(jnp.int32, (group * slots, rows), 1)
        seen = key_lane <= jnp.concatenate([row_place] * group, axis=0)
        mixed, lse = attend(q_own, slots, seen)
        lse_all[...] = jnp.full_like(lse_all, MASKED)
        lse_all[0, ctx] = lse
        for head in range(kv_heads):
            for j in range(group):
                part_all[0, ctx, :, lanes(head * group + j)] = mixed[head][
                    j * slots:(j + 1) * slots
                ]

        return mixed, lse

    def put_row(which, place, picked):
        for expert in range(n_ep):
            out_rows[which, expert, place * CAP:(place + 1) * CAP] = picked[
                expert * CAP:(expert + 1) * CAP
            ].astype(jnp.bfloat16)

    def send_rows(which):
        others(lambda other: row_copy(other, which).start())
        in_rows[me + which] = out_rows[which, ep]

    part_all[...] = jnp.zeros_like(part_all)
    q_all[...] = jnp.zeros_like(q_all)

    @pl.when(ctx == 0)
    def _():
        with scope("b_own0"):
            own_landed()
            own_part()
            for place in range(places):
                put_row(0, place, part_all[0, 0, :, lanes(place)])

    with scope("c_barrier"):
        pl.semaphore_wait(barrier, n - 1 + n_tp - 1)

    with scope("d_qsend"):
        lower(lambda other: q_copy(ctx, other).start())

    @pl.when(ctx == 0)
    def _():
        with scope("e_rows0"):
            send_rows(0)
            push_own(range(1))

    @pl.when(ctx > 0)
    def _():
        with scope("f_own"):
            own_landed()
            push_own(range(2))
            pl.when(ctx > 1)(lambda: push_own(range(2, kv_heads)))
            mixed, lse = own_part()

            @pl.when(ctx == last)
            def _():
                lse_out[last] = lse[:live]
                for place in range(places):
                    first = place % group * slots
                    part_out[last, :, lanes(place)] = mixed[place // group][
                        first:first + live
                    ].astype(jnp.bfloat16)
                for copy in back_copies(last):
                    copy.start()

    query_offset = lax.broadcasted_iota(jnp.int32, (rows, rows), 0)
    key_offset = lax.broadcasted_iota(jnp.int32, (rows, rows), 1)

    def scores(block, head):
        stacked = jnp.concatenate(
            [q_ref[:, lanes(head * group + j)] for j in range(group)], axis=0
        )
        return lax.dot_general(
            stacked, kv[block, head, 0], (((1,), (1,)), ((), ())),
            preferred_element_type=jnp.float32,
        )

    def mix(weights, block, head):
        return jnp.dot(
            weights.astype(jnp.bfloat16), kv[block, head, 1], preferred_element_type=jnp.float32
        )

    with scope("g_own_block"):
        visible = jnp.concatenate([query_offset >= key_offset] * group, axis=0)
        for head in range(kv_heads):
            raw = jnp.where(visible, scores(ctx, head), MASKED)
            top = jnp.broadcast_to(jnp.max(raw, axis=1, keepdims=True), raw.shape)
            weights = jnp.exp2((raw - top) * EXP2_SCALE)
            row_max[head] = top
            totals[head] = jnp.broadcast_to(
                jnp.sum(weights, axis=1, keepdims=True), weights.shape
            )
            acc[head] = mix(weights, ctx, head)

    def process(block, head, before_values=None):
        raw = scores(block, head)
        old_max = row_max[head]
        new_max = jnp.maximum(old_max, jnp.max(raw, axis=1, keepdims=True))
        factor = jnp.exp2((old_max - new_max) * EXP2_SCALE)
        weights = jnp.exp2((raw - new_max) * EXP2_SCALE)
        row_max[head] = new_max
        totals[head] = totals[head] * factor + jnp.sum(weights, axis=1, keepdims=True)
        if before_values is not None:
            before_values()
        acc[head] = acc[head] * factor + mix(weights, block, head)

    def visit(step):
        pl.when(ctx == last)(lambda: arrive(ctx - step, range(kv_heads)))
        for head in range(kv_heads):
            process(ctx - step, head)

    def visit_by_head(step):
        for head in range(kv_heads):
            pl.when(ctx == last)(lambda: arrive(ctx - step, [head]))
            relay(ctx - step, [head])
            process(ctx - step, head)

    @pl.when(ctx < last)
    def _():
        with scope("h_qwait"):
            upper(lambda other: q_copy(other, other).wait_recv())
        with scope("i_qpart"):
            for other in range(n_ctx):
                @pl.when(other > ctx)
                def _():
                    q_all[other * live:(other + 1) * live, :] = q_in[other].astype(jnp.float32)

            tall = n_ctx * live
            mixed, lse = attend(q_all, tall, None)
            @pl.when(ctx == home)
            def _():
                lse_all[1, home, :live] = lse[last * live:]
                for place in range(places):
                    first = place % group * tall + last * live
                    part_all[1, home, :live, lanes(place)] = mixed[place // group][
                        first:first + live
                    ]

            for other in range(n_ctx):
                lse_out[other] = lse[other * live:(other + 1) * live]
                for place in range(places):
                    first = place % group * tall + other * live
                    part_out[other, :, lanes(place)] = mixed[place // group][
                        first:first + live
                    ].astype(jnp.bfloat16)

        with scope("j_give"):
            def give_back(other):
                for copy in back_copies(other):
                    copy.start()

            pl.when(ctx < home)(lambda: upper(give_back))
            pl.when(ctx == 0)(lambda: push_own(range(1, kv_heads)))
    def gate(indices, wide_ref, part, part_in, sent, got, between):
        for at, index in enumerate(indices):
            dense = in_rows[index].astype(jnp.float32)
            for place in range(places):
                wide_ref[at * CAP:(at + 1) * CAP, lanes(place)] = dense[
                    place * CAP:(place + 1) * CAP
                ]
        wide = wide_ref[...]
        members = wide.astype(jnp.bfloat16)
        own_score = jnp.sum(wide * router_ref[...].astype(jnp.float32), axis=1, keepdims=True)
        chunks, _, double_width = part.shape
        width = double_width // 2
        for chunk in range(chunks):
            if chunk == 0:
                part[0] = jnp.broadcast_to(own_score, part.shape[1:]).astype(jnp.bfloat16)
            else:
                span = slice((chunk - 1) * width, chunk * width)
                for side in range(2):
                    part[chunk, :, side * width:(side + 1) * width] = jnp.dot(
                        members, wgu[side, :, span], preferred_element_type=jnp.float32
                    ).astype(jnp.bfloat16)
            which = chunk // (chunks - 1)
            pltpu.make_async_remote_copy(
                src_ref=part.at[chunk], dst_ref=part_in.at[chunk],
                send_sem=sent, recv_sem=got.at[which],
                device_id=peer, device_id_type=MESH,
            ).start()
            between(chunk, chunks - 1)

    def activate(part, part_in, sent, got, hidden):
        chunks = part.shape[0]
        width = part.shape[2] // 2
        settled(part_in.at[pl.ds(0, chunks - 1)], got.at[0]).wait_recv()
        gain = jax.nn.sigmoid(
            part[0, :, :1].astype(jnp.float32) + part_in[0, :, :1].astype(jnp.float32)
        )
        for chunk in range(1, chunks):
            if chunk == chunks - 1:
                settled(part_in.at[chunk], got.at[1]).wait_recv()
            both = part[chunk].astype(jnp.float32) + part_in[chunk].astype(jnp.float32)
            gate_part = gain * both[:, :width]
            up_part = gain * both[:, width:]
            hidden[:, (chunk - 1) * width:chunk * width] = (
                gate_part * jax.nn.sigmoid(gate_part) * up_part
            ).astype(jnp.bfloat16)

    def down(indices, hidden):
        for start, size in tiles_of(features, 512):
            product = jnp.dot(
                hidden[...], wd[:, start:start + size], preferred_element_type=jnp.float32
            )
            for at, index in enumerate(indices):
                for place in range(start // HEAD_WIDTH, (start + size) // HEAD_WIDTH):
                    lane = place * HEAD_WIDTH - start
                    down_out[index, place * CAP:(place + 1) * CAP] = product[
                        at * CAP:(at + 1) * CAP, lane:lane + HEAD_WIDTH
                    ].astype(jnp.bfloat16)

    def keep_own():
        down_in[me] = down_out[me]

    first = [index for index in range(n) if index % n_ctx == 0]
    later = [index for index in range(n) if index % n_ctx != 0]
    exchange_a = (part_a, part_in_a, a_send, a_recv)
    exchange_b = (part_b, part_in_b, b_send, b_recv)

    with scope("l_rows_a"):
        in_copies[2].wait()
        pltpu.make_async_copy(wgu, wgu, w_sem.at[0]).wait()

        @pl.when(ctx == 0)
        def _():
            if n_ep > 1:
                settled(in_rows.at[pl.ds(0, n_ep - 1)], row_recv.at[0]).wait_recv()

        @pl.when(ctx > 0)
        def _():
            settled(in_rows.at[pl.ds(0, n_ep)], row_recv.at[0]).wait_recv()
    def between_a(chunk, count):
        if chunk == (count + 1) // 2:
            pl.when(ctx == 1)(lambda: push_own(range(2, kv_heads)))
            pl.when(ctx > 1)(lambda: relay(ctx - 1, [0]))

    def between_b(chunk, count):
        if chunk == (count + 1) // 2:
            relay(ctx - 2, [0])

    with scope("m_gate_a"):
        gate(first, members_a, *exchange_a, between_a)

    def combine(which):
        peak = jnp.max(lse_all[which], axis=0)
        shares = [jnp.exp2(lse_all[which, other] - peak) for other in range(n_ctx)]
        share_total = functools.reduce(jnp.add, shares)
        shares = [share / share_total for share in shares]
        for place in range(places):
            put_row(which, place, functools.reduce(jnp.add, [
                shares[other][:, place:place + 1] * part_all[which, other, :, lanes(place)]
                for other in range(n_ctx)
            ]))

    def take(which, other):
        slot = which * n_ctx + other
        part_all[which, other, :live] = part_got[slot].astype(jnp.float32)
        lse_all[which, other, :live] = lse_in[slot]

    @pl.when((ctx > 0) & (ctx < last))
    def _():
        with scope("o_takeback"):
            def take_back(count):
                if 0 < count < last:
                    count = 2 * count + 1 if count == home else count
                    settled(part_got.at[pl.ds(0, count)], back_recv).wait_recv()
                    settled(lse_in.at[pl.ds(0, count)], lse_recv).wait_recv()

            by_ctx(take_back)
        with scope("p_combine"):
            for other in range(home):
                pl.when(other < ctx)(functools.partial(take, 0, other))

            @pl.when(ctx == home)
            def _():
                for other in range(n_ctx):
                    if other != home:
                        take(1, other)
                combine(1)
                send_rows(1)

            combine(0)
        with scope("q_rows"):
            send_rows(0)
            pl.when(ctx == 1)(lambda: relay(ctx - 1, [0]))
            pl.when(ctx > 1)(lambda: relay(ctx - 1, [1]))

    with scope("r_down_a"):
        w_copies[2].wait()
        activate(*exchange_a, hidden_a)
        down(first, hidden_a)
        first_owners(lambda other: down_copy(other, me).start())
        pl.when(ctx == 0)(keep_own)
    with scope("s_relay"):
        pl.when(ctx == 1)(lambda: relay(ctx - 1, range(1, kv_heads)))
        pl.when(ctx > 1)(lambda: relay(ctx - 1, range(2, kv_heads)))
    with scope("t_block1"):
        pl.when(ctx > 1)(lambda: visit(1))
    with scope("v_rows_b"):
        @pl.when((ctx == 0) | (ctx == last))
        def _():
            settled(in_rows.at[pl.ds(0, n - n_ep)], row_recv.at[1]).wait_recv()

        @pl.when((ctx > 0) & (ctx < home))
        def _():
            settled(in_rows.at[pl.ds(0, n - n_ep - 1)], row_recv.at[1]).wait_recv()

        @pl.when(ctx == home)
        def _():
            settled(in_rows.at[pl.ds(0, n - n_ep - 2)], row_recv.at[1]).wait_recv()

    with scope("w_gate_b"):
        gate(later, members_b, *exchange_b, between_b)
    ahead = tp == n_tp - 1
    early = ahead & (ctx > 2)
    with scope("x_relay"):
        relay(ctx - 2, [1])
        pl.when(ahead)(lambda: relay(ctx - 2, range(2, kv_heads)))
    with scope("xa_block2"):
        pl.when(early)(lambda: visit(2))
    with scope("xb_down_b"):
        activate(*exchange_b, hidden_b)
        down(later, hidden_b)
        later_owners(lambda other: down_copy(other, me).start())
        pl.when(ctx > 0)(keep_own)

    def remaining(step, carry):
        pl.when(ctx >= step)(lambda: visit_by_head(step))
        return carry

    def norm(head):
        normed = (acc[head] / totals[head]).astype(jnp.bfloat16)
        for j in range(group):
            att[:, lanes(head * group + j)] = normed[j * rows:(j + 1) * rows]

    def settle_down():
        settled(down_in.at[pl.ds(0, n - 1)], down_recv).wait_recv()
        returned[...] = jnp.zeros_like(returned)
        for expert in range(n_ep):
            total = down_in[expert * n_ctx].astype(jnp.float32)
            for index in range(1, n_ctx):
                total = total + down_in[expert * n_ctx + index].astype(jnp.float32)
            total = total.astype(jnp.bfloat16).astype(jnp.float32)
            for place in range(places):
                returned[expert * CAP:(expert + 1) * CAP, lanes(place)] = total[
                    place * CAP:(place + 1) * CAP
                ]

    def finish(head):
        width = group * HEAD_WIDTH
        span = slice(head * width, (head + 1) * width)
        routed = lax.dot_general(
            spread, returned[:, span].astype(jnp.bfloat16),
            (((0,), (0,)), ((), ())), preferred_element_type=jnp.float32,
        )
        out_ref[0, :, span] = (att[:, span].astype(jnp.float32) + routed).astype(jnp.bfloat16)

    with scope("xc_visit"):
        pl.when(jnp.logical_not(ahead))(lambda: relay(ctx - 2, range(2, kv_heads)))
        left = jnp.where(ctx == 1, 1, 2)

        @pl.when((ctx > 0) & jnp.logical_not(early))
        def _():
            visit(left)

    ends = (ctx == last) & (last > 2)

    @pl.when(ends)
    def _():
        with scope("xd_visit"):
            lax.fori_loop(3, last, remaining, 0)

            def arrived(head):
                first, *rest = kv_copies(0, head)
                first.wait_recv()
                process(0, head, rest[0].wait_recv if rest else None)
                norm(head)

            def run(before):
                for head in range(before):
                    arrived(head)
                settle_down()
                for head in range(before):
                    finish(head)
                for head in range(before, kv_heads):
                    arrived(head)
                    finish(head)

            pl.when(ahead)(lambda: run(kv_heads))
            pl.when(jnp.logical_not(ahead))(lambda: run(kv_heads - 2))

    @pl.when(jnp.logical_not(ends))
    def _():
        lax.fori_loop(3, n_ctx, remaining, 0)
        with scope("xd_norm"):
            for head in range(kv_heads):
                norm(head)
        with scope("xe_down"):
            settle_down()
        with scope("xg_final"):
            for head in range(kv_heads):
                finish(head)

    with scope("xh_sent"):
        settled(part_a, a_send).wait_send()
        settled(part_b, b_send).wait_send()

        def drain(index):
            if index:
                settled(q_in.at[pl.ds(0, index)], q_send).wait_send()
            given = {home: 0, last: 1}.get(index, last - index)
            if given:
                settled(part_out.at[pl.ds(0, given)], back_send).wait_send()
                settled(lse_out.at[pl.ds(0, given)], lse_send).wait_send()
            for which in range({home: 2, last: 0}.get(index, 1)):
                settled(in_rows.at[pl.ds(0, n - 1)], row_send.at[which]).wait_send()
            if index < last:
                settled(kv.at[pl.ds(0, index + 1)], kv_send).wait_send()

        by_ctx(drain)
        settled(down_out.at[pl.ds(0, n - 1)], down_send).wait_send()


def shards(queries, keys, values, expert_ids, router, w_gate, w_up, w_down):
    n_ctx, n_ep, n_tp = (lax.axis_size(axis) for axis in ("ctx", "ep", "tp"))
    n = n_ctx * n_ep
    _, rows, features = queries.shape
    kv_width = keys.shape[2]
    kv_heads = kv_width // HEAD_WIDTH
    group = features // kv_width
    hidden_width = w_gate.shape[2]
    chunk_width = min(hidden_width, 256)
    chunks = hidden_width // chunk_width
    dense = features // HEAD_WIDTH * CAP
    live = n_ep * CAP
    slots = padded(live)
    bf16, f32 = jnp.bfloat16, jnp.float32
    hbm = pl.BlockSpec(memory_space=pltpu.HBM)
    dma = pltpu.SemaphoreType.DMA

    def batch(count):
        return [
            pltpu.VMEM((count, features), f32),
            pltpu.VMEM((chunks + 1, count, 2 * chunk_width), bf16),
            pltpu.VMEM((chunks + 1, count, 2 * chunk_width), bf16),
            pltpu.VMEM((count, hidden_width), bf16),
        ]

    return pl.pallas_call(
        functools.partial(kernel, n_ctx, n_ep, n_tp),
        out_shape=pltpu.VMEM(queries.shape, bf16),
        in_specs=[hbm] * 8,
        out_specs=pl.BlockSpec(memory_space=pltpu.VMEM),
        scratch_shapes=[
            pltpu.VMEM((1, rows), jnp.int32),
            pltpu.VMEM((1, features), bf16),
            pltpu.VMEM((rows, features), bf16),
            pltpu.VMEM((2, *w_gate.shape[1:]), bf16),
            pltpu.VMEM(w_down.shape[1:], bf16),
            pltpu.VMEM((n_ctx, kv_heads, 2, rows, HEAD_WIDTH), bf16),
            pltpu.VMEM((kv_heads, group * rows, HEAD_WIDTH), f32),
            pltpu.VMEM((kv_heads, group * rows, HEAD_WIDTH), f32),
            pltpu.VMEM((kv_heads, group * rows, HEAD_WIDTH), f32),
            pltpu.VMEM((rows, features), bf16),
            pltpu.VMEM((slots, features), f32),
            pltpu.VMEM((live, features), bf16),
            pltpu.VMEM((n_ctx, live, features), bf16),
            pltpu.VMEM((n_ctx * live, features), f32),
            pltpu.VMEM((n_ctx, live, features), bf16),
            pltpu.VMEM((2 * n_ctx, live, features), bf16),
            pltpu.VMEM((2, n_ctx, slots, features), f32),
            pltpu.VMEM((n_ctx, live, 128), f32),
            pltpu.VMEM((2 * n_ctx, live, 128), f32),
            pltpu.VMEM((2, n_ctx, slots, 128), f32),
            pltpu.VMEM((2, n_ep, dense, HEAD_WIDTH), bf16),
            pltpu.VMEM((n, dense, HEAD_WIDTH), bf16),
            *batch(n_ep * CAP),
            *batch((n - n_ep) * CAP),
            pltpu.VMEM((n, dense, HEAD_WIDTH), bf16),
            pltpu.VMEM((n, dense, HEAD_WIDTH), bf16),
            pltpu.VMEM((slots, features), f32),
            dma((3,)),
            dma,
            dma((2,)),
            dma,
            dma((n_ctx - 1, kv_heads + 1)),
            dma((2,)),
            dma((2,)),
            dma,
            dma((2,)),
            dma,
            dma((2,)),
            dma,
            dma,
            dma,
            dma((n_ctx,)),
            *[dma] * 4,
        ],
        compiler_params=pltpu.CompilerParams(
            collective_id=0, has_side_effects=True, vmem_limit_bytes=60 * 1024 * 1024
        ),
    )(
        expert_ids.reshape(1, rows), router.reshape(1, features), queries, keys, values,
        w_gate, w_up, w_down,
    )


def solution(mesh):
    placed = (
        P(("groups", "ep"), "ctx", "tp"),
        P(("groups", "ep"), "ctx", "tp"),
        P(("groups", "ep"), "ctx", "tp"),
        P(("groups", "ep"), "ctx", None),
        P("tp", "ep"),
        P("ep", "tp", "ctx"),
        P("ep", "tp", "ctx"),
        P("ep", "ctx", "tp"),
    )
    return jax.shard_map(
        shards,
        mesh=mesh,
        in_specs=placed,
        out_specs=P(("groups", "ep"), "ctx", "tp"),
        check_vma=False,
    )
```

```python
import functools
import math

import jax
import jax.numpy as jnp
from jax import lax
from jax.experimental import pallas as pl
from jax.experimental.pallas import tpu as pltpu
from jax.sharding import PartitionSpec as P

HEAD_WIDTH = 128
CAP = 2
MESH = pl.DeviceIdType.MESH
MASKED = -1e30
EXP2_SCALE = HEAD_WIDTH ** (-0.5) * math.log2(math.e)
scope = jax.named_scope


def tiles_of(width, tile):
    tile = min(width, tile)
    return [(start, min(tile, width - start)) for start in range(0, width, tile)]


def padded(count, tile=8):
    return -(-count // tile) * tile


def each(count, body):
    if count <= 8:
        for index in range(count):
            body(index)
    else:
        pl.loop(0, count)(body)


def kernel(
    n_ctx, n_ep, n_tp,
    ids_hbm, router_hbm, q_hbm, k_hbm, v_hbm, wg_hbm, wu_hbm, wd_hbm,
    out_ref,
    ids_ref, router_ref, q_ref, wgu, wd, kv, acc, row_max, totals, att,
    q_own, q_out, q_in, q_all, part_out, part_got, part_all, lse_out, lse_in, lse_all,
    out_rows, in_rows,
    members_a, part_a, part_in_a, hidden_a,
    members_b, part_b, part_in_b, hidden_b,
    down_out, down_in, returned,
    in_sem, own_sem, w_sem, kv_send, kv_recv, row_send, row_recv,
    a_send, a_recv, b_send, b_recv,
    down_send, down_recv, q_send, q_recv, back_send, back_recv, lse_send, lse_recv,
):
    ctx = lax.axis_index("ctx")
    ep = lax.axis_index("ep")
    tp = lax.axis_index("tp")
    n = n_ctx * n_ep
    me = ep * n_ctx + ctx
    last = n_ctx - 1
    home = last - 1
    rows, features = q_ref.shape
    kv_heads = kv.shape[1]
    places = features // HEAD_WIDTH
    group = places // kv_heads
    slots = returned.shape[0]
    live = n_ep * CAP

    def lanes(place):
        return slice(place * HEAD_WIDTH, (place + 1) * HEAD_WIDTH)

    in_copies = [
        pltpu.make_async_copy(src, dst, in_sem.at[index])
        for index, (src, dst) in enumerate((
            (ids_hbm, ids_ref), (q_hbm.at[0], q_ref), (router_hbm, router_ref),
        ))
    ]
    own_copies = [
        pltpu.make_async_copy(
            src.at[0, :, lanes(head)], kv.at[ctx, head, which], own_sem
        )
        for head in range(kv_heads)
        for which, src in enumerate((k_hbm, v_hbm))
    ]
    w_copies = [
        pltpu.make_async_copy(src.at[0], dst, sem)
        for src, dst, sem in (
            (wg_hbm, wgu.at[0], w_sem.at[0]), (wu_hbm, wgu.at[1], w_sem.at[0]),
            (wd_hbm, wd, w_sem.at[1]),
        )
    ]
    for copy in in_copies[:2] + own_copies + in_copies[2:]:
        copy.start()

    barrier = pltpu.get_barrier_semaphore()

    def greet(other):
        @pl.when(other != me)
        def _():
            pl.semaphore_signal(
                barrier, inc=1,
                device_id={"ep": other // n_ctx, "ctx": other % n_ctx},
                device_id_type=MESH,
            )

    each(n, greet)
    for step in range(1, n_tp):
        pl.semaphore_signal(
            barrier, inc=1, device_id={"tp": (tp + step) % n_tp}, device_id_type=MESH
        )

    peer = {"tp": n_tp - 1 - tp}

    def settled(ref, sem):
        return pltpu.make_async_remote_copy(
            src_ref=ref, dst_ref=ref, send_sem=sem, recv_sem=sem,
            device_id=peer, device_id_type=MESH,
        )

    def by_ctx(body):
        for index in range(n_ctx):
            pl.when(ctx == index)(functools.partial(body, index))

    def kv_copies(block, head):
        parts = [kv.at[block, head]]
        if head == kv_heads - 1:
            parts = [kv.at[block, head, 0], kv.at[block, head, 1]]
        return [
            pltpu.make_async_remote_copy(
                src_ref=part, dst_ref=part,
                send_sem=kv_send, recv_sem=kv_recv.at[block, head + index],
                device_id={"ctx": ctx + 1}, device_id_type=MESH,
            )
            for index, part in enumerate(parts)
        ]

    def push_own(heads):
        @pl.when(ctx < last)
        def _():
            for head in heads:
                for copy in kv_copies(ctx, head):
                    copy.start()

    def relay(block, heads):
        @pl.when((block >= 0) & (ctx < last))
        def _():
            for head in heads:
                for copy in kv_copies(block, head):
                    copy.wait_recv()
                    copy.start()

    def arrive(block, heads):
        for head in heads:
            for copy in kv_copies(block, head):
                copy.wait_recv()

    def q_copy(source, target):
        return pltpu.make_async_remote_copy(
            src_ref=q_out, dst_ref=q_in.at[source],
            send_sem=q_send, recv_sem=q_recv.at[source],
            device_id={"ctx": target}, device_id_type=MESH,
        )

    def back_copies(target):
        slot = jnp.where(target == last, n_ctx, 0) + ctx
        return [
            pltpu.make_async_remote_copy(
                src_ref=out.at[target], dst_ref=into.at[slot],
                send_sem=sent, recv_sem=got,
                device_id={"ctx": jnp.minimum(target, home)}, device_id_type=MESH,
            )
            for out, into, sent, got in (
                (part_out, part_got, back_send, back_recv),
                (lse_out, lse_in, lse_send, lse_recv),
            )
        ]

    def to_index(other, out, into, sent, got, source):
        return pltpu.make_async_remote_copy(
            src_ref=out, dst_ref=into.at[source],
            send_sem=sent, recv_sem=got,
            device_id={"ep": other // n_ctx, "ctx": other % n_ctx}, device_id_type=MESH,
        )

    def row_copy(other, which):
        got = row_recv.at[jnp.where(ctx == 0, 0, 1)]
        return to_index(
            other, out_rows.at[which, other // n_ctx], in_rows, row_send.at[which], got, me + which
        )

    def down_copy(other, source):
        return to_index(other, down_out.at[other], down_in, down_send, down_recv, source)

    def lower(body):
        def one(other):
            @pl.when(other < ctx)
            def _():
                body(other)

        each(n_ctx, one)

    def upper(body):
        def one(step):
            other = last - step

            @pl.when(other > ctx)
            def _():
                body(other)

        each(n_ctx, one)

    def others(body):
        def one(other):
            @pl.when(other != me)
            def _():
                body(other)

        each(n, one)

    def first_owners(body):
        def one(expert):
            @pl.when(expert * n_ctx != me)
            def _():
                body(expert * n_ctx)

        each(n_ep, one)

    def later_owners(body):
        def one(other):
            @pl.when((other % n_ctx != 0) & (other != me))
            def _():
                body(other)

        each(n, one)

    with scope("a_ids"):
        in_copies[0].wait()
    with scope("a_pick"):
        ids = ids_ref[...]
        slot_row = lax.broadcasted_iota(jnp.int32, (slots, rows), 0)
        choose = jnp.where(ids == slot_row, 1.0, 0.0)
        below = lax.broadcasted_iota(jnp.int32, (rows, rows), 0)
        across = lax.broadcasted_iota(jnp.int32, (rows, rows), 1)
        strict = jnp.where(below < across, 1.0, 0.0).astype(jnp.bfloat16)
        earlier = jnp.dot(
            choose.astype(jnp.bfloat16), strict, preferred_element_type=jnp.float32
        )
        slot_index = jnp.sum(earlier * choose, axis=0, keepdims=True).astype(jnp.int32)
        target_row = jnp.where(ids < n_ep, ids * CAP + slot_index, -1)
        spread = jnp.where(target_row == slot_row, 1.0, 0.0).astype(jnp.bfloat16)
        lane_row = lax.broadcasted_iota(jnp.int32, (slots, rows), 1)
        row_place = jnp.sum(
            jnp.where(target_row == slot_row, lane_row, 0), axis=1, keepdims=True
        )
        in_copies[1].wait()
        for copy in w_copies:
            copy.start()
        for start, size in tiles_of(features, 512):
            picked = jnp.dot(
                spread, q_ref[:, start:start + size], preferred_element_type=jnp.float32
            )
            q_own[:, start:start + size] = picked
            q_out[:, start:start + size] = picked[:live].astype(jnp.bfloat16)

    def attend(source, tall, seen):
        raws = []
        for head in range(kv_heads):
            stacked = jnp.concatenate(
                [source[:, lanes(head * group + j)] for j in range(group)], axis=0
            ).astype(jnp.bfloat16)
            raw = lax.dot_general(
                stacked, kv[ctx, head, 0], (((1,), (1,)), ((), ())),
                preferred_element_type=jnp.float32,
            )
            raws.append(raw if seen is None else jnp.where(seen, raw, MASKED))
        tops = [jnp.max(raw, axis=1, keepdims=True) for raw in raws]
        weights = [jnp.exp2((raw - top) * EXP2_SCALE) for raw, top in zip(raws, tops)]
        sums = [jnp.sum(weight, axis=1, keepdims=True) for weight in weights]
        mixed = [
            jnp.dot(
                weight.astype(jnp.bfloat16), kv[ctx, head, 1],
                preferred_element_type=jnp.float32,
            ) / total
            for head, (weight, total) in enumerate(zip(weights, sums))
        ]
        columns = [top * EXP2_SCALE + jnp.log2(total) for top, total in zip(tops, sums)]
        head_lane = lax.broadcasted_iota(jnp.int32, (tall, 128), 1)
        lse = jnp.zeros((tall, 128), jnp.float32)
        for head in range(kv_heads):
            for j in range(group):
                lse = jnp.where(
                    head_lane == head * group + j, columns[head][j * tall:(j + 1) * tall], lse
                )
        return mixed, lse

    def own_landed():
        pltpu.make_async_copy(kv.at[ctx], kv.at[ctx], own_sem).wait()

    def own_part():
        key_lane = lax.broadcasted_iota(jnp.int32, (group * slots, rows), 1)
        seen = key_lane <= jnp.concatenate([row_place] * group, axis=0)
        mixed, lse = attend(q_own, slots, seen)
        lse_all[...] = jnp.full_like(lse_all, MASKED)
        lse_all[0, ctx] = lse
        for head in range(kv_heads):
            for j in range(group):
                part_all[0, ctx, :, lanes(head * group + j)] = mixed[head][
                    j * slots:(j + 1) * slots
                ]

        return mixed, lse

    def put_row(which, place, picked):
        for expert in range(n_ep):
            out_rows[which, expert, place * CAP:(place + 1) * CAP] = picked[
                expert * CAP:(expert + 1) * CAP
            ].astype(jnp.bfloat16)

    def send_rows(which):
        others(lambda other: row_copy(other, which).start())
        in_rows[me + which] = out_rows[which, ep]

    part_all[...] = jnp.zeros_like(part_all)
    q_all[...] = jnp.zeros_like(q_all)

    @pl.when(ctx == 0)
    def _():
        with scope("b_own0"):
            own_landed()
            own_part()
            for place in range(places):
                put_row(0, place, part_all[0, 0, :, lanes(place)])

    with scope("c_barrier"):
        pl.semaphore_wait(barrier, n - 1 + n_tp - 1)

    with scope("d_qsend"):
        lower(lambda other: q_copy(ctx, other).start())

    @pl.when(ctx == 0)
    def _():
        with scope("e_rows0"):
            send_rows(0)
            push_own(range(1))

    @pl.when(ctx > 0)
    def _():
        with scope("f_own"):
            own_landed()
            push_own(range(2))
            pl.when(ctx > 1)(lambda: push_own(range(2, kv_heads)))
            mixed, lse = own_part()

            @pl.when(ctx == last)
            def _():
                lse_out[last] = lse[:live]
                for place in range(places):
                    first = place % group * slots
                    part_out[last, :, lanes(place)] = mixed[place // group][
                        first:first + live
                    ].astype(jnp.bfloat16)
                for copy in back_copies(last):
                    copy.start()

    query_offset = lax.broadcasted_iota(jnp.int32, (rows, rows), 0)
    key_offset = lax.broadcasted_iota(jnp.int32, (rows, rows), 1)

    def scores(block, head):
        stacked = jnp.concatenate(
            [q_ref[:, lanes(head * group + j)] for j in range(group)], axis=0
        )
        return lax.dot_general(
            stacked, kv[block, head, 0], (((1,), (1,)), ((), ())),
            preferred_element_type=jnp.float32,
        )

    def mix(weights, block, head):
        return jnp.dot(
            weights.astype(jnp.bfloat16), kv[block, head, 1], preferred_element_type=jnp.float32
        )

    with scope("g_own_block"):
        visible = jnp.concatenate([query_offset >= key_offset] * group, axis=0)
        for head in range(kv_heads):
            raw = jnp.where(visible, scores(ctx, head), MASKED)
            top = jnp.broadcast_to(jnp.max(raw, axis=1, keepdims=True), raw.shape)
            weights = jnp.exp2((raw - top) * EXP2_SCALE)
            row_max[head] = top
            totals[head] = jnp.broadcast_to(
                jnp.sum(weights, axis=1, keepdims=True), weights.shape
            )
            acc[head] = mix(weights, ctx, head)

    def process(block, head, before_values=None):
        raw = scores(block, head)
        old_max = row_max[head]
        new_max = jnp.maximum(old_max, jnp.max(raw, axis=1, keepdims=True))
        factor = jnp.exp2((old_max - new_max) * EXP2_SCALE)
        weights = jnp.exp2((raw - new_max) * EXP2_SCALE)
        row_max[head] = new_max
        totals[head] = totals[head] * factor + jnp.sum(weights, axis=1, keepdims=True)
        if before_values is not None:
            before_values()
        acc[head] = acc[head] * factor + mix(weights, block, head)

    def visit(step):
        pl.when(ctx == last)(lambda: arrive(ctx - step, range(kv_heads)))
        for head in range(kv_heads):
            process(ctx - step, head)

    def visit_by_head(step):
        for head in range(kv_heads):
            pl.when(ctx == last)(lambda: arrive(ctx - step, [head]))
            relay(ctx - step, [head])
            process(ctx - step, head)

    @pl.when(ctx < last)
    def _():
        with scope("h_qwait"):
            upper(lambda other: q_copy(other, other).wait_recv())
        with scope("i_qpart"):
            for other in range(n_ctx):
                @pl.when(other > ctx)
                def _():
                    q_all[other * live:(other + 1) * live, :] = q_in[other].astype(jnp.float32)

            tall = n_ctx * live
            mixed, lse = attend(q_all, tall, None)
            @pl.when(ctx == home)
            def _():
                lse_all[1, home, :live] = lse[last * live:]
                for place in range(places):
                    first = place % group * tall + last * live
                    part_all[1, home, :live, lanes(place)] = mixed[place // group][
                        first:first + live
                    ]

            for other in range(n_ctx):
                lse_out[other] = lse[other * live:(other + 1) * live]
                for place in range(places):
                    first = place % group * tall + other * live
                    part_out[other, :, lanes(place)] = mixed[place // group][
                        first:first + live
                    ].astype(jnp.bfloat16)

        with scope("j_give"):
            def give_back(other):
                for copy in back_copies(other):
                    copy.start()

            pl.when(ctx < home)(lambda: upper(give_back))
            pl.when(ctx == 0)(lambda: push_own(range(1, kv_heads)))
    def gate(indices, wide_ref, part, part_in, sent, got, between):
        for at, index in enumerate(indices):
            dense = in_rows[index].astype(jnp.float32)
            for place in range(places):
                wide_ref[at * CAP:(at + 1) * CAP, lanes(place)] = dense[
                    place * CAP:(place + 1) * CAP
                ]
        wide = wide_ref[...]
        members = wide.astype(jnp.bfloat16)
        own_score = jnp.sum(wide * router_ref[...].astype(jnp.float32), axis=1, keepdims=True)
        chunks, _, double_width = part.shape
        width = double_width // 2
        for chunk in range(chunks):
            if chunk == 0:
                part[0] = jnp.broadcast_to(own_score, part.shape[1:]).astype(jnp.bfloat16)
            else:
                span = slice((chunk - 1) * width, chunk * width)
                for side in range(2):
                    part[chunk, :, side * width:(side + 1) * width] = jnp.dot(
                        members, wgu[side, :, span], preferred_element_type=jnp.float32
                    ).astype(jnp.bfloat16)
            which = chunk // (chunks - 1)
            pltpu.make_async_remote_copy(
                src_ref=part.at[chunk], dst_ref=part_in.at[chunk],
                send_sem=sent, recv_sem=got.at[which],
                device_id=peer, device_id_type=MESH,
            ).start()
            between(chunk, chunks - 1)

    def activate(part, part_in, sent, got, hidden):
        chunks = part.shape[0]
        width = part.shape[2] // 2
        settled(part_in.at[pl.ds(0, chunks - 1)], got.at[0]).wait_recv()
        gain = jax.nn.sigmoid(
            part[0, :, :1].astype(jnp.float32) + part_in[0, :, :1].astype(jnp.float32)
        )
        for chunk in range(1, chunks):
            if chunk == chunks - 1:
                settled(part_in.at[chunk], got.at[1]).wait_recv()
            both = part[chunk].astype(jnp.float32) + part_in[chunk].astype(jnp.float32)
            gate_part = gain * both[:, :width]
            up_part = gain * both[:, width:]
            hidden[:, (chunk - 1) * width:chunk * width] = (
                gate_part * jax.nn.sigmoid(gate_part) * up_part
            ).astype(jnp.bfloat16)

    def down(indices, hidden):
        for start, size in tiles_of(features, 512):
            product = jnp.dot(
                hidden[...], wd[:, start:start + size], preferred_element_type=jnp.float32
            )
            for at, index in enumerate(indices):
                for place in range(start // HEAD_WIDTH, (start + size) // HEAD_WIDTH):
                    lane = place * HEAD_WIDTH - start
                    down_out[index, place * CAP:(place + 1) * CAP] = product[
                        at * CAP:(at + 1) * CAP, lane:lane + HEAD_WIDTH
                    ].astype(jnp.bfloat16)

    def keep_own():
        down_in[me] = down_out[me]

    first = [index for index in range(n) if index % n_ctx == 0]
    later = [index for index in range(n) if index % n_ctx != 0]
    exchange_a = (part_a, part_in_a, a_send, a_recv)
    exchange_b = (part_b, part_in_b, b_send, b_recv)

    with scope("l_rows_a"):
        in_copies[2].wait()
        pltpu.make_async_copy(wgu, wgu, w_sem.at[0]).wait()

        @pl.when(ctx == 0)
        def _():
            if n_ep > 1:
                settled(in_rows.at[pl.ds(0, n_ep - 1)], row_recv.at[0]).wait_recv()

        @pl.when(ctx > 0)
        def _():
            settled(in_rows.at[pl.ds(0, n_ep)], row_recv.at[0]).wait_recv()
    def between_a(chunk, count):
        if chunk == (count + 1) // 2:
            pl.when(ctx == 1)(lambda: push_own(range(2, kv_heads)))
            pl.when(ctx > 1)(lambda: relay(ctx - 1, [0]))

    def between_b(chunk, count):
        if chunk == (count + 1) // 2:
            relay(ctx - 2, [0])

    with scope("m_gate_a"):
        gate(first, members_a, *exchange_a, between_a)

    def combine(which):
        peak = jnp.max(lse_all[which], axis=0)
        shares = [jnp.exp2(lse_all[which, other] - peak) for other in range(n_ctx)]
        share_total = functools.reduce(jnp.add, shares)
        shares = [share / share_total for share in shares]
        for place in range(places):
            put_row(which, place, functools.reduce(jnp.add, [
                shares[other][:, place:place + 1] * part_all[which, other, :, lanes(place)]
                for other in range(n_ctx)
            ]))

    def take(which, other):
        slot = which * n_ctx + other
        part_all[which, other, :live] = part_got[slot].astype(jnp.float32)
        lse_all[which, other, :live] = lse_in[slot]

    @pl.when((ctx > 0) & (ctx < last))
    def _():
        with scope("o_takeback"):
            def take_back(count):
                if 0 < count < last:
                    count = 2 * count + 1 if count == home else count
                    settled(part_got.at[pl.ds(0, count)], back_recv).wait_recv()
                    settled(lse_in.at[pl.ds(0, count)], lse_recv).wait_recv()

            by_ctx(take_back)
        with scope("p_combine"):
            for other in range(home):
                pl.when(other < ctx)(functools.partial(take, 0, other))

            @pl.when(ctx == home)
            def _():
                for other in range(n_ctx):
                    if other != home:
                        take(1, other)
                combine(1)
                send_rows(1)

            combine(0)
        with scope("q_rows"):
            send_rows(0)
            pl.when(ctx == 1)(lambda: relay(ctx - 1, [0]))
            pl.when(ctx > 1)(lambda: relay(ctx - 1, [1]))

    with scope("r_down_a"):
        w_copies[2].wait()
        activate(*exchange_a, hidden_a)
        down(first, hidden_a)
        first_owners(lambda other: down_copy(other, me).start())
        pl.when(ctx == 0)(keep_own)
    with scope("s_relay"):
        pl.when(ctx == 1)(lambda: relay(ctx - 1, range(1, kv_heads)))
        pl.when(ctx > 1)(lambda: relay(ctx - 1, range(2, kv_heads)))
    with scope("t_block1"):
        pl.when(ctx > 1)(lambda: visit(1))
    with scope("v_rows_b"):
        @pl.when((ctx == 0) | (ctx == last))
        def _():
            settled(in_rows.at[pl.ds(0, n - n_ep)], row_recv.at[1]).wait_recv()

        @pl.when((ctx > 0) & (ctx < home))
        def _():
            settled(in_rows.at[pl.ds(0, n - n_ep - 1)], row_recv.at[1]).wait_recv()

        @pl.when(ctx == home)
        def _():
            settled(in_rows.at[pl.ds(0, n - n_ep - 2)], row_recv.at[1]).wait_recv()

    with scope("w_gate_b"):
        gate(later, members_b, *exchange_b, between_b)
    ahead = tp == n_tp - 1
    early = ahead & (ctx > 2)
    with scope("x_relay"):
        relay(ctx - 2, [1])
        pl.when(ahead)(lambda: relay(ctx - 2, range(2, kv_heads)))
    with scope("xa_block2"):
        pl.when(early)(lambda: visit(2))
    with scope("xb_down_b"):
        activate(*exchange_b, hidden_b)
        down(later, hidden_b)
        later_owners(lambda other: down_copy(other, me).start())
        pl.when(ctx > 0)(keep_own)

    def remaining(step, carry):
        pl.when(ctx >= step)(lambda: visit_by_head(step))
        return carry

    def norm(head):
        normed = (acc[head] / totals[head]).astype(jnp.bfloat16)
        for j in range(group):
            att[:, lanes(head * group + j)] = normed[j * rows:(j + 1) * rows]

    def settle_down():
        settled(down_in.at[pl.ds(0, n - 1)], down_recv).wait_recv()
        returned[...] = jnp.zeros_like(returned)
        for expert in range(n_ep):
            total = down_in[expert * n_ctx].astype(jnp.float32)
            for index in range(1, n_ctx):
                total = total + down_in[expert * n_ctx + index].astype(jnp.float32)
            total = total.astype(jnp.bfloat16).astype(jnp.float32)
            for place in range(places):
                returned[expert * CAP:(expert + 1) * CAP, lanes(place)] = total[
                    place * CAP:(place + 1) * CAP
                ]

    def finish(head):
        width = group * HEAD_WIDTH
        span = slice(head * width, (head + 1) * width)
        routed = lax.dot_general(
            spread, returned[:, span].astype(jnp.bfloat16),
            (((0,), (0,)), ((), ())), preferred_element_type=jnp.float32,
        )
        out_ref[0, :, span] = (att[:, span].astype(jnp.float32) + routed).astype(jnp.bfloat16)

    with scope("xc_visit"):
        pl.when(jnp.logical_not(ahead))(lambda: relay(ctx - 2, range(2, kv_heads)))
        left = jnp.where(ctx == 1, 1, 2)

        @pl.when((ctx > 0) & jnp.logical_not(early))
        def _():
            visit(left)

    ends = (ctx == last) & (last > 2)

    @pl.when(ends)
    def _():
        with scope("xd_visit"):
            lax.fori_loop(3, last, remaining, 0)

            def arrived(head):
                first, *rest = kv_copies(0, head)
                first.wait_recv()
                process(0, head, rest[0].wait_recv if rest else None)
                norm(head)

            def run(before):
                for head in range(before):
                    arrived(head)
                settle_down()
                for head in range(before):
                    finish(head)
                final = list(range(before, kv_heads))
                values = [copy for head in final for copy in kv_copies(0, head)]
                for copy in values[:-1]:
                    copy.wait_recv()
                for head in final:
                    process(0, head, values[-1].wait_recv if head == kv_heads - 1 else None)
                for head in final:
                    norm(head)
                    finish(head)

            pl.when(ahead)(lambda: run(kv_heads))
            pl.when(jnp.logical_not(ahead))(lambda: run(kv_heads - 2))

    @pl.when(jnp.logical_not(ends))
    def _():
        lax.fori_loop(3, n_ctx, remaining, 0)
        with scope("xd_norm"):
            for head in range(kv_heads):
                norm(head)
        with scope("xe_down"):
            settle_down()
        with scope("xg_final"):
            for head in range(kv_heads):
                finish(head)

    with scope("xh_sent"):
        settled(part_a, a_send).wait_send()
        settled(part_b, b_send).wait_send()

        def drain(index):
            if index:
                settled(q_in.at[pl.ds(0, index)], q_send).wait_send()
            given = {home: 0, last: 1}.get(index, last - index)
            if given:
                settled(part_out.at[pl.ds(0, given)], back_send).wait_send()
                settled(lse_out.at[pl.ds(0, given)], lse_send).wait_send()
            for which in range({home: 2, last: 0}.get(index, 1)):
                settled(in_rows.at[pl.ds(0, n - 1)], row_send.at[which]).wait_send()
            if index < last:
                settled(kv.at[pl.ds(0, index + 1)], kv_send).wait_send()

        by_ctx(drain)
        settled(down_out.at[pl.ds(0, n - 1)], down_send).wait_send()


def shards(queries, keys, values, expert_ids, router, w_gate, w_up, w_down):
    n_ctx, n_ep, n_tp = (lax.axis_size(axis) for axis in ("ctx", "ep", "tp"))
    n = n_ctx * n_ep
    _, rows, features = queries.shape
    kv_width = keys.shape[2]
    kv_heads = kv_width // HEAD_WIDTH
    group = features // kv_width
    hidden_width = w_gate.shape[2]
    chunk_width = min(hidden_width, 256)
    chunks = hidden_width // chunk_width
    dense = features // HEAD_WIDTH * CAP
    live = n_ep * CAP
    slots = padded(live)
    bf16, f32 = jnp.bfloat16, jnp.float32
    hbm = pl.BlockSpec(memory_space=pltpu.HBM)
    dma = pltpu.SemaphoreType.DMA

    def batch(count):
        return [
            pltpu.VMEM((count, features), f32),
            pltpu.VMEM((chunks + 1, count, 2 * chunk_width), bf16),
            pltpu.VMEM((chunks + 1, count, 2 * chunk_width), bf16),
            pltpu.VMEM((count, hidden_width), bf16),
        ]

    return pl.pallas_call(
        functools.partial(kernel, n_ctx, n_ep, n_tp),
        out_shape=pltpu.VMEM(queries.shape, bf16),
        in_specs=[hbm] * 8,
        out_specs=pl.BlockSpec(memory_space=pltpu.VMEM),
        scratch_shapes=[
            pltpu.VMEM((1, rows), jnp.int32),
            pltpu.VMEM((1, features), bf16),
            pltpu.VMEM((rows, features), bf16),
            pltpu.VMEM((2, *w_gate.shape[1:]), bf16),
            pltpu.VMEM(w_down.shape[1:], bf16),
            pltpu.VMEM((n_ctx, kv_heads, 2, rows, HEAD_WIDTH), bf16),
            pltpu.VMEM((kv_heads, group * rows, HEAD_WIDTH), f32),
            pltpu.VMEM((kv_heads, group * rows, HEAD_WIDTH), f32),
            pltpu.VMEM((kv_heads, group * rows, HEAD_WIDTH), f32),
            pltpu.VMEM((rows, features), bf16),
            pltpu.VMEM((slots, features), f32),
            pltpu.VMEM((live, features), bf16),
            pltpu.VMEM((n_ctx, live, features), bf16),
            pltpu.VMEM((n_ctx * live, features), f32),
            pltpu.VMEM((n_ctx, live, features), bf16),
            pltpu.VMEM((2 * n_ctx, live, features), bf16),
            pltpu.VMEM((2, n_ctx, slots, features), f32),
            pltpu.VMEM((n_ctx, live, 128), f32),
            pltpu.VMEM((2 * n_ctx, live, 128), f32),
            pltpu.VMEM((2, n_ctx, slots, 128), f32),
            pltpu.VMEM((2, n_ep, dense, HEAD_WIDTH), bf16),
            pltpu.VMEM((n, dense, HEAD_WIDTH), bf16),
            *batch(n_ep * CAP),
            *batch((n - n_ep) * CAP),
            pltpu.VMEM((n, dense, HEAD_WIDTH), bf16),
            pltpu.VMEM((n, dense, HEAD_WIDTH), bf16),
            pltpu.VMEM((slots, features), f32),
            dma((3,)),
            dma,
            dma((2,)),
            dma,
            dma((n_ctx - 1, kv_heads + 1)),
            dma((2,)),
            dma((2,)),
            dma,
            dma((2,)),
            dma,
            dma((2,)),
            dma,
            dma,
            dma,
            dma((n_ctx,)),
            *[dma] * 4,
        ],
        compiler_params=pltpu.CompilerParams(
            collective_id=0, has_side_effects=True, vmem_limit_bytes=60 * 1024 * 1024
        ),
    )(
        expert_ids.reshape(1, rows), router.reshape(1, features), queries, keys, values,
        w_gate, w_up, w_down,
    )


def solution(mesh):
    placed = (
        P(("groups", "ep"), "ctx", "tp"),
        P(("groups", "ep"), "ctx", "tp"),
        P(("groups", "ep"), "ctx", "tp"),
        P(("groups", "ep"), "ctx", None),
        P("tp", "ep"),
        P("ep", "tp", "ctx"),
        P("ep", "tp", "ctx"),
        P("ep", "ctx", "tp"),
    )
    return jax.shard_map(
        shards,
        mesh=mesh,
        in_specs=placed,
        out_specs=P(("groups", "ep"), "ctx", "tp"),
        check_vma=False,
    )
```
